1024 devices in a mesh: band: 16 (over z, core), px: 16 (over y_lo, x), py: 4 (over y_hi).
Axes of the slice: x: 8, y: 8 (y_hi: 4, y_lo: 2; y = y_hi * 2 + y_lo), z: 8, core: 2. Of those that a mesh axis runs over, the one named last changes fastest.
Arguments:
- orbitals: bfloat16 [16, 8192, 384], P('band', ('px', 'py')), may hold values from -0.001953125 to 0.001953125
- occupations: float32 [16], P('band'), may hold values from 0.2 to 2
- stick_map: int32 [2, 8192], P(None, 'px'), may hold values from 0 to 191, as said below
- core_density: float32 [192, 192, 192], P('py', 'px'), may hold values from 0.05 to 0.5
Outputs:
- potential: float32 [192, 192, 192], P('py', 'px')
- gradient: float32 [3, 192, 192, 192], P(None, 'py', 'px')
The draws below stay inside these ranges and needn't reach their ends.
Inputs may be any that keep to these rules, and one draw needn't show every extreme that they name: `stick_map`: columns i * 128 * 4 to (i + 1) * 128 * 4 - 1 have x index from i * 12 to (i + 1) * 12 - 1; no two columns share a grid position.
All inputs are finite; a program needn't handle non-finite values.
Results may differ from the reference program's by a relative error of at most 0.0054.
Values may be sent and summed in bfloat16 or wider, within the bound.
A program may use at most 64 MiB of HBM per device.

```python
import math
import jax
import jax.numpy as jnp
from jax import lax

NG = 192
STK_DEV = 128
BANDS = 16
STICKS = 8192
N_PX = 16
N_PY = 4


def draw_stick_map(key, part):
    per_block = STK_DEV * N_PY
    xblock = NG // N_PX
    block_keys = jax.random.split(key, N_PX)

    def pick_block(one_key):
        return jax.random.permutation(one_key, xblock * NG)[:per_block]
    chosen = jax.vmap(pick_block)(block_keys)
    offsets = jnp.arange(N_PX, dtype=jnp.int32)[:, None] * xblock
    x_pos = offsets + chosen // NG
    y_pos = chosen % NG
    return jnp.stack([x_pos.reshape(-1), y_pos.reshape(-1)]).astype(jnp.int32)


def level_of(stream_key, shape, pieces, least, largest):
    def one(position, parts):
        heights = jax.random.uniform(jax.random.fold_in(jax.random.fold_in(stream_key, 6), position), (parts,), jnp.float32, least / len(pieces), largest / len(pieces))
        return jnp.repeat(jnp.exp(heights), shape[position] // parts).reshape((-1,) + (1,) * (len(shape) - position - 1))

    loudness = one(*pieces[0])
    for cut in pieces[1:]:
        loudness = loudness * one(*cut)
    return loudness


def scatter_about(own_key, dims, spread, limit, cuts=(), kind=jnp.bfloat16):
    entries = spread * jax.random.normal(own_key, dims, jnp.float32)
    if cuts:
        entries = entries * level_of(own_key, dims, cuts, -0.22, 0.18)
    return jnp.clip(entries, -limit, limit).astype(kind)


def setup_inputs(seed: int = 0) -> dict:
    seeds = jax.random.split(jax.random.key(seed), 5)
    orbitals = scatter_about(seeds[0], (BANDS, STICKS, 2 * NG), ((2 * STICKS * NG * BANDS) ** -0.5), 0.001953125, ((0, 16), (1, 64)))
    occupations = jnp.clip(0.2 + 1.8 * jax.random.uniform(seeds[1], (BANDS,), jnp.float32) ** level_of(seeds[1], (BANDS,), ((0, 16),), -0.2, 0.2), 0.2, 2.0)
    stick_map = draw_stick_map(jax.random.fold_in(seeds[4], 71), 0)
    core_density = jnp.clip(jnp.exp(math.log(0.5) - 2.3025851 * jax.random.uniform(seeds[3], (NG, NG, NG), jnp.float32) ** level_of(seeds[3], (NG, NG, NG), ((0, 4), (1, 16)), -0.2, 0.2)), 0.05, 0.5)
    return dict(orbitals=orbitals, occupations=occupations, stick_map=stick_map, core_density=core_density)


SPACING = 0.25
PBE_KAPPA = 0.804
PBE_MU = 0.2195
SLATER_COEF = 0.75 * (3.0 / math.pi) ** (1.0 / 3.0)
REDUCED_SCALE = 4.0 * (3.0 * math.pi ** 2) ** (2.0 / 3.0)


def rounded(values):
    return lax.optimization_barrier(values.astype(jnp.bfloat16)).astype(jnp.float32)


def exchange_part(density, hartree, grad_x, grad_y, grad_z):
    cube_root = jnp.cbrt(density)
    four_thirds = density * cube_root
    grad_square = grad_x * grad_x + grad_y * grad_y + grad_z * grad_z
    reduced = grad_square / (REDUCED_SCALE * four_thirds * four_thirds)
    denominator = 1.0 + PBE_MU * reduced / PBE_KAPPA
    enhance = 1.0 + PBE_KAPPA - PBE_KAPPA / denominator
    enhance_slope = PBE_MU / (denominator * denominator)
    return hartree - SLATER_COEF * cube_root * ((4.0 / 3.0) * enhance - (8.0 / 3.0) * reduced * enhance_slope)


def reference(orbitals, occupations, stick_map, core_density):
    points = orbitals.shape[2] // 2
    x_cols = stick_map[0]
    y_cols = stick_map[1]

    def add_band(summed, inputs):
        coeffs, weight = inputs
        real_in = coeffs[:, :points].astype(jnp.float32)
        imag_in = coeffs[:, points:].astype(jnp.float32)
        along_z = jnp.fft.ifft(real_in + 1j * imag_in, axis=1) * points
        plane_real = jnp.zeros((points, points, points), jnp.float32).at[:, y_cols, x_cols].set(rounded(along_z.real).T)
        plane_imag = jnp.zeros((points, points, points), jnp.float32).at[:, y_cols, x_cols].set(rounded(along_z.imag).T)
        along_y = jnp.fft.ifft(plane_real + 1j * plane_imag, axis=1) * points
        along_x = jnp.fft.ifft(rounded(along_y.real) + 1j * rounded(along_y.imag), axis=2) * points
        return summed + weight * (along_x.real * along_x.real + along_x.imag * along_x.imag), None

    valence = lax.scan(add_band, jnp.zeros((points, points, points), jnp.float32), (orbitals, occupations))[0]
    density = valence + core_density
    rho_hat = jnp.fft.fftn(density)
    every_index = jnp.arange(points)
    q_full = jnp.where(every_index <= points // 2, every_index, every_index - points).astype(jnp.float32)
    g_full = jnp.where(every_index == points // 2, 0.0, q_full).astype(jnp.float32)
    wave_unit = 2.0 * math.pi / (points * SPACING)
    squared = wave_unit ** 2 * (q_full[:, None, None] ** 2 + q_full[None, :, None] ** 2 + q_full[None, None, :] ** 2)
    hartree_factor = jnp.where(squared > 0, 4.0 * math.pi / jnp.where(squared > 0, squared, 1.0), 0.0)
    hartree = jnp.fft.ifftn(hartree_factor * rho_hat).real
    grad_x = jnp.fft.ifftn(1j * wave_unit * g_full[None, None, :] * rho_hat).real
    grad_y = jnp.fft.ifftn(1j * wave_unit * g_full[None, :, None] * rho_hat).real
    grad_z = jnp.fft.ifftn(1j * wave_unit * g_full[:, None, None] * rho_hat).real
    potential = exchange_part(density, hartree, grad_x, grad_y, grad_z)
    return potential, jnp.stack([grad_x, grad_y, grad_z])
```

```python
import functools
import math

import jax
import jax.numpy as jnp
import numpy as np
from jax import lax
from jax.experimental import pallas as pl
from jax.experimental.pallas import tpu as pltpu
from jax.sharding import PartitionSpec as P

N = 192
SPACING = 0.25
KAPPA = 0.804
MU = 0.2195
SLATER = 0.75 * (3.0 / math.pi) ** (1.0 / 3.0)
REDUCED = 4.0 * (3.0 * math.pi**2) ** (2.0 / 3.0)
UNIT = 2.0 * math.pi / (N * SPACING)
F32 = jnp.float32
BF = jnp.bfloat16
MESH = pl.DeviceIdType.MESH
roll = pltpu.roll


def hilo(a):
    a = np.asarray(a, np.float32)
    hi = a.astype(BF)
    lo = (a - hi.astype(np.float32)).astype(BF)
    return np.stack([hi, lo])


def real_basis():
    n = np.arange(N)
    k = np.where(n <= 96, n, n - 96)
    cosine = n <= 96
    x = np.arange(N)
    angle = 2 * np.pi * (k[:, None] * x[None, :] % N) / N
    forward = np.where(cosine[:, None], np.cos(angle), np.sin(angle))
    weight = np.where((k == 0) | (k == 96), 1.0, 2.0)
    weight = np.where(cosine, weight, 2.0) / N
    inverse = (forward * weight[:, None]).T
    g = np.where(k == 96, 0.0, k) * UNIT
    slope = np.where(cosine[:, None], -np.sin(angle), np.cos(angle)) * (g * weight)[:, None]
    return forward, inverse, slope.T, (UNIT * k) ** 2


def make_tables():
    fwd, inv, dif, q2 = real_basis()
    idx = np.arange(N)
    ang = 2 * np.pi * (idx[:, None] * idx[None, :] % N) / N
    c, s = np.cos(ang), np.sin(ang)
    ta = np.zeros((64, 8, 384))
    for j in range(3):
        z = 3 * np.arange(64) + j
        ta[:, j, :N], ta[:, j, N:] = c[z], -s[z]
        ta[:, 3 + j, :N], ta[:, 3 + j, N:] = s[z], c[z]
    tyc = np.zeros((256, 512))
    tyc[:N, :N], tyc[:N, 256 : 256 + N] = c, s
    tx = np.zeros((384, 256))
    xp = 16 * (idx // 12) + idx % 12
    tx[:N, xp], tx[N:, xp] = c, s
    band = idx // 12
    krow = 128 * (band % 2) + 16 * (band // 2) + idx % 12
    ry = np.zeros((256, 256))
    ry[krow, :N] = fwd
    px, py, i = idx // 12, (idx % 12) // 3, idx % 3
    rx = np.zeros((N, 256))
    rx[:, 64 * i + 16 * py + px] = fwd.T
    rx[:, 192] = fwd[0]
    zo = (3 * np.arange(64)[None, :] + np.arange(3)[:, None]).reshape(-1)
    rz = fwd[:, zo]
    hz = inv[zo, :]
    gz = (dif @ fwd)[zo][:, zo]
    kcol = 16 * (idx % 12) + 8 * (band % 2) + band // 2
    ryi = np.zeros((2, 256, N))
    ryi[0][np.ix_(xp, kcol)] = inv
    ryi[1][np.ix_(xp, kcol)] = dif
    kx = 16 * (4 * i + py) + px
    rxi = np.zeros((256, 512))
    rxi[kx, :N] = inv.T
    rxi[kx, 256 : 256 + N] = dif.T
    qx = np.zeros((64, 1, 128), np.float32)
    qy = np.zeros((16, 1, 128), np.float32)
    for ii in range(3):
        for t in range(12):
            p = np.arange(64)
            qx[:, 0, 12 * ii + t] = q2[12 * (p % 16) + 3 * (p // 16) + ii]
            qy[:, 0, 12 * ii + t] = q2[12 * np.arange(16) + t]
    qz = np.broadcast_to(q2[:, None], (N, 128)).astype(np.float32)
    tabs = [hilo(a) for a in (ta.reshape(512, 384), tyc, tx, ry, rx, rz, hz, gz, ryi, rxi)]
    return tabs + [qx, qy, qz]


def mm(a, b):
    return lax.dot_general(a, b, (((1,), (0,)), ((), ())), preferred_element_type=F32)


def mmt(a, b):
    return lax.dot_general(a, b, (((1,), (1,)), ((), ())), preferred_element_type=F32)


def split(x):
    hi = x.astype(BF)
    return hi, (x - hi.astype(F32)).astype(BF)


def mm3(a, b, dot=mm):
    return dot(a[0], b[0]) + dot(a[0], b[1]) + dot(a[1], b[0])


def stage_columns(orb, x_of, y_of, px, ta):
    out = mmt(ta[0], orb) + mmt(ta[1], orb)
    row = lax.broadcasted_iota(jnp.int32, (8, 128), 0)
    place = jnp.where(row == 6, (x_of - px * 12).astype(F32), jnp.where(row == 7, y_of.astype(F32), 0.0))
    return (out.reshape(64, 8, 128) + place[None]).astype(BF)


def stage_scatter(pieces):
    data = jnp.concatenate(pieces, axis=1).astype(F32)
    hot = (lax.broadcasted_iota(jnp.int32, (256, 512), 0).astype(F32) == data[7:8]).astype(F32).astype(BF)
    place = lax.broadcasted_iota(jnp.int32, (16, 512), 0).astype(F32) == data[6:7]
    rows = jnp.concatenate([jnp.where(place, data[r : r + 1], 0.0) for r in range(6)], axis=0)
    return mmt(rows.astype(BF), hot).astype(BF)


def stage_density(p_re, p_im, weight, tyc, tx):
    a = mm(p_re, tyc[0]) + mm(p_re, tyc[1])
    b = mm(p_im, tyc[0]) + mm(p_im, tyc[1])
    y_re = (a[:, :256] - b[:, 256:]).astype(BF)
    y_im = (a[:, 256:] + b[:, :256]).astype(BF)
    a = mm(tx[0], y_re) + mm(tx[1], y_re)
    b = mm(tx[0], y_im) + mm(tx[1], y_im)
    re = a[:N] - b[N:]
    im = a[N:] + b[:N]
    return weight * (re * re + im * im)


def stage_plane(rho, ry, rx):
    t = mm3(ry, split(rho), mmt)
    return mm3(split(t), rx)


def stage_core(core, band, ry, rx):
    core = jnp.concatenate([core, jnp.zeros((4, N), F32)], axis=0)
    part = split(mm3(split(core), rx))
    y = lax.broadcasted_iota(jnp.int32, (256, 16), 0)
    t = lax.broadcasted_iota(jnp.int32, (256, 16), 1)
    pick = jnp.where((y == 12 * band + t) & (t < 12), 1.0, 0.0).astype(BF)
    placed = [mm(pick, h).astype(BF) for h in part]
    return mm3(ry, placed)


def halves_for_wire(x):
    lane = lax.broadcasted_iota(jnp.int32, x.shape, x.ndim - 1)
    return jnp.where(lane == 192, x - x.astype(BF).astype(F32), x).astype(BF)


def stage_pack(s):
    gap = jnp.zeros((24, 256), F32)
    rows = jnp.concatenate([s[0], gap, s[1], gap, s[2], gap, gap[:8]], axis=0)
    t = rows.T
    return t[0:64] + t[192:256] + roll(t[64:128], 12, 1) + roll(t[128:192], 24, 1)


def stage_z(w, qx, qy, qz, rz, hz, gz):
    lane = lax.broadcasted_iota(jnp.int32, (64, 128), 1)
    inside = lane < 36
    cols = jnp.concatenate([jnp.where(inside, w if j == 0 else roll(w, 128 - 40 * j, 1), 0.0) for j in range(3)], axis=0)
    both = split(cols)
    spectrum = mm3(rz, both)
    squared = qz + (qx + qy)
    factor = jnp.where(squared > 0, 4.0 * math.pi / jnp.where(squared > 0, squared, 1.0), 0.0)
    hart = mm3(hz, split(spectrum * factor))
    slope = mm3(gz, both)
    full = cols + roll(hart, 40, 1) + roll(slope, 80, 1)
    group = jnp.where(lane % 40 < 36, lane % 40 // 12, 9)
    out = []
    for i in range(3):
        acc = jnp.zeros((64, 128), F32)
        for j in range(3):
            shift = (12 * (j - i)) % 128
            part = full[64 * j : 64 * j + 64]
            acc = jnp.where(group == j, roll(part, shift, 1) if shift else part, acc)
        out.append(acc)
    return out


def swap_minor(x):
    lane = lax.broadcasted_iota(jnp.int32, (16, 128), 1)
    moved = [x[u] if u == 0 else roll(x[u], u, 1) for u in range(12)]
    out = []
    for v in range(12):
        at = lane - v
        at = jnp.where((at >= 0) & (at < 120) & (at % 40 < 36), at % 40 % 12, 99)
        acc = jnp.zeros((16, 128), F32)
        for u in range(12):
            acc = jnp.where(at == u, moved[u], acc)
        out.append(acc if v == 0 else roll(acc, 128 - v, 1))
    return out


def stage_y(x, ryi):
    cols = split(jnp.concatenate(swap_minor(x), axis=0))
    return mm3((ryi[0][0], ryi[1][0]), cols), mm3((ryi[0][1], ryi[1][1]), cols)


def stage_x(a, g, rxi):
    fill = jnp.zeros((64, 128), F32)
    f = jnp.concatenate(swap_minor(a) + [fill], axis=0).T.astype(BF)
    s = jnp.concatenate(swap_minor(g) + [fill], axis=0).T.astype(BF)
    both = mm(f, rxi[0]) + mm(f, rxi[1])
    gy = mm(s[0:64], rxi[0][:, :256]) + mm(s[0:64], rxi[1][:, :256])
    return both[0:40, :256], both[40:80, :256], both[0:40, 256:], gy[0:40], both[80:120, :256]


def stage_potential(rho, hart, gx, gy, gz):
    rho = jnp.where(rho > 0, rho, 1.0)
    cube_root = jnp.exp(jnp.log(rho) * (1.0 / 3.0))
    four = rho * cube_root
    reduced = (gx * gx + gy * gy + gz * gz) / (REDUCED * four * four)
    inverse = 1.0 / (1.0 + MU * reduced / KAPPA)
    enhance = 1.0 + KAPPA - KAPPA * inverse
    slope = MU * inverse * inverse
    return hart - SLATER * cube_root * ((4.0 / 3.0) * enhance - (8.0 / 3.0) * reduced * slope)


def stage_block(fields):
    lane = lax.broadcasted_iota(jnp.int32, (40, 128), 1)
    rows = [f[:, :128] for f in fields]
    for k in (0, 2):
        rows.append(jnp.where(lane < 64, fields[k][:, 128:], roll(fields[k + 1][:, 128:], 64, 1)))
    return jnp.concatenate(rows, axis=0).astype(BF)


def kernel(
    orb, occ, sticks, core, ta, tyc, tx, ry, rx, rz, hz, gz, ryi, rxi, qx, qy, qz,
    pot, grad,
    s1, r1a, r1b, core_in, planes, part, r2a, sums, r2b, s3, r3a, r3b, s4, r4a, r4b, r4c,
    s5, r5a, r5b, wide, r6, send, recv,
):
    band, px, py = lax.axis_index("band"), lax.axis_index("px"), lax.axis_index("py")
    cz, cc = band // 2, band % 2
    cx, lo = px % 8, px // 8
    cy = 2 * py + lo

    def at(z=None, c=None, x=None, y=None):
        z, c = cz if z is None else z, cc if c is None else c
        x, y = cx if x is None else x, cy if y is None else y
        return (z * 2 + c, (y % 2) * 8 + x, y // 2)

    def ring(me, d, n):
        return lax.rem(me + d, n)

    bar = pltpu.get_barrier_semaphore()

    def hail(target):
        pl.semaphore_signal(bar, inc=1, device_id=target, device_id_type=MESH)

    swapped = (px, band, py)
    for d in range(1, 8):
        hail(at(x=ring(cx, d, 8)))
        hail(at(y=ring(cy, d, 8)))
        hail(at(z=ring(cz, d, 8)))
    hail(at(c=1 - cc))

    @pl.when(band != px)
    def _():
        hail(swapped)

    count = [0]

    def copy(src, dst, target):
        k = count[0]
        count[0] += 1
        c = pltpu.make_async_remote_copy(
            src_ref=src, dst_ref=dst, send_sem=send.at[k], recv_sem=recv.at[k],
            device_id=target, device_id_type=MESH,
        )
        c.start()
        return c

    mine = pl.ds(pl.multiple_of(py * 128, 128), 128)
    s1[...] = stage_columns(orb[...], sticks[0:1, mine], sticks[1:2, mine], px, ta).reshape(8, 8, 8, 128)
    pl.semaphore_wait(bar, 22 + jnp.where(band != px, 1, 0))

    flights = [copy(s1.at[ring(cy, d, 8)], r1a.at[cy], at(y=ring(cy, d, 8))) for d in range(1, 8)]
    rows = core.at[pl.ds(3 * band, 3)]
    core_copy = pltpu.make_async_remote_copy(
        src_ref=rows, dst_ref=core_in, send_sem=send.at[80], recv_sem=recv.at[80],
        device_id=swapped, device_id_type=MESH,
    )
    own_copy = pltpu.make_async_copy(rows, core_in, send.at[81])

    @pl.when(band != px)
    def _():
        core_copy.start()

    @pl.when(band == px)
    def _():
        own_copy.start()

    r1a[cy] = s1[cy]
    for f in flights:
        f.wait()
    flights = [copy(r1a.at[:, ring(cx, d, 8)], r1b.at[:, cx], at(x=ring(cx, d, 8))) for d in range(1, 8)]
    for y in range(8):
        r1b[y, cx] = r1a[y, cx]

    @pl.when(band != px)
    def _():
        core_copy.wait()

    @pl.when(band == px)
    def _():
        own_copy.wait()

    def core_step(j, carry):
        part[j] = stage_core(core_in[j], band, ry, rx)
        return carry

    lax.fori_loop(0, 3, core_step, 0)
    for f in flights:
        f.wait()

    def scatter_step(k, carry):
        block = stage_scatter([r1b[2 * q + k // 8, k % 8] for q in range(4)])
        for r in range(6):
            planes[r, pl.ds(pl.multiple_of(k * 16, 16), 16), :] = block[16 * r : 16 * r + 16]
        return carry

    lax.fori_loop(0, 16, scatter_step, 0)

    def plane_step(j, carry):
        rho = stage_density(planes[j], planes[3 + j], occ[0, 0], tyc, tx)
        part[j] = part[j] + stage_plane(rho, ry, rx)
        return carry

    lax.fori_loop(0, 3, plane_step, 0)

    other = 1 - cc
    f = copy(part.at[:, pl.ds(pl.multiple_of(other * 128, 128), 128)], r2a, at(c=other))
    f.wait()
    for j in range(3):
        total = part[j, pl.ds(pl.multiple_of(cc * 128, 128), 128)] + r2a[j]
        sums[j] = halves_for_wire(total).reshape(8, 16, 256)
    flights = [copy(sums.at[:, ring(cz, d, 8)], r2b.at[cz], at(z=ring(cz, d, 8))) for d in range(1, 8)]
    r2b[cz] = sums[:, cz]
    for f in flights:
        f.wait()
    acc = r2b[0].astype(F32)
    for z in range(1, 8):
        acc = acc + r2b[z].astype(F32)

    s3[...] = stage_pack(acc).reshape(8, 8, 128)
    flights = [copy(s3.at[ring(cy, d, 8)], r3a.at[cy], at(y=ring(cy, d, 8))) for d in range(1, 8)]
    r3a[cy] = s3[cy]
    for f in flights:
        f.wait()
    flights = [
        copy(r3a.at[:, pl.ds(ring(cx, d, 8), 1)], r3b.at[:, pl.ds(cx, 1)], at(x=ring(cx, d, 8))) for d in range(1, 8)
    ]
    r3b[:, pl.ds(cx, 1)] = r3a[:, pl.ds(cx, 1)]
    for f in flights:
        f.wait()
    out = stage_z(r3b[...].reshape(64, 128), qx[py * 16 + px], qy[band], qz[...], rz, hz, gz)

    for i in range(3):
        s4[:, i] = out[i].reshape(4, 16, 128)
    flights = [
        copy(s4.at[ring(py, d, 4)], r4a.at[py], at(y=2 * ring(py, d, 4) + lo)) for d in range(1, 4)
    ]
    r4a[py] = s4[py]
    for f in flights:
        f.wait()
    f = copy(r4a.at[:, :, pl.ds(pl.multiple_of(other * 8, 8), 8)], r4b.at[cc], at(c=other))
    r4b[cc] = r4a[:, :, pl.ds(pl.multiple_of(cc * 8, 8), 8)]
    f.wait()
    flights = [
        copy(r4b.at[:, :, :, pl.ds(ring(cz, d, 8), 1)], r4c.at[:, :, :, pl.ds(cz, 1)], at(z=ring(cz, d, 8)))
        for d in range(1, 8)
    ]
    r4c[:, :, :, pl.ds(cz, 1)] = r4b[:, :, :, pl.ds(cz, 1)]
    for f in flights:
        f.wait()
    x = [jnp.concatenate([r4c[0, q, i], r4c[1, q, i]], axis=0) for i in range(3) for q in range(4)]
    along, slope = stage_y(x, ryi)

    s5[:, :, 0] = along.astype(BF).reshape(2, 8, 16, 128)
    s5[:, :, 1] = slope.astype(BF).reshape(2, 8, 16, 128)
    f = copy(s5.at[1 - lo], r5a.at[lo], at(y=2 * py + 1 - lo))
    r5a[lo] = s5[lo]
    f.wait()
    flights = [copy(r5a.at[:, ring(cx, d, 8)], r5b.at[:, cx], at(x=ring(cx, d, 8))) for d in range(1, 8)]
    for q in range(2):
        r5b[q, cx] = r5a[q, cx]
    for f in flights:
        f.wait()
    wide[...] = r5b[...].astype(F32).reshape(512, 128)
    a = [wide[pl.ds(y, 16, stride=32), :] for y in range(12)]
    g = [wide[pl.ds(16 + y, 16, stride=32), :] for y in range(12)]
    rho, hart, gx, gy, gzz = stage_x(a, g, rxi)
    value = stage_potential(rho, hart, gx, gy, gzz)

    r6[cc, cz] = stage_block([value, gx, gy, gzz])
    flights = [copy(r6.at[cc, cz], r6.at[cc, cz], at(z=ring(cz, d, 8))) for d in range(1, 8)]
    last = [copy(r6.at[cc, cz], r6.at[cc, cz], at(c=other))]
    for d in range(1, 8):
        flights[d - 1].wait_recv()
        z = ring(cz, 8 - d, 8)
        last.append(copy(r6.at[cc, z], r6.at[cc, z], at(c=other)))
    for f in flights:
        f.wait_send()
    for f in last:
        f.wait()

    def lay(s, carry):
        v = r6[s // 8, s % 8].astype(F32)
        tail = roll(v, 64, 1)
        for k in range(4):
            half = (v, tail)[k % 2]
            for j in range(3):
                r, h = 40 * k + 12 * j, 160 + 40 * (k // 2) + 12 * j
                ref = pot.at[3 * s + j] if k == 0 else grad.at[k - 1, 3 * s + j]
                ref[:, 0:128] = v[r : r + 12]
                ref[:, 128:192] = half[h : h + 12, 0:64]
        return carry

    lax.fori_loop(0, 16, lay, 0)


def body(orbitals, occupations, stick_map, core_density):
    tables = make_tables()
    vmem = pl.BlockSpec(memory_space=pltpu.VMEM)
    scratch = [
        pltpu.VMEM((8, 8, 8, 128), BF),
        pltpu.VMEM((8, 8, 8, 128), BF),
        pltpu.VMEM((8, 8, 8, 128), BF),
        pltpu.VMEM((3, 12, N), F32),
        pltpu.VMEM((6, 256, 256), BF),
        pltpu.VMEM((3, 256, 256), F32),
        pltpu.VMEM((3, 128, 256), F32),
        pltpu.VMEM((3, 8, 16, 256), BF),
        pltpu.VMEM((8, 3, 16, 256), BF),
        pltpu.VMEM((8, 8, 128), F32),
        pltpu.VMEM((8, 8, 128), F32),
        pltpu.VMEM((8, 8, 128), F32),
        pltpu.VMEM((4, 3, 16, 128), F32),
        pltpu.VMEM((4, 3, 16, 128), F32),
        pltpu.VMEM((2, 4, 3, 8, 128), F32),
        pltpu.VMEM((2, 4, 3, 8, 128), F32),
        pltpu.VMEM((2, 8, 2, 16, 128), BF),
        pltpu.VMEM((2, 8, 2, 16, 128), BF),
        pltpu.VMEM((2, 8, 2, 16, 128), BF),
        pltpu.VMEM((512, 128), F32),
        pltpu.VMEM((2, 8, 240, 128), BF),
        pltpu.SemaphoreType.DMA((82,)),
        pltpu.SemaphoreType.DMA((82,)),
    ]
    return pl.pallas_call(
        kernel,
        out_shape=(
            jax.ShapeDtypeStruct((48, 12, N), F32),
            jax.ShapeDtypeStruct((3, 48, 12, N), F32),
        ),
        in_specs=[vmem, pl.BlockSpec(memory_space=pltpu.SMEM), vmem, pl.BlockSpec(memory_space=pl.ANY)]
        + [vmem] * len(tables),
        out_specs=(vmem, vmem),
        scratch_shapes=scratch,
        compiler_params=pltpu.CompilerParams(collective_id=0, has_side_effects=True, vmem_limit_bytes=60 * 1024 * 1024),
    )(orbitals[0], occupations.reshape(1, 1), stick_map, core_density, *tables)


def solution(mesh):
    return jax.shard_map(
        body,
        mesh=mesh,
        in_specs=(P("band", ("px", "py"), None), P("band"), P(None, "px"), P("py", "px", None)),
        out_specs=(P("py", "px", None), P(None, "py", "px", None)),
        check_vma=False,
    )
```

```python
import functools
import math

import jax
import jax.numpy as jnp
import numpy as np
from jax import lax
from jax.experimental import pallas as pl
from jax.experimental.pallas import tpu as pltpu
from jax.sharding import PartitionSpec as P

N = 192
SPACING = 0.25
KAPPA = 0.804
MU = 0.2195
SLATER = 0.75 * (3.0 / math.pi) ** (1.0 / 3.0)
REDUCED = 4.0 * (3.0 * math.pi**2) ** (2.0 / 3.0)
UNIT = 2.0 * math.pi / (N * SPACING)
F32 = jnp.float32
BF = jnp.bfloat16
MESH = pl.DeviceIdType.MESH
roll = pltpu.roll


def hilo(a):
    a = np.asarray(a, np.float32)
    hi = a.astype(BF)
    lo = (a - hi.astype(np.float32)).astype(BF)
    return np.stack([hi, lo])


def real_basis():
    n = np.arange(N)
    k = np.where(n <= 96, n, n - 96)
    cosine = n <= 96
    x = np.arange(N)
    angle = 2 * np.pi * (k[:, None] * x[None, :] % N) / N
    forward = np.where(cosine[:, None], np.cos(angle), np.sin(angle))
    weight = np.where((k == 0) | (k == 96), 1.0, 2.0)
    weight = np.where(cosine, weight, 2.0) / N
    inverse = (forward * weight[:, None]).T
    g = np.where(k == 96, 0.0, k) * UNIT
    slope = np.where(cosine[:, None], -np.sin(angle), np.cos(angle)) * (g * weight)[:, None]
    return forward, inverse, slope.T, (UNIT * k) ** 2


def make_tables():
    fwd, inv, dif, q2 = real_basis()
    idx = np.arange(N)
    ang = 2 * np.pi * (idx[:, None] * idx[None, :] % N) / N
    c, s = np.cos(ang), np.sin(ang)
    ta = np.zeros((64, 8, 384))
    for j in range(3):
        z = 3 * np.arange(64) + j
        ta[:, j, :N], ta[:, j, N:] = c[z], -s[z]
        ta[:, 3 + j, :N], ta[:, 3 + j, N:] = s[z], c[z]
    xp = 16 * (idx // 12) + idx % 12
    tyc = np.zeros((256, 512))
    tyc[xp, :N], tyc[xp, 256 : 256 + N] = c, s
    band = idx // 12
    krow = 128 * (band % 2) + 16 * (band // 2) + idx % 12
    ry = np.zeros((256, 256))
    ry[krow, :N] = fwd
    px, py, i = idx // 12, (idx % 12) // 3, idx % 3
    rx = np.zeros((N, 256))
    rx[:, 64 * i + 16 * py + px] = fwd.T
    rx[:, 192] = fwd[0]
    zo = (3 * np.arange(64)[None, :] + np.arange(3)[:, None]).reshape(-1)
    rz = fwd[:, zo]
    gz = (dif @ fwd)[zo][:, zo]
    kcol = 16 * (idx % 12) + 8 * (band % 2) + band // 2
    ryi = np.zeros((2, 256, N))
    ryi[0][np.ix_(xp, kcol)] = inv
    ryi[1][np.ix_(xp, kcol)] = dif
    kx = 16 * (4 * i + py) + px
    rxi = np.zeros((N, 512))
    rxi[kx, :N] = inv.T
    rxi[kx, 256 : 256 + N] = dif.T
    qx = np.zeros((64, 1, 128), np.float32)
    qy = np.zeros((16, 1, 128), np.float32)
    for ii in range(3):
        for t in range(12):
            p = np.arange(64)
            qx[:, 0, 12 * ii + t] = q2[12 * (p % 16) + 3 * (p // 16) + ii]
            qy[:, 0, 12 * ii + t] = q2[12 * np.arange(16) + t]
    tabs = [hilo(a) for a in (ta.reshape(512, 384), tyc, ry, rx, rz, gz, ryi, rxi)]
    return tabs + [qx, qy]


def mm(a, b):
    return lax.dot_general(a, b, (((1,), (0,)), ((), ())), preferred_element_type=F32)


def mmt(a, b):
    return lax.dot_general(a, b, (((1,), (1,)), ((), ())), preferred_element_type=F32)


def split(x):
    hi = x.astype(BF)
    return hi, (x - hi.astype(F32)).astype(BF)


def mtm(a, b):
    return lax.dot_general(a, b, (((0,), (0,)), ((), ())), preferred_element_type=F32)


def mm3(a, b, dot=mm):
    return dot(a[0], b[0]) + dot(a[0], b[1]) + dot(a[1], b[0])


def stage_columns(orb, x_of, y_of, px, ta):
    out = mmt(ta[0], orb) + mmt(ta[1], orb)
    row = lax.broadcasted_iota(jnp.int32, (8, 128), 0)
    y_row = y_of + 4 * (y_of // 12)
    place = jnp.where(row == 6, (x_of - px * 12).astype(F32), jnp.where(row == 7, y_row.astype(F32), 0.0))
    return (out.reshape(64, 8, 128) + place[None]).astype(BF)


def stage_scatter(pieces):
    data = jnp.concatenate(pieces, axis=1).astype(F32)
    hot = (lax.broadcasted_iota(jnp.int32, (256, 512), 0).astype(F32) == data[7:8]).astype(F32).astype(BF)
    place = lax.broadcasted_iota(jnp.int32, (16, 512), 0).astype(F32) == data[6:7]
    rows = jnp.concatenate([jnp.where(place, data[r : r + 1], 0.0) for r in range(6)], axis=0)
    return mmt(rows.astype(BF), hot).astype(BF)


def stage_density(p_re, p_im, weight, tyc, tx):
    a = mm(p_re, tyc[0]) + mm(p_re, tyc[1])
    b = mm(p_im, tyc[0]) + mm(p_im, tyc[1])
    y_re = (a[:, :256] - b[:, 256:]).astype(BF)
    y_im = (a[:, 256:] + b[:, :256]).astype(BF)
    a = mm(tx[0], y_re) + mm(tx[1], y_re)
    b = mm(tx[0], y_im) + mm(tx[1], y_im)
    re = a[:N] - b[256 : 256 + N]
    im = a[256 : 256 + N] + b[:N]
    return weight * (re * re + im * im)


def stage_plane(rho, ry, rx):
    t = mm3(ry, split(rho), mmt)
    return mm3(split(t), rx)


def stage_core(core, band, ry, rx):
    core = jnp.concatenate([core, jnp.zeros((4, N), F32)], axis=0)
    part = split(mm3(split(core), rx))
    y = lax.broadcasted_iota(jnp.int32, (256, 16), 0)
    t = lax.broadcasted_iota(jnp.int32, (256, 16), 1)
    pick = jnp.where((y == 12 * band + t) & (t < 12), 1.0, 0.0).astype(BF)
    placed = [mm(pick, h).astype(BF) for h in part]
    return mm3(ry, placed)


def halves_for_wire(x):
    lane = lax.broadcasted_iota(jnp.int32, x.shape, x.ndim - 1)
    return jnp.where(lane == 192, x - x.astype(BF).astype(F32), x).astype(BF)


def stage_pack(s):
    gap = jnp.zeros((24, 256), F32)
    rows = jnp.concatenate([s[0], gap, s[1], gap, s[2], gap, gap[:8]], axis=0)
    t = rows.T
    return t[0:64] + t[192:256] + roll(t[64:128], 12, 1) + roll(t[128:192], 24, 1)


def stage_z(w, qx, qy, rz, gz):
    lane = lax.broadcasted_iota(jnp.int32, (64, 128), 1)
    inside = lane < 36
    cols = jnp.concatenate([jnp.where(inside, w if j == 0 else roll(w, 128 - 40 * j, 1), 0.0) for j in range(3)], axis=0)
    both = split(cols)
    spectrum = mm3(rz, both)
    n = lax.broadcasted_iota(jnp.int32, (N, 128), 0)
    k = jnp.where(n <= 96, n, n - 96)
    weight = jnp.where((n == 0) | (n == 96), 1.0 / N, 2.0 / N)
    squared = UNIT**2 * (k * k).astype(F32) + (qx + qy)
    factor = jnp.where(squared > 0, 4.0 * math.pi / jnp.where(squared > 0, squared, 1.0), 0.0)
    hart = mm3(rz, split(spectrum * (factor * weight)), mtm)
    slope = mm3(gz, both)
    full = cols + roll(hart, 40, 1) + roll(slope, 80, 1)
    group = jnp.where(lane % 40 < 36, lane % 40 // 12, 9)
    out = []
    for i in range(3):
        acc = jnp.zeros((64, 128), F32)
        for j in range(3):
            shift = (12 * (j - i)) % 128
            part = full[64 * j : 64 * j + 64]
            acc = jnp.where(group == j, roll(part, shift, 1) if shift else part, acc)
        out.append(acc)
    return out


def swap_minor(x):
    lane = lax.broadcasted_iota(jnp.int32, (16, 128), 1)
    moved = [x[u] if u == 0 else roll(x[u], u, 1) for u in range(12)]
    out = []
    for v in range(12):
        at = lane - v
        at = jnp.where((at >= 0) & (at < 120) & (at % 40 < 36), at % 40 % 12, 99)
        acc = jnp.zeros((16, 128), F32)
        for u in range(12):
            acc = jnp.where(at == u, moved[u], acc)
        out.append(acc if v == 0 else roll(acc, 128 - v, 1))
    return out


def stage_y(x, ryi):
    cols = split(jnp.concatenate(swap_minor(x), axis=0))
    return mm3((ryi[0][0], ryi[1][0]), cols), mm3((ryi[0][1], ryi[1][1]), cols)


def stage_x(a, g, rxi):
    fill = jnp.zeros((64, 128), F32)
    f = jnp.concatenate(swap_minor(a) + [fill], axis=0).T[:, :N].astype(BF)
    s = jnp.concatenate(swap_minor(g) + [fill], axis=0).T[:, :N].astype(BF)
    both = mm(f, rxi[0]) + mm(f, rxi[1])
    gy = mm(s[0:64], rxi[0][:, :256]) + mm(s[0:64], rxi[1][:, :256])
    return both[0:40, :256], both[40:80, :256], both[0:40, 256:], gy[0:40], both[80:120, :256]


def stage_potential(rho, hart, gx, gy, gz):
    rho = jnp.where(rho > 0, rho, 1.0)
    cube_root = jnp.exp(jnp.log(rho) * (1.0 / 3.0))
    four = rho * cube_root
    reduced = (gx * gx + gy * gy + gz * gz) / (REDUCED * four * four)
    inverse = 1.0 / (1.0 + MU * reduced / KAPPA)
    enhance = 1.0 + KAPPA - KAPPA * inverse
    slope = MU * inverse * inverse
    return hart - SLATER * cube_root * ((4.0 / 3.0) * enhance - (8.0 / 3.0) * reduced * slope)


def stage_block(fields):
    lane = lax.broadcasted_iota(jnp.int32, (40, 128), 1)
    rows = [f[:, :128] for f in fields]
    for k in (0, 2):
        rows.append(jnp.where(lane < 64, fields[k][:, 128:], roll(fields[k + 1][:, 128:], 64, 1)))
    return jnp.concatenate(rows, axis=0).astype(BF)


def kernel(
    orb, occ, sticks, core, ta, tyc, ry, rx, rz, gz, ryi, rxi, qx, qy,
    r6,
    tx, s1, r1a, r1b, core_out, core_in, planes, part, r2a, sums, r2b, s3, r3a, r3b, s4, r4a, r4b, r4c,
    s5, r5a, r5b, wide, send, recv,
):
    band, px, py = lax.axis_index("band"), lax.axis_index("px"), lax.axis_index("py")
    cz, cc = band // 2, band % 2
    cx, lo = px % 8, px // 8
    cy = 2 * py + lo

    def at(z=None, c=None, x=None, y=None):
        z, c = cz if z is None else z, cc if c is None else c
        x, y = cx if x is None else x, cy if y is None else y
        return (z * 2 + c, (y % 2) * 8 + x, y // 2)

    open_scope = [None]

    def phase(name):
        if open_scope[0] is not None:
            open_scope[0].__exit__(None, None, None)
        open_scope[0] = jax.named_scope(name) if name else None
        if name:
            open_scope[0].__enter__()

    def ring(me, d, n):
        return lax.rem(me + d, n)

    bar = pltpu.get_barrier_semaphore()

    def hail(target):
        pl.semaphore_signal(bar, inc=1, device_id=target, device_id_type=MESH)

    swapped = (px, band, py)
    for d in range(1, 8):
        hail(at(x=ring(cx, d, 8)))
        hail(at(y=ring(cy, d, 8)))
        hail(at(z=ring(cz, d, 8)))
    hail(at(c=1 - cc))

    @pl.when(band != px)
    def _():
        hail(swapped)

    count = [0]

    def copy(src, dst, target):
        k = count[0]
        count[0] += 1
        c = pltpu.make_async_remote_copy(
            src_ref=src, dst_ref=dst, send_sem=send.at[k], recv_sem=recv.at[k],
            device_id=target, device_id_type=MESH,
        )
        c.start()
        return c

    phase("columns")
    mine = pl.ds(pl.multiple_of(py * 128, 128), 128)
    s1[...] = stage_columns(orb[...], sticks[0:1, mine], sticks[1:2, mine], px, ta).reshape(8, 8, 8, 128)
    for j in range(3):
        core_out[j] = core[:, pl.ds(3 * band + j, 1)].reshape(12, N)
    for h in range(2):
        tx[h] = tyc[h].astype(F32).T.astype(BF)
    phase("barrier")
    pl.semaphore_wait(bar, 22 + jnp.where(band != px, 1, 0))

    phase("e1_y")
    flights = [copy(s1.at[ring(cy, d, 8)], r1a.at[cy], at(y=ring(cy, d, 8))) for d in range(1, 8)]
    core_copy = pltpu.make_async_remote_copy(
        src_ref=core_out, dst_ref=core_in, send_sem=send.at[80], recv_sem=recv.at[80],
        device_id=swapped, device_id_type=MESH,
    )

    @pl.when(band != px)
    def _():
        core_copy.start()

    @pl.when(band == px)
    def _():
        core_in[...] = core_out[...]

    r1a[cy] = s1[cy]
    for f in flights:
        f.wait()
    phase("e1_x_core")
    flights = [copy(r1a.at[:, ring(cx, d, 8)], r1b.at[:, cx], at(x=ring(cx, d, 8))) for d in range(1, 8)]
    for y in range(8):
        r1b[y, cx] = r1a[y, cx]

    @pl.when(band != px)
    def _():
        core_copy.wait()

    def core_step(j, carry):
        part[j] = stage_core(core_in[j], band, ry, rx)
        return carry

    lax.fori_loop(0, 3, core_step, 0)
    phase("e1_x_wait")
    for f in flights:
        f.wait()

    phase("scatter")
    def scatter_step(k, carry):
        block = stage_scatter([r1b[2 * q + k // 8, k % 8] for q in range(4)])
        for r in range(6):
            planes[r, pl.ds(pl.multiple_of(k * 16, 16), 16), :] = block[16 * r : 16 * r + 16]
        return carry

    lax.fori_loop(0, 16, scatter_step, 0)

    phase("plane")

    def plane_step(j, carry):
        rho = stage_density(planes[j], planes[3 + j], occ[0, 0], tyc, tx)
        part[j] = part[j] + stage_plane(rho, ry, rx)
        return carry

    lax.fori_loop(0, 3, plane_step, 0)

    phase("e2_core")
    other = 1 - cc
    f = copy(part.at[:, pl.ds(pl.multiple_of(other * 128, 128), 128)], r2a, at(c=other))
    f.wait()
    for j in range(3):
        total = part[j, pl.ds(pl.multiple_of(cc * 128, 128), 128)] + r2a[j]
        sums[j] = halves_for_wire(total).reshape(8, 16, 256)
    phase("e2_z")
    flights = [copy(sums.at[:, ring(cz, d, 8)], r2b.at[cz], at(z=ring(cz, d, 8))) for d in range(1, 8)]
    r2b[cz] = sums[:, cz]
    for f in flights:
        f.wait()
    acc = r2b[0].astype(F32)
    for z in range(1, 8):
        acc = acc + r2b[z].astype(F32)

    phase("pack")
    s3[...] = stage_pack(acc).reshape(8, 8, 128)
    phase("e3_y")
    flights = [copy(s3.at[ring(cy, d, 8)], r3a.at[cy], at(y=ring(cy, d, 8))) for d in range(1, 8)]
    r3a[cy] = s3[cy]
    for f in flights:
        f.wait()
    phase("e3_x")
    flights = [
        copy(r3a.at[:, pl.ds(ring(cx, d, 8), 1)], r3b.at[:, pl.ds(cx, 1)], at(x=ring(cx, d, 8))) for d in range(1, 8)
    ]
    r3b[:, pl.ds(cx, 1)] = r3a[:, pl.ds(cx, 1)]
    for f in flights:
        f.wait()
    phase("z")
    out = stage_z(r3b[...].reshape(64, 128), qx[py * 16 + px], qy[band], rz, gz)

    for i in range(3):
        s4[:, i] = out[i].reshape(4, 16, 128)
    phase("e4_y")
    flights = [
        copy(s4.at[ring(py, d, 4)], r4a.at[py], at(y=2 * ring(py, d, 4) + lo)) for d in range(1, 4)
    ]
    r4a[py] = s4[py]
    for f in flights:
        f.wait()
    phase("e4_core")
    f = copy(r4a.at[:, :, pl.ds(pl.multiple_of(other * 8, 8), 8)], r4b.at[cc], at(c=other))
    r4b[cc] = r4a[:, :, pl.ds(pl.multiple_of(cc * 8, 8), 8)]
    f.wait()
    phase("e4_z")
    flights = [
        copy(r4b.at[:, :, :, pl.ds(ring(cz, d, 8), 1)], r4c.at[:, :, :, pl.ds(cz, 1)], at(z=ring(cz, d, 8)))
        for d in range(1, 8)
    ]
    r4c[:, :, :, pl.ds(cz, 1)] = r4b[:, :, :, pl.ds(cz, 1)]
    for f in flights:
        f.wait()
    phase("y")
    x = [jnp.concatenate([r4c[0, q, i], r4c[1, q, i]], axis=0) for i in range(3) for q in range(4)]
    along, slope = stage_y(x, ryi)

    s5[:, :, 0] = along.astype(BF).reshape(2, 8, 16, 128)
    s5[:, :, 1] = slope.astype(BF).reshape(2, 8, 16, 128)
    phase("e5_y")
    f = copy(s5.at[1 - lo], r5a.at[lo], at(y=2 * py + 1 - lo))
    r5a[lo] = s5[lo]
    f.wait()
    phase("e5_x")
    flights = [copy(r5a.at[:, ring(cx, d, 8)], r5b.at[:, cx], at(x=ring(cx, d, 8))) for d in range(1, 8)]
    for q in range(2):
        r5b[q, cx] = r5a[q, cx]
    for f in flights:
        f.wait()
    phase("x")
    wide[...] = r5b[...].astype(F32).reshape(512, 128)
    a = [wide[pl.ds(y, 16, stride=32), :] for y in range(12)]
    g = [wide[pl.ds(16 + y, 16, stride=32), :] for y in range(12)]
    rho, hart, gx, gy, gzz = stage_x(a, g, rxi)
    value = stage_potential(rho, hart, gx, gy, gzz)

    r6[cc, cz] = stage_block([value, gx, gy, gzz])
    phase("e6")
    flights = [copy(r6.at[cc, cz], r6.at[cc, cz], at(z=ring(cz, d, 8))) for d in range(1, 8)]
    last = [copy(r6.at[cc, cz], r6.at[cc, cz], at(c=other))]
    for d in range(1, 8):
        flights[d - 1].wait_recv()
        z = ring(cz, 8 - d, 8)
        last.append(copy(r6.at[cc, z], r6.at[cc, z], at(c=other)))
    for f in flights:
        f.wait_send()
    for f in last:
        f.wait()
    phase(None)


def lay_kernel(r6, pot, grad, wide, woven):
    wide[...] = r6[...].astype(F32).reshape(3840, 128)

    def step(y, carry):
        for k in range(4):
            ref = pot.at[y] if k == 0 else grad.at[k - 1, y]
            for j in range(3):
                z = pl.ds(j, 16, stride=3)
                woven[k, 0, z] = wide[pl.ds(40 * k + 12 * j + y, 16, stride=240), :]
                tail = wide[pl.ds(160 + 40 * (k // 2) + 12 * j + y, 16, stride=240), :]
                woven[k, 1, z] = roll(tail, 64, 1) if k % 2 else tail
            ref[:, 0:128] = woven[k, 0]
            ref[:, 128:192] = woven[k, 1, :, 0:64]
        return carry

    lax.fori_loop(0, 12, step, 0)


def body(orbitals, occupations, stick_map, core_density):
    tables = make_tables()
    vmem = pl.BlockSpec(memory_space=pltpu.VMEM)
    scratch = [
        pltpu.VMEM((2, 512, 256), BF),
        pltpu.VMEM((8, 8, 8, 128), BF),
        pltpu.VMEM((8, 8, 8, 128), BF),
        pltpu.VMEM((8, 8, 8, 128), BF),
        pltpu.VMEM((3, 12, N), F32),
        pltpu.VMEM((3, 12, N), F32),
        pltpu.VMEM((6, 256, 256), BF),
        pltpu.VMEM((3, 256, 256), F32),
        pltpu.VMEM((3, 128, 256), F32),
        pltpu.VMEM((3, 8, 16, 256), BF),
        pltpu.VMEM((8, 3, 16, 256), BF),
        pltpu.VMEM((8, 8, 128), F32),
        pltpu.VMEM((8, 8, 128), F32),
        pltpu.VMEM((8, 8, 128), F32),
        pltpu.VMEM((4, 3, 16, 128), F32),
        pltpu.VMEM((4, 3, 16, 128), F32),
        pltpu.VMEM((2, 4, 3, 8, 128), F32),
        pltpu.VMEM((2, 4, 3, 8, 128), F32),
        pltpu.VMEM((2, 8, 2, 16, 128), BF),
        pltpu.VMEM((2, 8, 2, 16, 128), BF),
        pltpu.VMEM((2, 8, 2, 16, 128), BF),
        pltpu.VMEM((512, 128), F32),
        pltpu.SemaphoreType.DMA((82,)),
        pltpu.SemaphoreType.DMA((82,)),
    ]
    blocks = pl.pallas_call(
        kernel,
        out_shape=jax.ShapeDtypeStruct((2, 8, 240, 128), BF),
        in_specs=[vmem, pl.BlockSpec(memory_space=pltpu.SMEM), vmem, vmem]
        + [vmem] * len(tables),
        out_specs=vmem,
        scratch_shapes=scratch,
        compiler_params=pltpu.CompilerParams(collective_id=0, has_side_effects=True, vmem_limit_bytes=40 * 1024 * 1024),
    )(orbitals[0], occupations.reshape(1, 1), stick_map, core_density.transpose(1, 0, 2), *tables)
    pot, grad = pl.pallas_call(
        lay_kernel,
        out_shape=(
            jax.ShapeDtypeStruct((12, 48, N), F32),
            jax.ShapeDtypeStruct((3, 12, 48, N), F32),
        ),
        in_specs=[vmem],
        out_specs=(vmem, vmem),
        scratch_shapes=[pltpu.VMEM((3840, 128), F32), pltpu.VMEM((4, 2, 48, 128), F32)],
        compiler_params=pltpu.CompilerParams(vmem_limit_bytes=20 * 1024 * 1024),
    )(blocks)
    return pot.transpose(1, 0, 2), grad.transpose(0, 2, 1, 3)


def solution(mesh):
    return jax.shard_map(
        body,
        mesh=mesh,
        in_specs=(P("band", ("px", "py"), None), P("band"), P(None, "px"), P("py", "px", None)),
        out_specs=(P("py", "px", None), P(None, "py", "px", None)),
        check_vma=False,
    )
```

```python
import functools
import math

import jax
import jax.numpy as jnp
import numpy as np
from jax import lax
from jax.experimental import pallas as pl
from jax.experimental.pallas import tpu as pltpu
from jax.sharding import PartitionSpec as P

N = 192
SPACING = 0.25
KAPPA = 0.804
MU = 0.2195
SLATER = 0.75 * (3.0 / math.pi) ** (1.0 / 3.0)
REDUCED = 4.0 * (3.0 * math.pi**2) ** (2.0 / 3.0)
UNIT = 2.0 * math.pi / (N * SPACING)
F32 = jnp.float32
BF = jnp.bfloat16
MESH = pl.DeviceIdType.MESH
roll = pltpu.roll


def hilo(a):
    a = np.asarray(a, np.float32)
    hi = a.astype(BF)
    lo = (a - hi.astype(np.float32)).astype(BF)
    return np.stack([hi, lo])


def real_basis():
    n = np.arange(N)
    k = np.where(n <= 96, n, n - 96)
    cosine = n <= 96
    x = np.arange(N)
    angle = 2 * np.pi * (k[:, None] * x[None, :] % N) / N
    forward = np.where(cosine[:, None], np.cos(angle), np.sin(angle))
    weight = np.where((k == 0) | (k == 96), 1.0, 2.0)
    weight = np.where(cosine, weight, 2.0) / N
    inverse = (forward * weight[:, None]).T
    g = np.where(k == 96, 0.0, k) * UNIT
    slope = np.where(cosine[:, None], -np.sin(angle), np.cos(angle)) * (g * weight)[:, None]
    return forward, inverse, slope.T, (UNIT * k) ** 2


def make_tables():
    fwd, inv, dif, q2 = real_basis()
    idx = np.arange(N)
    ang = 2 * np.pi * (idx[:, None] * idx[None, :] % N) / N
    c, s = np.cos(ang), np.sin(ang)
    ta = np.zeros((64, 8, 384))
    for j in range(3):
        z = 3 * np.arange(64) + j
        ta[:, j, :N], ta[:, j, N:] = c[z], -s[z]
        ta[:, 3 + j, :N], ta[:, 3 + j, N:] = s[z], c[z]
    xp = 16 * (idx // 12) + idx % 12
    tyc = np.zeros((256, 512))
    tyc[xp, :N], tyc[xp, 256 : 256 + N] = c, s
    band = idx // 12
    krow = 128 * (band % 2) + 16 * (band // 2) + idx % 12
    ry = np.zeros((256, 256))
    ry[krow, :N] = fwd
    px, py, i = idx // 12, (idx % 12) // 3, idx % 3
    rx = np.zeros((N, 256))
    rx[:, 64 * i + 16 * py + px] = fwd.T
    rx[:, 192] = fwd[0]
    zo = (3 * np.arange(64)[None, :] + np.arange(3)[:, None]).reshape(-1)
    rz = fwd[:, zo]
    gz = (dif @ fwd)[zo][:, zo]
    kcol = 16 * (idx % 12) + 8 * (band % 2) + band // 2
    ryi = np.zeros((2, 256, N))
    ryi[0][np.ix_(xp, kcol)] = inv
    ryi[1][np.ix_(xp, kcol)] = dif
    kx = 16 * (4 * i + py) + px
    rxi = np.zeros((N, 512))
    rxi[kx, :N] = inv.T
    rxi[kx, 256 : 256 + N] = dif.T
    qx = np.zeros((64, 1, 128), np.float32)
    qy = np.zeros((16, 1, 128), np.float32)
    for ii in range(3):
        for t in range(12):
            p = np.arange(64)
            qx[:, 0, 12 * ii + t] = q2[12 * (p % 16) + 3 * (p // 16) + ii]
            qy[:, 0, 12 * ii + t] = q2[12 * np.arange(16) + t]
    tabs = [hilo(a) for a in (ta.reshape(512, 384), tyc, ry, rx, rz, gz, ryi, rxi)]
    return tabs + [qx, qy]


def mm(a, b):
    return lax.dot_general(a, b, (((1,), (0,)), ((), ())), preferred_element_type=F32)


def mmt(a, b):
    return lax.dot_general(a, b, (((1,), (1,)), ((), ())), preferred_element_type=F32)


def split(x):
    hi = x.astype(BF)
    return hi, (x - hi.astype(F32)).astype(BF)


def mtm(a, b):
    return lax.dot_general(a, b, (((0,), (0,)), ((), ())), preferred_element_type=F32)


def mm3(a, b, dot=mm):
    return dot(a[0], b[0]) + dot(a[0], b[1]) + dot(a[1], b[0])


def stage_columns(orb, x_of, y_of, px, ta):
    out = mmt(ta[0], orb) + mmt(ta[1], orb)
    row = lax.broadcasted_iota(jnp.int32, (8, 128), 0)
    y_row = y_of + 4 * (y_of // 12)
    place = jnp.where(row == 6, (x_of - px * 12).astype(F32), jnp.where(row == 7, y_row.astype(F32), 0.0))
    return (out.reshape(64, 8, 128) + place[None]).astype(BF)


def stage_scatter(pieces):
    data = jnp.concatenate(pieces, axis=1).astype(F32)
    hot = (lax.broadcasted_iota(jnp.int32, (256, 512), 0).astype(F32) == data[7:8]).astype(F32).astype(BF)
    place = lax.broadcasted_iota(jnp.int32, (16, 512), 0).astype(F32) == data[6:7]
    rows = jnp.concatenate([jnp.where(place, data[r : r + 1], 0.0) for r in range(6)], axis=0)
    return mmt(rows.astype(BF), hot).astype(BF)


def stage_density(p_re, p_im, weight, tyc, tx):
    a = mm(p_re, tyc[0]) + mm(p_re, tyc[1])
    b = mm(p_im, tyc[0]) + mm(p_im, tyc[1])
    y_re = (a[:, :256] - b[:, 256:]).astype(BF)
    y_im = (a[:, 256:] + b[:, :256]).astype(BF)
    a = mm(tx[0], y_re) + mm(tx[1], y_re)
    b = mm(tx[0], y_im) + mm(tx[1], y_im)
    re = a[:N] - b[256 : 256 + N]
    im = a[256 : 256 + N] + b[:N]
    return weight * (re * re + im * im)


def stage_plane(rho, ry, rx):
    t = mm3(ry, split(rho), mmt)
    return mm3(split(t), rx)


def stage_core(core, band, ry, rx):
    core = jnp.concatenate([core, jnp.zeros((4, N), F32)], axis=0)
    part = split(mm3(split(core), rx))
    y = lax.broadcasted_iota(jnp.int32, (256, 16), 0)
    t = lax.broadcasted_iota(jnp.int32, (256, 16), 1)
    pick = jnp.where((y == 12 * band + t) & (t < 12), 1.0, 0.0).astype(BF)
    placed = [mm(pick, h).astype(BF) for h in part]
    return mm3(ry, placed)


def halves_for_wire(x):
    lane = lax.broadcasted_iota(jnp.int32, x.shape, x.ndim - 1)
    return jnp.where(lane == 192, x - x.astype(BF).astype(F32), x).astype(BF)


def stage_pack(s):
    gap = jnp.zeros((24, 256), F32)
    rows = jnp.concatenate([s[0], gap, s[1], gap, s[2], gap, gap[:8]], axis=0)
    t = rows.T
    return t[0:64] + t[192:256] + roll(t[64:128], 12, 1) + roll(t[128:192], 24, 1)


def stage_z(w, qx, qy, rz, gz):
    lane = lax.broadcasted_iota(jnp.int32, (64, 128), 1)
    inside = lane < 36
    cols = jnp.concatenate([jnp.where(inside, w if j == 0 else roll(w, 128 - 40 * j, 1), 0.0) for j in range(3)], axis=0)
    both = split(cols)
    spectrum = mm3(rz, both)
    n = lax.broadcasted_iota(jnp.int32, (N, 128), 0)
    k = jnp.where(n <= 96, n, n - 96)
    weight = jnp.where((n == 0) | (n == 96), 1.0 / N, 2.0 / N)
    squared = UNIT**2 * (k * k).astype(F32) + (qx + qy)
    factor = jnp.where(squared > 0, 4.0 * math.pi / jnp.where(squared > 0, squared, 1.0), 0.0)
    hart = mm3(rz, split(spectrum * (factor * weight)), mtm)
    slope = mm3(gz, both)
    full = cols + roll(hart, 40, 1) + roll(slope, 80, 1)
    group = jnp.where(lane % 40 < 36, lane % 40 // 12, 9)
    out = []
    for i in range(3):
        acc = jnp.zeros((64, 128), F32)
        for j in range(3):
            shift = (12 * (j - i)) % 128
            part = full[64 * j : 64 * j + 64]
            acc = jnp.where(group == j, roll(part, shift, 1) if shift else part, acc)
        out.append(acc)
    return out


def swap_minor(x):
    lane = lax.broadcasted_iota(jnp.int32, (16, 128), 1)
    moved = [x[u] if u == 0 else roll(x[u], u, 1) for u in range(12)]
    out = []
    for v in range(12):
        at = lane - v
        at = jnp.where((at >= 0) & (at < 120) & (at % 40 < 36), at % 40 % 12, 99)
        acc = jnp.zeros((16, 128), F32)
        for u in range(12):
            acc = jnp.where(at == u, moved[u], acc)
        out.append(acc if v == 0 else roll(acc, 128 - v, 1))
    return out


def stage_y(x, ryi):
    cols = split(jnp.concatenate(swap_minor(x), axis=0))
    return mm3((ryi[0][0], ryi[1][0]), cols), mm3((ryi[0][1], ryi[1][1]), cols)


def stage_x(a, g, rxi):
    fill = jnp.zeros((64, 128), F32)
    f = jnp.concatenate(swap_minor(a) + [fill], axis=0).T[:, :N].astype(BF)
    s = jnp.concatenate(swap_minor(g) + [fill], axis=0).T[:, :N].astype(BF)
    both = mm(f, rxi[0]) + mm(f, rxi[1])
    gy = mm(s[0:64], rxi[0][:, :256]) + mm(s[0:64], rxi[1][:, :256])
    return both[0:40, :256], both[40:80, :256], both[0:40, 256:], gy[0:40], both[80:120, :256]


def stage_potential(rho, hart, gx, gy, gz):
    rho = jnp.where(rho > 0, rho, 1.0)
    cube_root = jnp.exp(jnp.log(rho) * (1.0 / 3.0))
    four = rho * cube_root
    reduced = (gx * gx + gy * gy + gz * gz) / (REDUCED * four * four)
    inverse = 1.0 / (1.0 + MU * reduced / KAPPA)
    enhance = 1.0 + KAPPA - KAPPA * inverse
    slope = MU * inverse * inverse
    return hart - SLATER * cube_root * ((4.0 / 3.0) * enhance - (8.0 / 3.0) * reduced * slope)


def stage_block(fields):
    lane = lax.broadcasted_iota(jnp.int32, (40, 128), 1)
    rows = [f[:, :128] for f in fields]
    for k in (0, 2):
        rows.append(jnp.where(lane < 64, fields[k][:, 128:], roll(fields[k + 1][:, 128:], 64, 1)))
    return jnp.concatenate(rows, axis=0).astype(BF)


def kernel(
    occ, *rest,
):
    far, rest = rest[:13], rest[13:]
    r6, near, rest = rest[0], rest[1:14], rest[14:]
    orb, sticks, core, ta, tyc, ry, rx, rz, gz, ryi, rxi, qx, qy = near
    (
    tx, s1, r1a, r1b, core_out, core_in, planes, part, r2a, sums, r2b, s3, r3a, r3b, s4, r4a, r4c,
    s5, r5b, wide, send, recv, load,
    ) = rest
    band, px, py = lax.axis_index("band"), lax.axis_index("px"), lax.axis_index("py")
    cz, cc = band // 2, band % 2
    cx, lo = px % 8, px // 8
    cy = 2 * py + lo

    def at(z=None, c=None, x=None, y=None):
        z, c = cz if z is None else z, cc if c is None else c
        x, y = cx if x is None else x, cy if y is None else y
        return (z * 2 + c, (y % 2) * 8 + x, y // 2)

    open_scope = [None]

    def phase(name):
        if open_scope[0] is not None:
            open_scope[0].__exit__(None, None, None)
        open_scope[0] = jax.named_scope(name) if name else None
        if name:
            open_scope[0].__enter__()

    def ring(me, d, n):
        return lax.rem(me + d, n)

    bar = pltpu.get_barrier_semaphore()

    def hail(target):
        pl.semaphore_signal(bar, inc=1, device_id=target, device_id_type=MESH)

    swapped = (px, band, py)
    for d in range(1, 8):
        hail(at(x=ring(cx, d, 8)))
        hail(at(y=ring(cy, d, 8)))
        hail(at(z=ring(cz, d, 8)))
        hail(at(z=ring(cz, d, 8), c=1 - cc))
        hail(at(x=ring(cx, d, 8), y=2 * py + 1 - lo))
    hail(at(c=1 - cc))

    @pl.when(band != px)
    def _():
        hail(swapped)

    loads = {}
    for k in (0, 1, 3, 2, 4, 5, 6, 7, 8, 9, 10, 11, 12):
        loads[k] = pltpu.make_async_copy(far[k], near[k], load.at[k])
        loads[k].start()
    count = [0]

    def copy(src, dst, target):
        k = count[0]
        count[0] += 1
        c = pltpu.make_async_remote_copy(
            src_ref=src, dst_ref=dst, send_sem=send.at[k], recv_sem=recv.at[k],
            device_id=target, device_id_type=MESH,
        )
        c.start()
        return c

    phase("columns")
    for k in (0, 1, 3):
        loads[k].wait()
    mine = pl.ds(pl.multiple_of(py * 128, 128), 128)
    s1[...] = stage_columns(orb[...], sticks[0:1, mine], sticks[1:2, mine], px, ta).reshape(8, 8, 8, 128)
    for k in (2, 4, 5, 6):
        loads[k].wait()
    for j in range(3):
        core_out[j] = core[:, pl.ds(3 * band + j, 1)].reshape(12, N)
    for h in range(2):
        tx[h] = tyc[h].astype(F32).T.astype(BF)
    phase("barrier")
    pl.semaphore_wait(bar, 36 + jnp.where(band != px, 1, 0))

    phase("e1_y")
    flights = [copy(s1.at[ring(cy, d, 8)], r1a.at[cy], at(y=ring(cy, d, 8))) for d in range(1, 8)]
    core_copy = pltpu.make_async_remote_copy(
        src_ref=core_out, dst_ref=core_in, send_sem=send.at[99], recv_sem=recv.at[99],
        device_id=swapped, device_id_type=MESH,
    )

    @pl.when(band != px)
    def _():
        core_copy.start()

    @pl.when(band == px)
    def _():
        core_in[...] = core_out[...]

    r1a[cy] = s1[cy]
    for f in flights:
        f.wait()
    phase("e1_x_core")
    flights = [copy(r1a.at[:, ring(cx, d, 8)], r1b.at[:, cx], at(x=ring(cx, d, 8))) for d in range(1, 8)]
    for y in range(8):
        r1b[y, cx] = r1a[y, cx]

    @pl.when(band != px)
    def _():
        core_copy.wait()

    def core_step(j, carry):
        part[j] = stage_core(core_in[j], band, ry, rx)
        return carry

    lax.fori_loop(0, 3, core_step, 0)
    phase("e1_x_wait")
    for f in flights:
        f.wait()

    phase("scatter")
    def scatter_step(k, carry):
        block = stage_scatter([r1b[2 * q + k // 8, k % 8] for q in range(4)])
        for r in range(6):
            planes[r, pl.ds(pl.multiple_of(k * 16, 16), 16), :] = block[16 * r : 16 * r + 16]
        return carry

    lax.fori_loop(0, 16, scatter_step, 0, unroll=2)

    phase("plane")

    def plane_step(j, carry):
        rho = stage_density(planes[j], planes[3 + j], occ[0], tyc, tx)
        part[j] = part[j] + stage_plane(rho, ry, rx)
        return carry

    lax.fori_loop(0, 3, plane_step, 0)

    phase("e2_core")
    other = 1 - cc
    f = copy(part.at[:, pl.ds(pl.multiple_of(other * 128, 128), 128)], r2a, at(c=other))
    f.wait()
    for j in range(3):
        total = part[j, pl.ds(pl.multiple_of(cc * 128, 128), 128)] + r2a[j]
        sums[j] = halves_for_wire(total).reshape(8, 16, 256)
    phase("e2_z")
    flights = [copy(sums.at[:, ring(cz, d, 8)], r2b.at[cz], at(z=ring(cz, d, 8))) for d in range(1, 8)]
    r2b[cz] = sums[:, cz]
    for f in flights:
        f.wait()
    acc = r2b[0].astype(F32)
    for z in range(1, 8):
        acc = acc + r2b[z].astype(F32)

    phase("pack")
    s3[...] = stage_pack(acc).reshape(8, 8, 128)
    phase("e3_y")
    flights = [copy(s3.at[ring(cy, d, 8)], r3a.at[cy], at(y=ring(cy, d, 8))) for d in range(1, 8)]
    r3a[cy] = s3[cy]
    for f in flights:
        f.wait()
    phase("e3_x")
    flights = [
        copy(r3a.at[:, pl.ds(ring(cx, d, 8), 1)], r3b.at[:, pl.ds(cx, 1)], at(x=ring(cx, d, 8))) for d in range(1, 8)
    ]
    r3b[:, pl.ds(cx, 1)] = r3a[:, pl.ds(cx, 1)]
    for f in flights:
        f.wait()
    phase("z")
    for k in (7, 8, 9, 10, 11, 12):
        loads[k].wait()
    out = stage_z(r3b[...].reshape(64, 128), qx[py * 16 + px], qy[band], rz, gz)

    for i in range(3):
        s4[:, i] = out[i].reshape(4, 16, 128)
    phase("e4_y")
    flights = [
        copy(s4.at[ring(py, d, 4)], r4a.at[py], at(y=2 * ring(py, d, 4) + lo)) for d in range(1, 4)
    ]
    r4a[py] = s4[py]
    for f in flights:
        f.wait()
    phase("e4_z")
    flights = []
    for d in range(15, 0, -1):
        z, c = ring(cz, d // 2, 8), lax.rem(cc + d % 2, 2)
        rows = r4a.at[:, :, pl.ds(c * 8 + z, 1)]
        flights.append(copy(rows, r4c.at[cc, :, :, pl.ds(cz, 1)], at(z=z, c=c)))
    r4c[cc, :, :, pl.ds(cz, 1)] = r4a[:, :, pl.ds(cc * 8 + cz, 1)]
    for f in flights:
        f.wait()
    phase("y")
    x = [jnp.concatenate([r4c[0, q, i], r4c[1, q, i]], axis=0) for i in range(3) for q in range(4)]
    along, slope = stage_y(x, ryi)

    s5[:, :, 0] = along.astype(BF).reshape(2, 8, 16, 128)
    s5[:, :, 1] = slope.astype(BF).reshape(2, 8, 16, 128)
    phase("e5")
    flights = []
    for d in range(15, 0, -1):
        to_x, to_lo = ring(cx, d // 2, 8), lax.rem(lo + d % 2, 2)
        flights.append(copy(s5.at[to_lo, to_x], r5b.at[lo, cx], at(x=to_x, y=2 * py + to_lo)))
    r5b[lo, cx] = s5[lo, cx]
    for f in flights:
        f.wait()
    phase("x")
    wide[...] = r5b[...].astype(F32).reshape(512, 128)
    a = [wide[pl.ds(y, 16, stride=32), :] for y in range(12)]
    g = [wide[pl.ds(16 + y, 16, stride=32), :] for y in range(12)]
    rho, hart, gx, gy, gzz = stage_x(a, g, rxi)
    value = stage_potential(rho, hart, gx, gy, gzz)

    r6[cc, cz] = stage_block([value, gx, gy, gzz])
    phase("e6")
    mine = r6.at[cc, cz]
    hops = {d: copy(mine, mine, at(z=ring(cz, d % 8, 8))) for d in (2, -2, 1, -1)}
    last = [copy(mine, mine, at(c=other))]
    relays = {}
    cut = {1: pl.ds(0, 128), -1: pl.ds(128, 112)}
    for way in (1, -1):
        hops[2 * way].wait_recv()
        got = r6.at[cc, ring(cz, -2 * way % 8, 8)]
        relays[3 * way] = copy(got, got, at(z=ring(cz, way % 8, 8)))
        part4 = got.at[cut[way]]
        relays[4 * way] = copy(part4, part4, at(z=ring(cz, 2 * way % 8, 8)))
        last.append(copy(got, got, at(c=other)))
    for way in (1, -1):
        hops[way].wait_recv()
        got = r6.at[cc, ring(cz, -way % 8, 8)]
        last.append(copy(got, got, at(c=other)))
    for way in (1, -1):
        relays[3 * way].wait_recv()
        got = r6.at[cc, ring(cz, -3 * way % 8, 8)]
        last.append(copy(got, got, at(c=other)))
    for way in (1, -1):
        relays[4 * way].wait_recv()
    got = r6.at[cc, ring(cz, 4, 8)]
    last.append(copy(got, got, at(c=other)))
    for f in list(hops.values()) + list(relays.values()):
        f.wait_send()
    for f in last:
        f.wait()
    phase(None)


def lay_kernel(r6, pot, grad, wide, woven):
    wide[...] = r6[...].astype(F32).reshape(3840, 128)

    def step(y, carry):
        for k in range(4):
            ref = pot.at[y] if k == 0 else grad.at[k - 1, y]
            for j in range(3):
                z = pl.ds(j, 16, stride=3)
                woven[k, 0, z] = wide[pl.ds(40 * k + 12 * j + y, 16, stride=240), :]
                tail = wide[pl.ds(160 + 40 * (k // 2) + 12 * j + y, 16, stride=240), :]
                woven[k, 1, z] = roll(tail, 64, 1) if k % 2 else tail
            ref[:, 0:128] = woven[k, 0]
            ref[:, 128:192] = woven[k, 1, :, 0:64]
        return carry

    lax.fori_loop(0, 12, step, 0)


def body(orbitals, occupations, stick_map, core_density):
    tables = make_tables()
    vmem = pl.BlockSpec(memory_space=pltpu.VMEM)
    operands = [orbitals[0], stick_map, core_density.transpose(1, 0, 2), *tables]
    scratch = [pltpu.VMEM(a.shape, a.dtype) for a in operands] + [
        pltpu.VMEM((2, 512, 256), BF),
        pltpu.VMEM((8, 8, 8, 128), BF),
        pltpu.VMEM((8, 8, 8, 128), BF),
        pltpu.VMEM((8, 8, 8, 128), BF),
        pltpu.VMEM((3, 12, N), F32),
        pltpu.VMEM((3, 12, N), F32),
        pltpu.VMEM((6, 256, 256), BF),
        pltpu.VMEM((3, 256, 256), F32),
        pltpu.VMEM((3, 128, 256), F32),
        pltpu.VMEM((3, 8, 16, 256), BF),
        pltpu.VMEM((8, 3, 16, 256), BF),
        pltpu.VMEM((8, 8, 128), F32),
        pltpu.VMEM((8, 8, 128), F32),
        pltpu.VMEM((8, 8, 128), F32),
        pltpu.VMEM((4, 3, 16, 128), F32),
        pltpu.VMEM((4, 3, 16, 128), F32),
        pltpu.VMEM((2, 4, 3, 8, 128), F32),
        pltpu.VMEM((2, 8, 2, 16, 128), BF),
        pltpu.VMEM((2, 8, 2, 16, 128), BF),
        pltpu.VMEM((512, 128), F32),
        pltpu.SemaphoreType.DMA((100,)),
        pltpu.SemaphoreType.DMA((100,)),
        pltpu.SemaphoreType.DMA((13,)),
    ]
    blocks = pl.pallas_call(
        kernel,
        out_shape=jax.ShapeDtypeStruct((2, 8, 240, 128), BF),
        in_specs=[pl.BlockSpec(memory_space=pltpu.SMEM)] + [pl.BlockSpec(memory_space=pltpu.HBM)] * len(operands),
        out_specs=vmem,
        scratch_shapes=scratch,
        compiler_params=pltpu.CompilerParams(collective_id=0, has_side_effects=True, vmem_limit_bytes=67_043_328),
    )(occupations, *operands)
    pot, grad = pl.pallas_call(
        lay_kernel,
        out_shape=(
            jax.ShapeDtypeStruct((12, 48, N), F32),
            jax.ShapeDtypeStruct((3, 12, 48, N), F32),
        ),
        in_specs=[vmem],
        out_specs=(vmem, vmem),
        scratch_shapes=[pltpu.VMEM((3840, 128), F32), pltpu.VMEM((4, 2, 48, 128), F32)],
        compiler_params=pltpu.CompilerParams(vmem_limit_bytes=20 * 1024 * 1024),
    )(blocks)
    return pot.transpose(1, 0, 2), grad.transpose(0, 2, 1, 3)


def solution(mesh):
    return jax.shard_map(
        body,
        mesh=mesh,
        in_specs=(P("band", ("px", "py"), None), P("band"), P(None, "px"), P("py", "px", None)),
        out_specs=(P("py", "px", None), P(None, "py", "px", None)),
        check_vma=False,
    )
```

```python
import functools
import math

import jax
import jax.numpy as jnp
import numpy as np
from jax import lax
from jax.experimental import pallas as pl
from jax.experimental.pallas import tpu as pltpu
from jax.sharding import PartitionSpec as P

N = 192
SPACING = 0.25
KAPPA = 0.804
MU = 0.2195
SLATER = 0.75 * (3.0 / math.pi) ** (1.0 / 3.0)
REDUCED = 4.0 * (3.0 * math.pi**2) ** (2.0 / 3.0)
UNIT = 2.0 * math.pi / (N * SPACING)
F32 = jnp.float32
BF = jnp.bfloat16
MESH = pl.DeviceIdType.MESH
roll = pltpu.roll


def hilo(a):
    a = np.asarray(a, np.float32)
    hi = a.astype(BF)
    lo = (a - hi.astype(np.float32)).astype(BF)
    return np.stack([hi, lo])


def real_basis():
    n = np.arange(N)
    k = np.where(n <= 96, n, n - 96)
    cosine = n <= 96
    x = np.arange(N)
    angle = 2 * np.pi * (k[:, None] * x[None, :] % N) / N
    forward = np.where(cosine[:, None], np.cos(angle), np.sin(angle))
    weight = np.where((k == 0) | (k == 96), 1.0, 2.0)
    weight = np.where(cosine, weight, 2.0) / N
    inverse = (forward * weight[:, None]).T
    g = np.where(k == 96, 0.0, k) * UNIT
    slope = np.where(cosine[:, None], -np.sin(angle), np.cos(angle)) * (g * weight)[:, None]
    return forward, inverse, slope.T, (UNIT * k) ** 2


def make_tables():
    fwd, inv, dif, q2 = real_basis()
    idx = np.arange(N)
    ang = 2 * np.pi * (idx[:, None] * idx[None, :] % N) / N
    c, s = np.cos(ang), np.sin(ang)
    ta = np.zeros((64, 8, 384))
    for j in range(3):
        z = 3 * np.arange(64) + j
        ta[:, j, :N], ta[:, j, N:] = c[z], -s[z]
        ta[:, 3 + j, :N], ta[:, 3 + j, N:] = s[z], c[z]
    xp = 16 * (idx // 12) + idx % 12
    tyc = np.zeros((256, 512))
    tyc[xp, :N], tyc[xp, 256 : 256 + N] = c, s
    band = idx // 12
    krow = 128 * (band % 2) + 16 * (band // 2) + idx % 12
    ry = np.zeros((256, 256))
    ry[krow, :N] = fwd
    px, py, i = idx // 12, (idx % 12) // 3, idx % 3
    rx = np.zeros((N, 256))
    rx[:, 64 * i + 16 * py + px] = fwd.T
    rx[:, 192] = fwd[0]
    zo = (3 * np.arange(64)[None, :] + np.arange(3)[:, None]).reshape(-1)
    rz = fwd[:, zo]
    gz = (dif @ fwd)[zo][:, zo]
    kcol = 16 * (idx % 12) + 8 * (band % 2) + band // 2
    ryi = np.zeros((2, 256, N))
    ryi[0][np.ix_(xp, kcol)] = inv
    ryi[1][np.ix_(xp, kcol)] = dif
    kx = 16 * (4 * i + py) + px
    rxi = np.zeros((N, 512))
    rxi[kx, :N] = inv.T
    rxi[kx, 256 : 256 + N] = dif.T
    qx = np.zeros((64, 1, 128), np.float32)
    qy = np.zeros((16, 1, 128), np.float32)
    for ii in range(3):
        for t in range(12):
            p = np.arange(64)
            qx[:, 0, 12 * ii + t] = q2[12 * (p % 16) + 3 * (p // 16) + ii]
            qy[:, 0, 12 * ii + t] = q2[12 * np.arange(16) + t]
    tabs = [hilo(a) for a in (ta.reshape(512, 384), tyc, ry, rx, rz, gz, ryi, rxi)]
    return tabs + [qx, qy]


def mm(a, b):
    return lax.dot_general(a, b, (((1,), (0,)), ((), ())), preferred_element_type=F32)


def mmt(a, b):
    return lax.dot_general(a, b, (((1,), (1,)), ((), ())), preferred_element_type=F32)


def split(x):
    hi = x.astype(BF)
    return hi, (x - hi.astype(F32)).astype(BF)


def mtm(a, b):
    return lax.dot_general(a, b, (((0,), (0,)), ((), ())), preferred_element_type=F32)


def mm3(a, b, dot=mm):
    return dot(a[0], b[0]) + dot(a[0], b[1]) + dot(a[1], b[0])


def stage_columns(orb, x_of, y_of, px, ta):
    out = mmt(ta[0], orb) + mmt(ta[1], orb)
    row = lax.broadcasted_iota(jnp.int32, (8, 128), 0)
    y_row = y_of + 4 * (y_of // 12)
    place = jnp.where(row == 6, (x_of - px * 12).astype(F32), jnp.where(row == 7, y_row.astype(F32), 0.0))
    return (out.reshape(64, 8, 128) + place[None]).astype(BF)


def stage_scatter(pieces):
    data = jnp.concatenate(pieces, axis=1).astype(F32)
    hot = (lax.broadcasted_iota(jnp.int32, (256, 512), 0).astype(F32) == data[7:8]).astype(F32).astype(BF)
    place = lax.broadcasted_iota(jnp.int32, (16, 512), 0).astype(F32) == data[6:7]
    rows = jnp.concatenate([jnp.where(place, data[r : r + 1], 0.0) for r in range(6)], axis=0)
    return mmt(rows.astype(BF), hot).astype(BF)


def stage_tables(tyc, ty, tx):
    for h in range(2):
        c, s = tyc[h, :, :256], tyc[h, :, 256:]
        ty[512 * h : 512 * h + 256, 0:256] = c
        ty[512 * h : 512 * h + 256, 256:512] = s
        ty[512 * h + 256 : 512 * h + 512, 0:256] = -s
        ty[512 * h + 256 : 512 * h + 512, 256:512] = c
        ct, st = (t.astype(F32).T[:N].astype(BF) for t in (c, s))
        tx[0:N, 512 * h : 512 * h + 256] = ct
        tx[0:N, 512 * h + 256 : 512 * h + 512] = -st
        tx[N : 2 * N, 512 * h : 512 * h + 256] = st
        tx[N : 2 * N, 512 * h + 256 : 512 * h + 512] = ct


def stage_density(p_re, p_im, weight, ty, tx):
    along = mm(jnp.concatenate([p_re, p_im, p_re, p_im], axis=1), ty[...]).astype(BF)
    rows = jnp.concatenate([along[:, :256], along[:, 256:]], axis=0)
    both = mm(tx[...], jnp.concatenate([rows, rows], axis=0))
    re, im = both[:N], both[N:]
    return weight * (re * re + im * im)


def stage_plane(rho, ry, rx):
    t = mm3(ry, split(rho), mmt)
    return mm3(split(t), rx)


def stage_core(core, band, ry, rx):
    core = jnp.concatenate([core, jnp.zeros((4, N), F32)], axis=0)
    part = split(mm3(split(core), rx))
    y = lax.broadcasted_iota(jnp.int32, (256, 16), 0)
    t = lax.broadcasted_iota(jnp.int32, (256, 16), 1)
    pick = jnp.where((y == 12 * band + t) & (t < 12), 1.0, 0.0).astype(BF)
    placed = [mm(pick, h).astype(BF) for h in part]
    return mm3(ry, placed)


def halves_for_wire(x):
    lane = lax.broadcasted_iota(jnp.int32, x.shape, x.ndim - 1)
    return jnp.where(lane == 192, x - x.astype(BF).astype(F32), x).astype(BF)


def stage_pack(s):
    gap = jnp.zeros((24, 256), F32)
    rows = jnp.concatenate([s[0], gap, s[1], gap, s[2], gap, gap[:8]], axis=0)
    t = rows.T
    return t[0:64] + t[192:256] + roll(t[64:128], 12, 1) + roll(t[128:192], 24, 1)


def stage_z(w, qx, qy, rz, gz):
    lane = lax.broadcasted_iota(jnp.int32, (64, 128), 1)
    inside = lane < 36
    cols = jnp.concatenate([jnp.where(inside, w if j == 0 else roll(w, 128 - 40 * j, 1), 0.0) for j in range(3)], axis=0)
    both = split(cols)
    spectrum = mm3(rz, both)
    n = lax.broadcasted_iota(jnp.int32, (N, 128), 0)
    k = jnp.where(n <= 96, n, n - 96)
    weight = jnp.where((n == 0) | (n == 96), 1.0 / N, 2.0 / N)
    squared = UNIT**2 * (k * k).astype(F32) + (qx + qy)
    factor = jnp.where(squared > 0, 4.0 * math.pi / jnp.where(squared > 0, squared, 1.0), 0.0)
    hart = mm3(rz, split(spectrum * (factor * weight)), mtm)
    slope = mm3(gz, both)
    full = cols + roll(hart, 40, 1) + roll(slope, 80, 1)
    group = jnp.where(lane % 40 < 36, lane % 40 // 12, 9)
    out = []
    for i in range(3):
        acc = jnp.zeros((64, 128), F32)
        for j in range(3):
            shift = (12 * (j - i)) % 128
            part = full[64 * j : 64 * j + 64]
            acc = jnp.where(group == j, roll(part, shift, 1) if shift else part, acc)
        out.append(acc)
    return out


def swap_minor(x):
    lane = lax.broadcasted_iota(jnp.int32, (16, 128), 1)
    moved = [x[u] if u == 0 else roll(x[u], u, 1) for u in range(12)]
    out = []
    for v in range(12):
        at = lane - v
        at = jnp.where((at >= 0) & (at < 120) & (at % 40 < 36), at % 40 % 12, 99)
        acc = jnp.zeros((16, 128), F32)
        for u in range(12):
            acc = jnp.where(at == u, moved[u], acc)
        out.append(acc if v == 0 else roll(acc, 128 - v, 1))
    return out


def stage_y(x, ryi):
    cols = split(jnp.concatenate(swap_minor(x), axis=0))
    return mm3((ryi[0][0], ryi[1][0]), cols), mm3((ryi[0][1], ryi[1][1]), cols)


def stage_x(a, g, rxi):
    fill = jnp.zeros((64, 128), F32)
    f = jnp.concatenate(swap_minor(a) + [fill], axis=0).T[:, :N].astype(BF)
    s = jnp.concatenate(swap_minor(g) + [fill], axis=0).T[:, :N].astype(BF)
    both = mm(f, rxi[0]) + mm(f, rxi[1])
    gy = mm(s[0:64], rxi[0][:, :256]) + mm(s[0:64], rxi[1][:, :256])
    return both[0:40, :256], both[40:80, :256], both[0:40, 256:], gy[0:40], both[80:120, :256]


def stage_potential(rho, hart, gx, gy, gz):
    rho = jnp.where(rho > 0, rho, 1.0)
    cube_root = jnp.exp(jnp.log(rho) * (1.0 / 3.0))
    four = rho * cube_root
    reduced = (gx * gx + gy * gy + gz * gz) / (REDUCED * four * four)
    inverse = 1.0 / (1.0 + MU * reduced / KAPPA)
    enhance = 1.0 + KAPPA - KAPPA * inverse
    slope = MU * inverse * inverse
    return hart - SLATER * cube_root * ((4.0 / 3.0) * enhance - (8.0 / 3.0) * reduced * slope)


def stage_block(fields):
    lane = lax.broadcasted_iota(jnp.int32, (40, 128), 1)
    rows = [f[:, :128] for f in fields]
    for k in (0, 2):
        rows.append(jnp.where(lane < 64, fields[k][:, 128:], roll(fields[k + 1][:, 128:], 64, 1)))
    return jnp.concatenate(rows, axis=0).astype(BF)


def kernel(
    occ, *rest,
):
    far, rest = rest[:13], rest[13:]
    r6, near, rest = rest[0], rest[1:14], rest[14:]
    orb, sticks, core, ta, tyc, ry, rx, rz, gz, ryi, rxi, qx, qy = near
    (
    ty, tx, s1, r1a, r1b, core_out, core_in, planes, part, r2a, sums, r2b, s3, r3a, r3b, s4, r4a, r4c,
    s5, r5b, wide, send, recv, load,
    ) = rest
    band, px, py = lax.axis_index("band"), lax.axis_index("px"), lax.axis_index("py")
    cz, cc = band // 2, band % 2
    cx, lo = px % 8, px // 8
    cy = 2 * py + lo

    def at(z=None, c=None, x=None, y=None):
        z, c = cz if z is None else z, cc if c is None else c
        x, y = cx if x is None else x, cy if y is None else y
        return (z * 2 + c, (y % 2) * 8 + x, y // 2)

    open_scope = [None]

    def phase(name):
        if open_scope[0] is not None:
            open_scope[0].__exit__(None, None, None)
        open_scope[0] = jax.named_scope(name) if name else None
        if name:
            open_scope[0].__enter__()

    def ring(me, d, n):
        return lax.rem(me + d, n)

    bar = pltpu.get_barrier_semaphore()

    def hail(target):
        pl.semaphore_signal(bar, inc=1, device_id=target, device_id_type=MESH)

    swapped = (px, band, py)
    for d in range(1, 8):
        hail(at(x=ring(cx, d, 8)))
        hail(at(y=ring(cy, d, 8)))
        hail(at(z=ring(cz, d, 8)))
        hail(at(z=ring(cz, d, 8), c=1 - cc))
        hail(at(x=ring(cx, d, 8), y=2 * py + 1 - lo))
    hail(at(c=1 - cc))

    @pl.when(band != px)
    def _():
        hail(swapped)

    loads = {}
    for k in (0, 1, 3, 2, 4, 5, 6, 7, 8, 9, 10, 11, 12):
        loads[k] = pltpu.make_async_copy(far[k], near[k], load.at[k])
        loads[k].start()
    count = [0]

    def copy(src, dst, target):
        k = count[0]
        count[0] += 1
        c = pltpu.make_async_remote_copy(
            src_ref=src, dst_ref=dst, send_sem=send.at[k], recv_sem=recv.at[k],
            device_id=target, device_id_type=MESH,
        )
        c.start()
        return c

    phase("columns")
    for k in (0, 1, 3):
        loads[k].wait()
    mine = pl.ds(pl.multiple_of(py * 128, 128), 128)
    s1[...] = stage_columns(orb[...], sticks[0:1, mine], sticks[1:2, mine], px, ta).reshape(8, 8, 8, 128)
    loads[2].wait()
    for j in range(3):
        core_out[j] = core[:, pl.ds(3 * band + j, 1)].reshape(12, N)
    phase("barrier")
    pl.semaphore_wait(bar, 36 + jnp.where(band != px, 1, 0))

    phase("e1_y")
    flights = [copy(s1.at[ring(cy, d, 8)], r1a.at[cy], at(y=ring(cy, d, 8))) for d in range(1, 8)]
    core_copy = pltpu.make_async_remote_copy(
        src_ref=core_out, dst_ref=core_in, send_sem=send.at[119], recv_sem=recv.at[119],
        device_id=swapped, device_id_type=MESH,
    )

    @pl.when(band != px)
    def _():
        core_copy.start()

    @pl.when(band == px)
    def _():
        core_in[...] = core_out[...]

    r1a[cy] = s1[cy]
    for k in (4, 5, 6):
        loads[k].wait()
    stage_tables(tyc, ty, tx)
    for f in flights:
        f.wait()
    phase("e1_x_core")
    flights = [copy(r1a.at[:, ring(cx, d, 8)], r1b.at[:, cx], at(x=ring(cx, d, 8))) for d in range(1, 8)]
    for y in range(8):
        r1b[y, cx] = r1a[y, cx]

    @pl.when(band != px)
    def _():
        core_copy.wait()

    def core_step(j, carry):
        part[j] = stage_core(core_in[j], band, ry, rx)
        return carry

    lax.fori_loop(0, 3, core_step, 0)
    phase("scatter")
    arrival = count[0] - 8

    def scatter_step(q, carry):
        odd = q % 2
        d = odd * ((q + 1) // 2) + (1 - odd) * (8 - q // 2)
        source = lax.rem(cx + 8 - d, 8)

        @pl.when(q > 0)
        def _():
            pltpu.make_async_remote_copy(
                src_ref=r1a.at[:, source], dst_ref=r1b.at[:, source],
                send_sem=send.at[arrival + d], recv_sem=recv.at[arrival + d],
                device_id=at(x=source), device_id_type=MESH,
            ).wait_recv()

        for l in range(2):
            block = stage_scatter([r1b[2 * q4 + l, source] for q4 in range(4)])
            row = pl.ds(pl.multiple_of(128 * l + source * 16, 16), 16)
            for r in range(6):
                planes[r, row, :] = block[16 * r : 16 * r + 16]
        return carry

    lax.fori_loop(0, 8, scatter_step, 0)
    for f in flights:
        f.wait_send()

    other = 1 - cc
    flights, pairs = [], []

    def spread(j):
        pairs[j].wait()
        total = part[j, pl.ds(pl.multiple_of(cc * 128, 128), 128)] + r2a[j]
        sums[j] = halves_for_wire(total).reshape(8, 16, 256)
        for d in (4, 3, 5, 2, 6, 1, 7):
            z = ring(cz, d, 8)
            flights.append(copy(sums.at[j, z], r2b.at[cz, j], at(z=z)))
        r2b[cz, j] = sums[j, cz]

    for j in range(3):
        phase(f"plane{j}")
        rho = stage_density(planes[j], planes[3 + j], occ[0], ty, tx)
        part[j] = part[j] + stage_plane(rho, ry, rx)
        pairs.append(copy(part.at[j, pl.ds(pl.multiple_of(other * 128, 128), 128)], r2a.at[j], at(c=other)))
        if j > 0:
            phase(f"spread{j}")
            spread(j - 1)
    phase("spread3")
    spread(2)
    phase("e2_z")
    for f in flights:
        f.wait()
    acc = r2b[0].astype(F32)
    for z in range(1, 8):
        acc = acc + r2b[z].astype(F32)

    phase("pack")
    s3[...] = stage_pack(acc).reshape(8, 8, 128)
    phase("e3_y")
    flights = [copy(s3.at[ring(cy, d, 8)], r3a.at[cy], at(y=ring(cy, d, 8))) for d in range(1, 8)]
    r3a[cy] = s3[cy]
    for f in flights:
        f.wait()
    phase("e3_x")
    flights = [
        copy(r3a.at[:, pl.ds(ring(cx, d, 8), 1)], r3b.at[:, pl.ds(cx, 1)], at(x=ring(cx, d, 8))) for d in range(1, 8)
    ]
    r3b[:, pl.ds(cx, 1)] = r3a[:, pl.ds(cx, 1)]
    for f in flights:
        f.wait()
    phase("z")
    for k in (7, 8, 9, 10, 11, 12):
        loads[k].wait()
    out = stage_z(r3b[...].reshape(64, 128), qx[py * 16 + px], qy[band], rz, gz)

    for i in range(3):
        s4[:, i] = out[i].reshape(4, 16, 128)
    phase("e4_y")
    flights = [
        copy(s4.at[ring(py, d, 4)], r4a.at[py], at(y=2 * ring(py, d, 4) + lo)) for d in range(1, 4)
    ]
    r4a[py] = s4[py]
    for f in flights:
        f.wait()
    phase("e4_z")
    flights = []
    for d in range(15, 0, -1):
        z, c = ring(cz, d // 2, 8), lax.rem(cc + d % 2, 2)
        rows = r4a.at[:, :, pl.ds(c * 8 + z, 1)]
        flights.append(copy(rows, r4c.at[cc, :, :, pl.ds(cz, 1)], at(z=z, c=c)))
    r4c[cc, :, :, pl.ds(cz, 1)] = r4a[:, :, pl.ds(cc * 8 + cz, 1)]
    for f in flights:
        f.wait()
    phase("y")
    x = [jnp.concatenate([r4c[0, q, i], r4c[1, q, i]], axis=0) for i in range(3) for q in range(4)]
    along, slope = stage_y(x, ryi)

    s5[:, :, 0] = along.astype(BF).reshape(2, 8, 16, 128)
    s5[:, :, 1] = slope.astype(BF).reshape(2, 8, 16, 128)
    phase("e5")
    flights = []
    for d in range(15, 0, -1):
        to_x, to_lo = ring(cx, d // 2, 8), lax.rem(lo + d % 2, 2)
        flights.append(copy(s5.at[to_lo, to_x], r5b.at[lo, cx], at(x=to_x, y=2 * py + to_lo)))
    r5b[lo, cx] = s5[lo, cx]
    for f in flights:
        f.wait()
    phase("x")
    wide[...] = r5b[...].astype(F32).reshape(512, 128)
    a = [wide[pl.ds(y, 16, stride=32), :] for y in range(12)]
    g = [wide[pl.ds(16 + y, 16, stride=32), :] for y in range(12)]
    rho, hart, gx, gy, gzz = stage_x(a, g, rxi)
    value = stage_potential(rho, hart, gx, gy, gzz)

    r6[cc, cz] = stage_block([value, gx, gy, gzz])
    phase("e6")
    mine = r6.at[cc, cz]
    hops = {d: copy(mine, mine, at(z=ring(cz, d % 8, 8))) for d in (2, -2, 1, -1)}
    last = [copy(mine, mine, at(c=other))]
    relays = {}
    cut = {1: pl.ds(0, 128), -1: pl.ds(128, 112)}
    for way in (1, -1):
        hops[2 * way].wait_recv()
        got = r6.at[cc, ring(cz, -2 * way % 8, 8)]
        relays[3 * way] = copy(got, got, at(z=ring(cz, way % 8, 8)))
        part4 = got.at[cut[way]]
        relays[4 * way] = copy(part4, part4, at(z=ring(cz, 2 * way % 8, 8)))
        last.append(copy(got, got, at(c=other)))
    for way in (1, -1):
        hops[way].wait_recv()
        got = r6.at[cc, ring(cz, -way % 8, 8)]
        last.append(copy(got, got, at(c=other)))
    for way in (1, -1):
        relays[3 * way].wait_recv()
        got = r6.at[cc, ring(cz, -3 * way % 8, 8)]
        last.append(copy(got, got, at(c=other)))
    for way in (1, -1):
        relays[4 * way].wait_recv()
    got = r6.at[cc, ring(cz, 4, 8)]
    last.append(copy(got, got, at(c=other)))
    for f in list(hops.values()) + list(relays.values()):
        f.wait_send()
    for f in last:
        f.wait()
    phase(None)


def lay_kernel(r6, pot, grad, got, wide, woven, done, load, store):
    loads = [pltpu.make_async_copy(r6.at[c], got.at[c], load.at[c]) for c in range(2)]
    for c in loads:
        c.start()
    for c in range(2):
        loads[c].wait()
        wide[1920 * c : 1920 * c + 1920] = got[c].astype(F32).reshape(1920, 128)

    def step(y, carry):
        for k in range(4):
            for j in range(3):
                z = pl.ds(j, 16, stride=3)
                woven[k, 0, z] = wide[pl.ds(40 * k + 12 * j + y, 16, stride=240), :]
                tail = wide[pl.ds(160 + 40 * (k // 2) + 12 * j + y, 16, stride=240), :]
                woven[k, 1, z] = roll(tail, 64, 1) if k % 2 else tail
            done[k, y, :, 0:128] = woven[k, 0]
            done[k, y, :, 128:192] = woven[k, 1, :, 0:64]
        return carry

    stores = []
    for q in range(3):
        lax.fori_loop(4 * q, 4 * q + 4, step, 0)
        rows = pl.ds(4 * q, 4)
        for k in range(4):
            target = pot.at[rows] if k == 0 else grad.at[k - 1, rows]
            stores.append(pltpu.make_async_copy(done.at[k, rows], target, store.at[4 * q + k]))
            stores[-1].start()
    for c in stores:
        c.wait()


def body(orbitals, occupations, stick_map, core_density):
    tables = make_tables()
    far = pl.BlockSpec(memory_space=pltpu.HBM)
    operands = [orbitals[0], stick_map, core_density.transpose(1, 0, 2), *tables]
    scratch = [pltpu.VMEM(a.shape, a.dtype) for a in operands] + [
        pltpu.VMEM((1024, 512), BF),
        pltpu.VMEM((384, 1024), BF),
        pltpu.VMEM((8, 8, 8, 128), BF),
        pltpu.VMEM((8, 8, 8, 128), BF),
        pltpu.VMEM((8, 8, 8, 128), BF),
        pltpu.VMEM((3, 12, N), F32),
        pltpu.VMEM((3, 12, N), F32),
        pltpu.VMEM((6, 256, 256), BF),
        pltpu.VMEM((3, 256, 256), F32),
        pltpu.VMEM((3, 128, 256), F32),
        pltpu.VMEM((3, 8, 16, 256), BF),
        pltpu.VMEM((8, 3, 16, 256), BF),
        pltpu.VMEM((8, 8, 128), F32),
        pltpu.VMEM((8, 8, 128), F32),
        pltpu.VMEM((8, 8, 128), F32),
        pltpu.VMEM((4, 3, 16, 128), F32),
        pltpu.VMEM((4, 3, 16, 128), F32),
        pltpu.VMEM((2, 4, 3, 8, 128), F32),
        pltpu.VMEM((2, 8, 2, 16, 128), BF),
        pltpu.VMEM((2, 8, 2, 16, 128), BF),
        pltpu.VMEM((512, 128), F32),
        pltpu.SemaphoreType.DMA((120,)),
        pltpu.SemaphoreType.DMA((120,)),
        pltpu.SemaphoreType.DMA((13,)),
    ]
    blocks = pl.pallas_call(
        kernel,
        out_shape=jax.ShapeDtypeStruct((2, 8, 240, 128), BF),
        in_specs=[pl.BlockSpec(memory_space=pltpu.SMEM)] + [far] * len(operands),
        out_specs=pl.BlockSpec(memory_space=pltpu.VMEM),
        scratch_shapes=scratch,
        compiler_params=pltpu.CompilerParams(collective_id=0, has_side_effects=True, vmem_limit_bytes=67_043_328),
    )(occupations, *operands)
    pot, grad = pl.pallas_call(
        lay_kernel,
        out_shape=(
            jax.ShapeDtypeStruct((12, 48, N), F32),
            jax.ShapeDtypeStruct((3, 12, 48, N), F32),
        ),
        in_specs=[far],
        out_specs=(far, far),
        scratch_shapes=[
            pltpu.VMEM((2, 8, 240, 128), BF),
            pltpu.VMEM((3840, 128), F32),
            pltpu.VMEM((4, 2, 48, 128), F32),
            pltpu.VMEM((4, 12, 48, N), F32),
            pltpu.SemaphoreType.DMA((2,)),
            pltpu.SemaphoreType.DMA((12,)),
        ],
        compiler_params=pltpu.CompilerParams(vmem_limit_bytes=67_043_328),
    )(blocks)
    return pot.transpose(1, 0, 2), grad.transpose(0, 2, 1, 3)


def solution(mesh):
    return jax.shard_map(
        body,
        mesh=mesh,
        in_specs=(P("band", ("px", "py"), None), P("band"), P(None, "px"), P("py", "px", None)),
        out_specs=(P("py", "px", None), P(None, "py", "px", None)),
        check_vma=False,
    )
```

```python
import functools
import math

import jax
import jax.numpy as jnp
import numpy as np
from jax import lax
from jax.experimental import pallas as pl
from jax.experimental.pallas import tpu as pltpu
from jax.sharding import PartitionSpec as P

N = 192
SPACING = 0.25
KAPPA = 0.804
MU = 0.2195
SLATER = 0.75 * (3.0 / math.pi) ** (1.0 / 3.0)
REDUCED = 4.0 * (3.0 * math.pi**2) ** (2.0 / 3.0)
UNIT = 2.0 * math.pi / (N * SPACING)
F32 = jnp.float32
BF = jnp.bfloat16
MESH = pl.DeviceIdType.MESH
FAR_FIRST = (4, 3, 5, 2, 6, 1, 7)
roll = pltpu.roll


def hilo(a):
    a = np.asarray(a, np.float32)
    hi = a.astype(BF)
    lo = (a - hi.astype(np.float32)).astype(BF)
    return np.stack([hi, lo])


def real_basis():
    n = np.arange(N)
    k = np.where(n <= 96, n, n - 96)
    cosine = n <= 96
    x = np.arange(N)
    angle = 2 * np.pi * (k[:, None] * x[None, :] % N) / N
    forward = np.where(cosine[:, None], np.cos(angle), np.sin(angle))
    weight = np.where((k == 0) | (k == 96), 1.0, 2.0)
    weight = np.where(cosine, weight, 2.0) / N
    inverse = (forward * weight[:, None]).T
    g = np.where(k == 96, 0.0, k) * UNIT
    slope = np.where(cosine[:, None], -np.sin(angle), np.cos(angle)) * (g * weight)[:, None]
    return forward, inverse, slope.T, (UNIT * k) ** 2


def make_tables():
    fwd, inv, dif, q2 = real_basis()
    idx = np.arange(N)
    ang = 2 * np.pi * (idx[:, None] * idx[None, :] % N) / N
    c, s = np.cos(ang), np.sin(ang)
    ta = np.zeros((64, 8, 384))
    for j in range(3):
        z = 3 * np.arange(64) + j
        ta[:, j, :N], ta[:, j, N:] = c[z], -s[z]
        ta[:, 3 + j, :N], ta[:, 3 + j, N:] = s[z], c[z]
    xp = 16 * (idx // 12) + idx % 12
    tyc = np.zeros((256, 512))
    tyc[xp, :N], tyc[xp, 256 : 256 + N] = c, s
    band = idx // 12
    krow = 128 * (band % 2) + 16 * (band // 2) + idx % 12
    ry = np.zeros((256, 256))
    ry[krow, :N] = fwd
    px, py, i = idx // 12, (idx % 12) // 3, idx % 3
    rx = np.zeros((N, 256))
    rx[:, 64 * i + 16 * py + px] = fwd.T
    rx[:, 192] = fwd[0]
    zo = (3 * np.arange(64)[None, :] + np.arange(3)[:, None]).reshape(-1)
    rz = fwd[:, zo]
    gz = (dif @ fwd)[zo][:, zo]
    kcol = 16 * (idx % 12) + 8 * (band % 2) + band // 2
    ryi = np.zeros((2, 256, N))
    ryi[0][np.ix_(xp, kcol)] = inv
    ryi[1][np.ix_(xp, kcol)] = dif
    kx = 16 * (4 * i + py) + px
    rxi = np.zeros((N, 512))
    rxi[kx, :N] = inv.T
    rxi[kx, 256 : 256 + N] = dif.T
    qx = np.zeros((64, 1, 128), np.float32)
    qy = np.zeros((16, 1, 128), np.float32)
    for ii in range(3):
        for t in range(12):
            p = np.arange(64)
            qx[:, 0, 12 * ii + t] = q2[12 * (p % 16) + 3 * (p // 16) + ii]
            qy[:, 0, 12 * ii + t] = q2[12 * np.arange(16) + t]
    tabs = [hilo(a) for a in (ta.reshape(512, 384), tyc, ry, rx, rz, gz, ryi, rxi)]
    return tabs + [qx, qy]


def mm(a, b):
    return lax.dot_general(a, b, (((1,), (0,)), ((), ())), preferred_element_type=F32)


def mmt(a, b):
    return lax.dot_general(a, b, (((1,), (1,)), ((), ())), preferred_element_type=F32)


def split(x):
    hi = x.astype(BF)
    return hi, (x - hi.astype(F32)).astype(BF)


def mtm(a, b):
    return lax.dot_general(a, b, (((0,), (0,)), ((), ())), preferred_element_type=F32)


def mm3(a, b, dot=mm):
    return dot(a[0], b[0]) + dot(a[0], b[1]) + dot(a[1], b[0])


def stage_columns(orb, x_of, y_of, px, ta):
    out = mmt(ta[0], orb) + mmt(ta[1], orb)
    row = lax.broadcasted_iota(jnp.int32, (8, 128), 0)
    y_row = y_of + 4 * (y_of // 12)
    place = jnp.where(row == 6, (x_of - px * 12).astype(F32), jnp.where(row == 7, y_row.astype(F32), 0.0))
    return (out.reshape(64, 8, 128) + place[None]).astype(BF)


def stage_scatter(pieces):
    data = jnp.concatenate(pieces, axis=1).astype(F32)
    hot = (lax.broadcasted_iota(jnp.int32, (256, 512), 0).astype(F32) == data[7:8]).astype(F32).astype(BF)
    place = lax.broadcasted_iota(jnp.int32, (16, 512), 0).astype(F32) == data[6:7]
    rows = jnp.concatenate([jnp.where(place, data[r : r + 1], 0.0) for r in range(6)], axis=0)
    return mmt(rows.astype(BF), hot).astype(BF)


def stage_tables(tyc, ty, tx):
    for h in range(2):
        c, s = tyc[h, :, :256], tyc[h, :, 256:]
        ty[512 * h : 512 * h + 256, 0:256] = c
        ty[512 * h : 512 * h + 256, 256:512] = s
        ty[512 * h + 256 : 512 * h + 512, 0:256] = -s
        ty[512 * h + 256 : 512 * h + 512, 256:512] = c
        ct, st = (t.astype(F32).T[:N].astype(BF) for t in (c, s))
        tx[0:N, 512 * h : 512 * h + 256] = ct
        tx[0:N, 512 * h + 256 : 512 * h + 512] = -st
        tx[N : 2 * N, 512 * h : 512 * h + 256] = st
        tx[N : 2 * N, 512 * h + 256 : 512 * h + 512] = ct


def stage_density(p_re, p_im, weight, ty, tx):
    along = mm(jnp.concatenate([p_re, p_im, p_re, p_im], axis=1), ty[...]).astype(BF)
    rows = jnp.concatenate([along[:, :256], along[:, 256:]], axis=0)
    both = mm(tx[...], jnp.concatenate([rows, rows], axis=0))
    re, im = both[:N], both[N:]
    return weight * (re * re + im * im)


def stage_plane(rho, ry, rx):
    t = mm3(ry, split(rho), mmt)
    return mm3(split(t), rx)


def stage_core(core, band, ry, rx):
    core = jnp.concatenate([core, jnp.zeros((4, N), F32)], axis=0)
    part = split(mm3(split(core), rx))
    y = lax.broadcasted_iota(jnp.int32, (256, 16), 0)
    t = lax.broadcasted_iota(jnp.int32, (256, 16), 1)
    pick = jnp.where((y == 12 * band + t) & (t < 12), 1.0, 0.0).astype(BF)
    placed = [mm(pick, h).astype(BF) for h in part]
    return mm3(ry, placed)


def halves_for_wire(x):
    lane = lax.broadcasted_iota(jnp.int32, x.shape, x.ndim - 1)
    return jnp.where(lane == 192, x - x.astype(BF).astype(F32), x).astype(BF)


def stage_pack(s):
    gap = jnp.zeros((24, 256), F32)
    rows = jnp.concatenate([s[0], gap, s[1], gap, s[2], gap, gap[:8]], axis=0)
    t = rows.T
    return t[0:64] + t[192:256] + roll(t[64:128], 12, 1) + roll(t[128:192], 24, 1)


def stage_z(w, qx, qy, rz, gz):
    lane = lax.broadcasted_iota(jnp.int32, (64, 128), 1)
    inside = lane < 36
    cols = jnp.concatenate([jnp.where(inside, w if j == 0 else roll(w, 128 - 40 * j, 1), 0.0) for j in range(3)], axis=0)
    both = split(cols)
    spectrum = mm3(rz, both)
    n = lax.broadcasted_iota(jnp.int32, (N, 128), 0)
    k = jnp.where(n <= 96, n, n - 96)
    weight = jnp.where((n == 0) | (n == 96), 1.0 / N, 2.0 / N)
    squared = UNIT**2 * (k * k).astype(F32) + (qx + qy)
    factor = jnp.where(squared > 0, 4.0 * math.pi / jnp.where(squared > 0, squared, 1.0), 0.0)
    hart = mm3(rz, split(spectrum * (factor * weight)), mtm)
    slope = mm3(gz, both)
    full = cols + roll(hart, 40, 1) + roll(slope, 80, 1)
    group = jnp.where(lane % 40 < 36, lane % 40 // 12, 9)
    out = []
    for i in range(3):
        acc = jnp.zeros((64, 128), F32)
        for j in range(3):
            shift = (12 * (j - i)) % 128
            part = full[64 * j : 64 * j + 64]
            acc = jnp.where(group == j, roll(part, shift, 1) if shift else part, acc)
        out.append(acc)
    return out


def swap_minor(x):
    lane = lax.broadcasted_iota(jnp.int32, (16, 128), 1)
    moved = [x[u] if u == 0 else roll(x[u], u, 1) for u in range(12)]
    out = []
    for v in range(12):
        at = lane - v
        at = jnp.where((at >= 0) & (at < 120) & (at % 40 < 36), at % 40 % 12, 99)
        acc = jnp.zeros((16, 128), F32)
        for u in range(12):
            acc = jnp.where(at == u, moved[u], acc)
        out.append(acc if v == 0 else roll(acc, 128 - v, 1))
    return out


def stage_y(x, ryi):
    cols = split(jnp.concatenate(swap_minor(x), axis=0))
    along, slope = mm3((ryi[0][0], ryi[1][0]), cols), mm3((ryi[0][1], ryi[1][1]), cols)
    row = lax.broadcasted_iota(jnp.int32, (256, 128), 0) % 16
    lane = lax.broadcasted_iota(jnp.int32, (256, 128), 1)
    spare = roll(jnp.where(lane < 36, slope, 0.0), 12, 0)
    for h in (1, 2):
        moved = roll(roll(slope, 12 - 4 * h, 0), 40 * h, 1)
        spare = jnp.where((lane >= 40 * h) & (lane < 40 * h + 36), moved, spare)
    return jnp.where(row < 12, along, spare)


def stage_x(a, g, rxi):
    fill = jnp.zeros((64, 128), F32)
    f = jnp.concatenate(swap_minor(a) + [fill], axis=0).T[:, :N].astype(BF)
    s = jnp.concatenate(swap_minor(g) + [fill], axis=0).T[:, :N].astype(BF)
    both = mm(f, rxi[0]) + mm(f, rxi[1])
    gy = mm(s[0:64], rxi[0][:, :256]) + mm(s[0:64], rxi[1][:, :256])
    return both[0:40, :256], both[40:80, :256], both[0:40, 256:], gy[0:40], both[80:120, :256]


def stage_potential(rho, hart, gx, gy, gz):
    rho = jnp.where(rho > 0, rho, 1.0)
    cube_root = jnp.exp(jnp.log(rho) * (1.0 / 3.0))
    four = rho * cube_root
    reduced = (gx * gx + gy * gy + gz * gz) / (REDUCED * four * four)
    inverse = 1.0 / (1.0 + MU * reduced / KAPPA)
    enhance = 1.0 + KAPPA - KAPPA * inverse
    slope = MU * inverse * inverse
    return hart - SLATER * cube_root * ((4.0 / 3.0) * enhance - (8.0 / 3.0) * reduced * slope)


def stage_block(fields):
    lane = lax.broadcasted_iota(jnp.int32, (40, 128), 1)
    rows = [f[:, :128] for f in fields]
    for k in (0, 2):
        rows.append(jnp.where(lane < 64, fields[k][:, 128:], roll(fields[k + 1][:, 128:], 64, 1)))
    return jnp.concatenate(rows, axis=0).astype(BF)


def kernel(
    occ, *rest,
):
    far, rest = rest[:13], rest[13:]
    out, near, rest = rest[0], rest[1:14], rest[14:]
    orb, sticks, core, ta, tyc, ry, rx, rz, gz, ryi, rxi, qx, qy = near
    (
    ty, tx, s1, r1a, r1b, core_out, core_in, planes, part, r2a, sums, r2b, s3, r3a, r3b, s4, r4a, r4c,
    s5, r5b, wide, r6, send, recv, load, store,
    ) = rest
    band, px, py = lax.axis_index("band"), lax.axis_index("px"), lax.axis_index("py")
    cz, cc = band // 2, band % 2
    cx, lo = px % 8, px // 8
    cy = 2 * py + lo

    def at(z=None, c=None, x=None, y=None):
        z, c = cz if z is None else z, cc if c is None else c
        x, y = cx if x is None else x, cy if y is None else y
        return (z * 2 + c, (y % 2) * 8 + x, y // 2)

    open_scope = [None]

    def phase(name):
        if open_scope[0] is not None:
            open_scope[0].__exit__(None, None, None)
        open_scope[0] = jax.named_scope(name) if name else None
        if name:
            open_scope[0].__enter__()

    def ring(me, d, n):
        return lax.rem(me + d, n)

    bar = pltpu.get_barrier_semaphore()

    def hail(target):
        pl.semaphore_signal(bar, inc=1, device_id=target, device_id_type=MESH)

    swapped = (px, band, py)
    for d in range(1, 8):
        hail(at(x=ring(cx, d, 8)))
        hail(at(y=ring(cy, d, 8)))
        hail(at(z=ring(cz, d, 8)))
        hail(at(z=ring(cz, d, 8), c=1 - cc))
        hail(at(x=ring(cx, d, 8), y=2 * py + 1 - lo))
    hail(at(c=1 - cc))

    @pl.when(band != px)
    def _():
        hail(swapped)

    loads = {}
    for k in (0, 1, 3, 2, 4, 5, 6, 7, 8, 9, 10, 11, 12):
        loads[k] = pltpu.make_async_copy(far[k], near[k], load.at[k])
        loads[k].start()
    count = [0]

    def copy(src, dst, target, k=None):
        if k is None:
            k = count[0]
            count[0] += 1
        c = pltpu.make_async_remote_copy(
            src_ref=src, dst_ref=dst, send_sem=send.at[k], recv_sem=recv.at[k],
            device_id=target, device_id_type=MESH,
        )
        c.start()
        return c

    phase("columns")
    for k in (0, 1, 3):
        loads[k].wait()
    mine = pl.ds(pl.multiple_of(py * 128, 128), 128)
    s1[...] = stage_columns(orb[...], sticks[0:1, mine], sticks[1:2, mine], px, ta).reshape(8, 8, 8, 128)
    loads[2].wait()
    for j in range(3):
        core_out[j] = core[:, pl.ds(3 * band + j, 1)].reshape(12, N)
    phase("barrier")
    pl.semaphore_wait(bar, 36 + jnp.where(band != px, 1, 0))

    phase("e1_y")
    flights = [copy(s1.at[ring(cy, d, 8)], r1a.at[cy], at(y=ring(cy, d, 8))) for d in FAR_FIRST]
    core_copy = pltpu.make_async_remote_copy(
        src_ref=core_out, dst_ref=core_in, send_sem=send.at[119], recv_sem=recv.at[119],
        device_id=swapped, device_id_type=MESH,
    )

    @pl.when(band != px)
    def _():
        core_copy.start()

    @pl.when(band == px)
    def _():
        core_in[...] = core_out[...]

    r1a[cy] = s1[cy]
    for k in (4, 5, 6):
        loads[k].wait()
    stage_tables(tyc, ty, tx)
    for f in flights:
        f.wait()
    phase("e1_x_core")
    arrival = count[0] - 1
    flights = [
        copy(r1a.at[:, ring(cx, d, 8)], r1b.at[:, cx], at(x=ring(cx, d, 8)), arrival + d) for d in FAR_FIRST
    ]
    count[0] += 7
    for y in range(8):
        r1b[y, cx] = r1a[y, cx]

    @pl.when(band != px)
    def _():
        core_copy.wait()

    def core_step(j, carry):
        part[j] = stage_core(core_in[j], band, ry, rx)
        return carry

    lax.fori_loop(0, 3, core_step, 0)
    phase("scatter")
    def scatter_step(q, carry):
        odd = q % 2
        d = odd * ((q + 1) // 2) + (1 - odd) * (8 - q // 2)
        source = lax.rem(cx + 8 - d, 8)

        @pl.when(q > 0)
        def _():
            pltpu.make_async_remote_copy(
                src_ref=r1a.at[:, source], dst_ref=r1b.at[:, source],
                send_sem=send.at[arrival + d], recv_sem=recv.at[arrival + d],
                device_id=at(x=source), device_id_type=MESH,
            ).wait_recv()

        for l in range(2):
            block = stage_scatter([r1b[2 * q4 + l, source] for q4 in range(4)])
            row = pl.ds(pl.multiple_of(128 * l + source * 16, 16), 16)
            for r in range(6):
                planes[r, row, :] = block[16 * r : 16 * r + 16]
        return carry

    lax.fori_loop(0, 8, scatter_step, 0)
    for f in flights:
        f.wait_send()

    other = 1 - cc
    flights, pairs = [], []

    def spread(j):
        pairs[j].wait()
        total = part[j, pl.ds(pl.multiple_of(cc * 128, 128), 128)] + r2a[j]
        sums[j] = halves_for_wire(total).reshape(8, 16, 256)
        for d in FAR_FIRST:
            z = ring(cz, d, 8)
            flights.append(copy(sums.at[j, z], r2b.at[cz, j], at(z=z)))
        r2b[cz, j] = sums[j, cz]

    for j in range(3):
        phase(f"plane{j}")
        rho = stage_density(planes[j], planes[3 + j], occ[0], ty, tx)
        part[j] = part[j] + stage_plane(rho, ry, rx)
        pairs.append(copy(part.at[j, pl.ds(pl.multiple_of(other * 128, 128), 128)], r2a.at[j], at(c=other)))
        if j > 0:
            phase(f"spread{j}")
            spread(j - 1)
    phase("spread3")
    spread(2)
    phase("e2_z")
    for f in flights:
        f.wait()
    acc = r2b[0].astype(F32)
    for z in range(1, 8):
        acc = acc + r2b[z].astype(F32)

    phase("pack")
    s3[...] = stage_pack(acc).reshape(8, 8, 128)
    phase("e3_y")
    flights = [copy(s3.at[ring(cy, d, 8)], r3a.at[cy], at(y=ring(cy, d, 8))) for d in FAR_FIRST]
    r3a[cy] = s3[cy]
    for f in flights:
        f.wait()
    phase("e3_x")
    flights = [
        copy(r3a.at[:, pl.ds(ring(cx, d, 8), 1)], r3b.at[:, pl.ds(cx, 1)], at(x=ring(cx, d, 8))) for d in FAR_FIRST
    ]
    r3b[:, pl.ds(cx, 1)] = r3a[:, pl.ds(cx, 1)]
    for f in flights:
        f.wait()
    phase("z")
    for k in (7, 8, 9, 10, 11, 12):
        loads[k].wait()
    turned = stage_z(r3b[...].reshape(64, 128), qx[py * 16 + px], qy[band], rz, gz)

    for i in range(3):
        s4[:, i] = turned[i].reshape(4, 16, 128)
    phase("e4_y")
    flights = [
        copy(s4.at[ring(py, d, 4)], r4a.at[py], at(y=2 * ring(py, d, 4) + lo)) for d in range(1, 4)
    ]
    r4a[py] = s4[py]
    for f in flights:
        f.wait()
    phase("e4_z")
    flights = []
    for d, flip in [(d, flip) for d in FAR_FIRST for flip in (1, 0)] + [(0, 1)]:
        z, c = ring(cz, d, 8), lax.rem(cc + flip, 2)
        rows = r4a.at[:, :, pl.ds(c * 8 + z, 1)]
        flights.append(copy(rows, r4c.at[cc, :, :, pl.ds(cz, 1)], at(z=z, c=c)))
    r4c[cc, :, :, pl.ds(cz, 1)] = r4a[:, :, pl.ds(cc * 8 + cz, 1)]
    for f in flights:
        f.wait()
    phase("y")
    x = [jnp.concatenate([r4c[0, q, i], r4c[1, q, i]], axis=0) for i in range(3) for q in range(4)]
    along = stage_y(x, ryi)

    s5[...] = along.astype(BF).reshape(2, 8, 16, 128)
    phase("e5")
    flights = []
    for d, flip in [(d, flip) for d in FAR_FIRST for flip in (1, 0)] + [(0, 1)]:
        to_x, to_lo = ring(cx, d, 8), lax.rem(lo + flip, 2)
        flights.append(copy(s5.at[to_lo, to_x], r5b.at[lo, cx], at(x=to_x, y=2 * py + to_lo)))
    r5b[lo, cx] = s5[lo, cx]
    for f in flights:
        f.wait()
    phase("x")
    wide[...] = r5b[...].astype(F32).reshape(256, 128)
    a = [wide[pl.ds(y, 16, stride=16), :] for y in range(16)]
    g = [a[12 + y % 4] if y < 4 else roll(a[12 + y % 4], 128 - 40 * (y // 4), 1) for y in range(12)]
    rho, hart, gx, gy, gzz = stage_x(a[:12], g, rxi)
    value = stage_potential(rho, hart, gx, gy, gzz)

    r6[cc, cz] = stage_block([value, gx, gy, gzz])
    phase("e6")
    chunks = (pl.ds(0, 128), pl.ds(128, 112))
    hops, relays, last, home = {}, {}, [], []

    def block(away):
        return r6.at[cc, ring(cz, away % 8, 8)]

    def go(ref, away):
        return copy(ref, ref, at(z=ring(cz, away % 8, 8)))

    def settle(away):
        last.append(copy(block(away), block(away), at(c=other)))
        for c in (cc, other):
            k = len(home)
            ref = (c, ring(cz, away % 8, 8))
            home.append(pltpu.make_async_copy(r6.at[ref], out.at[ref], store.at[k]))
        home[-2].start()

    for d in (2, -2):
        for h in (0, 1):
            hops[d, h] = go(block(0).at[chunks[h]], d)
    for d in (1, -1):
        hops[d, 0] = go(block(0), d)
    settle(0)
    for h in (0, 1):
        for way in (1, -1):
            hops[2 * way, h].wait_recv()
            got = block(-2 * way).at[chunks[h]]
            relays[3 * way, h] = go(got, way)
            if h == (1 - way) // 2:
                relays[4 * way, h] = go(got, 2 * way)
    settle(-2)
    settle(2)
    for way in (1, -1):
        hops[way, 0].wait_recv()
        settle(-way)
    for way in (1, -1):
        for h in (0, 1):
            relays[3 * way, h].wait_recv()
        settle(-3 * way)
    relays[4, 0].wait_recv()
    relays[-4, 1].wait_recv()
    settle(4)
    for k in range(8):
        last[k].wait()
        home[2 * k + 1].start()
    for f in list(hops.values()) + list(relays.values()):
        f.wait_send()
    for f in home:
        f.wait()
    phase(None)


def lay_kernel(r6, pot, grad, got, wide, woven, done, load, store):
    loads = [pltpu.make_async_copy(r6.at[c], got.at[c], load.at[c]) for c in range(2)]
    for c in loads:
        c.start()
    for c in range(2):
        loads[c].wait()
        wide[1920 * c : 1920 * c + 1920] = got[c].astype(F32).reshape(1920, 128)

    def step(y, carry):
        for k in range(4):
            for j in range(3):
                z = pl.ds(j, 16, stride=3)
                woven[k, 0, z] = wide[pl.ds(40 * k + 12 * j + y, 16, stride=240), :]
                tail = wide[pl.ds(160 + 40 * (k // 2) + 12 * j + y, 16, stride=240), :]
                woven[k, 1, z] = roll(tail, 64, 1) if k % 2 else tail
            done[k, y, :, 0:128] = woven[k, 0]
            done[k, y, :, 128:192] = woven[k, 1, :, 0:64]
        return carry

    stores = []
    for q in range(3):
        lax.fori_loop(4 * q, 4 * q + 4, step, 0)
        rows = pl.ds(4 * q, 4)
        for k in range(4):
            target = pot.at[rows] if k == 0 else grad.at[k - 1, rows]
            stores.append(pltpu.make_async_copy(done.at[k, rows], target, store.at[4 * q + k]))
            stores[-1].start()
    for c in stores:
        c.wait()


def body(orbitals, occupations, stick_map, core_density):
    tables = make_tables()
    far = pl.BlockSpec(memory_space=pltpu.HBM)
    operands = [orbitals[0], stick_map, core_density.transpose(1, 0, 2), *tables]
    scratch = [pltpu.VMEM(a.shape, a.dtype) for a in operands] + [
        pltpu.VMEM((1024, 512), BF),
        pltpu.VMEM((384, 1024), BF),
        pltpu.VMEM((8, 8, 8, 128), BF),
        pltpu.VMEM((8, 8, 8, 128), BF),
        pltpu.VMEM((8, 8, 8, 128), BF),
        pltpu.VMEM((3, 12, N), F32),
        pltpu.VMEM((3, 12, N), F32),
        pltpu.VMEM((6, 256, 256), BF),
        pltpu.VMEM((3, 256, 256), F32),
        pltpu.VMEM((3, 128, 256), F32),
        pltpu.VMEM((3, 8, 16, 256), BF),
        pltpu.VMEM((8, 3, 16, 256), BF),
        pltpu.VMEM((8, 8, 128), F32),
        pltpu.VMEM((8, 8, 128), F32),
        pltpu.VMEM((8, 8, 128), F32),
        pltpu.VMEM((4, 3, 16, 128), F32),
        pltpu.VMEM((4, 3, 16, 128), F32),
        pltpu.VMEM((2, 4, 3, 8, 128), F32),
        pltpu.VMEM((2, 8, 16, 128), BF),
        pltpu.VMEM((2, 8, 16, 128), BF),
        pltpu.VMEM((256, 128), F32),
        pltpu.VMEM((2, 8, 240, 128), BF),
        pltpu.SemaphoreType.DMA((120,)),
        pltpu.SemaphoreType.DMA((120,)),
        pltpu.SemaphoreType.DMA((13,)),
        pltpu.SemaphoreType.DMA((16,)),
    ]
    blocks = pl.pallas_call(
        kernel,
        out_shape=jax.ShapeDtypeStruct((2, 8, 240, 128), BF),
        in_specs=[pl.BlockSpec(memory_space=pltpu.SMEM)] + [far] * len(operands),
        out_specs=far,
        scratch_shapes=scratch,
        compiler_params=pltpu.CompilerParams(collective_id=0, has_side_effects=True, vmem_limit_bytes=67_043_328),
    )(occupations, *operands)
    pot, grad = pl.pallas_call(
        lay_kernel,
        out_shape=(
            jax.ShapeDtypeStruct((12, 48, N), F32),
            jax.ShapeDtypeStruct((3, 12, 48, N), F32),
        ),
        in_specs=[far],
        out_specs=(far, far),
        scratch_shapes=[
            pltpu.VMEM((2, 8, 240, 128), BF),
            pltpu.VMEM((3840, 128), F32),
            pltpu.VMEM((4, 2, 48, 128), F32),
            pltpu.VMEM((4, 12, 48, N), F32),
            pltpu.SemaphoreType.DMA((2,)),
            pltpu.SemaphoreType.DMA((12,)),
        ],
        compiler_params=pltpu.CompilerParams(vmem_limit_bytes=67_043_328),
    )(blocks)
    return pot.transpose(1, 0, 2), grad.transpose(0, 2, 1, 3)


def solution(mesh):
    return jax.shard_map(
        body,
        mesh=mesh,
        in_specs=(P("band", ("px", "py"), None), P("band"), P(None, "px"), P("py", "px", None)),
        out_specs=(P("py", "px", None), P(None, "py", "px", None)),
        check_vma=False,
    )
```

```python
import functools
import math

import jax
import jax.numpy as jnp
import numpy as np
from jax import lax
from jax.experimental import pallas as pl
from jax.experimental.pallas import tpu as pltpu
from jax.sharding import PartitionSpec as P

N = 192
SPACING = 0.25
KAPPA = 0.804
MU = 0.2195
SLATER = 0.75 * (3.0 / math.pi) ** (1.0 / 3.0)
REDUCED = 4.0 * (3.0 * math.pi**2) ** (2.0 / 3.0)
UNIT = 2.0 * math.pi / (N * SPACING)
F32 = jnp.float32
BF = jnp.bfloat16
MESH = pl.DeviceIdType.MESH
FAR_FIRST = (4, 3, 5, 2, 6, 1, 7)
roll = pltpu.roll


def hilo(a):
    a = np.asarray(a, np.float32)
    hi = a.astype(BF)
    lo = (a - hi.astype(np.float32)).astype(BF)
    return np.stack([hi, lo])


def real_basis():
    n = np.arange(N)
    k = np.where(n <= 96, n, n - 96)
    cosine = n <= 96
    x = np.arange(N)
    angle = 2 * np.pi * (k[:, None] * x[None, :] % N) / N
    forward = np.where(cosine[:, None], np.cos(angle), np.sin(angle))
    weight = np.where((k == 0) | (k == 96), 1.0, 2.0)
    weight = np.where(cosine, weight, 2.0) / N
    inverse = (forward * weight[:, None]).T
    g = np.where(k == 96, 0.0, k) * UNIT
    slope = np.where(cosine[:, None], -np.sin(angle), np.cos(angle)) * (g * weight)[:, None]
    return forward, inverse, slope.T, (UNIT * k) ** 2


def make_tables():
    fwd, inv, dif, q2 = real_basis()
    idx = np.arange(N)
    ang = 2 * np.pi * (idx[:, None] * idx[None, :] % N) / N
    c, s = np.cos(ang), np.sin(ang)
    ta = np.zeros((64, 8, 384))
    for j in range(3):
        z = 3 * np.arange(64) + j
        ta[:, j, :N], ta[:, j, N:] = c[z], -s[z]
        ta[:, 3 + j, :N], ta[:, 3 + j, N:] = s[z], c[z]
    xp = 16 * (idx // 12) + idx % 12
    tyc = np.zeros((256, 512))
    tyc[xp, :N], tyc[xp, 256 : 256 + N] = c, s
    band = idx // 12
    krow = 128 * (band % 2) + 16 * (band // 2) + idx % 12
    ry = np.zeros((256, 256))
    ry[krow, :N] = fwd
    px, py, i = idx // 12, (idx % 12) // 3, idx % 3
    rx = np.zeros((N, 256))
    rx[:, 64 * i + 16 * py + px] = fwd.T
    rx[:, 192] = fwd[0]
    zo = (3 * np.arange(64)[None, :] + np.arange(3)[:, None]).reshape(-1)
    rz = fwd[:, zo]
    gz = (dif @ fwd)[zo][:, zo]
    kcol = 16 * (idx % 12) + 8 * (band % 2) + band // 2
    ryi = np.zeros((2, 256, N))
    ryi[0][np.ix_(xp, kcol)] = inv
    ryi[1][np.ix_(xp, kcol)] = dif
    kx = 16 * (4 * i + py) + px
    rxi = np.zeros((N, 512))
    rxi[kx, :N] = inv.T
    rxi[kx, 256 : 256 + N] = dif.T
    qx = np.zeros((64, 1, 128), np.float32)
    qy = np.zeros((16, 1, 128), np.float32)
    for ii in range(3):
        for t in range(12):
            p = np.arange(64)
            qx[:, 0, 12 * ii + t] = q2[12 * (p % 16) + 3 * (p // 16) + ii]
            qy[:, 0, 12 * ii + t] = q2[12 * np.arange(16) + t]
    tabs = [hilo(a) for a in (ta.reshape(512, 384), tyc, ry, rx, rz, gz, ryi, rxi)]
    return tabs + [qx, qy]


def mm(a, b):
    return lax.dot_general(a, b, (((1,), (0,)), ((), ())), preferred_element_type=F32)


def mmt(a, b):
    return lax.dot_general(a, b, (((1,), (1,)), ((), ())), preferred_element_type=F32)


def split(x):
    hi = x.astype(BF)
    return hi, (x - hi.astype(F32)).astype(BF)


def mtm(a, b):
    return lax.dot_general(a, b, (((0,), (0,)), ((), ())), preferred_element_type=F32)


def mm3(a, b, dot=mm):
    return dot(a[0], b[0]) + dot(a[0], b[1]) + dot(a[1], b[0])


def stage_columns(orb, x_of, y_of, px, ta):
    out = mmt(ta[0], orb) + mmt(ta[1], orb)
    row = lax.broadcasted_iota(jnp.int32, (8, 128), 0)
    y_row = y_of + 4 * (y_of // 12)
    place = jnp.where(row == 6, (x_of - px * 12).astype(F32), jnp.where(row == 7, y_row.astype(F32), 0.0))
    return (out.reshape(64, 8, 128) + place[None]).astype(BF)


def stage_scatter(pieces):
    data = jnp.concatenate(pieces, axis=1).astype(F32)
    hot = (lax.broadcasted_iota(jnp.int32, (256, 512), 0).astype(F32) == data[7:8]).astype(F32).astype(BF)
    place = lax.broadcasted_iota(jnp.int32, (16, 512), 0).astype(F32) == data[6:7]
    rows = jnp.concatenate([jnp.where(place, data[r : r + 1], 0.0) for r in range(6)], axis=0)
    return mmt(rows.astype(BF), hot).astype(BF)


def stage_tables(tyc, ty, tx):
    for h in range(2):
        c, s = tyc[h, :, :256], tyc[h, :, 256:]
        ty[512 * h : 512 * h + 256, 0:256] = c
        ty[512 * h : 512 * h + 256, 256:512] = s
        ty[512 * h + 256 : 512 * h + 512, 0:256] = -s
        ty[512 * h + 256 : 512 * h + 512, 256:512] = c
        ct, st = (t.astype(F32).T[:N].astype(BF) for t in (c, s))
        tx[0:N, 512 * h : 512 * h + 256] = ct
        tx[0:N, 512 * h + 256 : 512 * h + 512] = -st
        tx[N : 2 * N, 512 * h : 512 * h + 256] = st
        tx[N : 2 * N, 512 * h + 256 : 512 * h + 512] = ct


def stage_density(p_re, p_im, weight, ty, tx):
    along = mm(jnp.concatenate([p_re, p_im, p_re, p_im], axis=1), ty[...]).astype(BF)
    rows = jnp.concatenate([along[:, :256], along[:, 256:]], axis=0)
    both = mm(tx[...], jnp.concatenate([rows, rows], axis=0))
    re, im = both[:N], both[N:]
    return weight * (re * re + im * im)


def stage_plane(rho, ry, rx):
    t = mm3(ry, split(rho), mmt)
    return mm3(split(t), rx)


def stage_core(core, band, ry, rx):
    core = jnp.concatenate([core, jnp.zeros((4, N), F32)], axis=0)
    part = split(mm3(split(core), rx))
    y = lax.broadcasted_iota(jnp.int32, (256, 16), 0)
    t = lax.broadcasted_iota(jnp.int32, (256, 16), 1)
    pick = jnp.where((y == 12 * band + t) & (t < 12), 1.0, 0.0).astype(BF)
    placed = [mm(pick, h).astype(BF) for h in part]
    return mm3(ry, placed)


def halves_for_wire(x):
    lane = lax.broadcasted_iota(jnp.int32, x.shape, x.ndim - 1)
    return jnp.where(lane == 192, x - x.astype(BF).astype(F32), x).astype(BF)


def stage_pack(s):
    gap = jnp.zeros((24, 256), F32)
    rows = jnp.concatenate([s[0], gap, s[1], gap, s[2], gap, gap[:8]], axis=0)
    t = rows.T
    return t[0:64] + t[192:256] + roll(t[64:128], 12, 1) + roll(t[128:192], 24, 1)


def stage_z(w, qx, qy, rz, gz):
    lane = lax.broadcasted_iota(jnp.int32, (64, 128), 1)
    inside = lane < 36
    cols = jnp.concatenate([jnp.where(inside, w if j == 0 else roll(w, 128 - 40 * j, 1), 0.0) for j in range(3)], axis=0)
    both = split(cols)
    spectrum = mm3(rz, both)
    n = lax.broadcasted_iota(jnp.int32, (N, 128), 0)
    k = jnp.where(n <= 96, n, n - 96)
    weight = jnp.where((n == 0) | (n == 96), 1.0 / N, 2.0 / N)
    squared = UNIT**2 * (k * k).astype(F32) + (qx + qy)
    factor = jnp.where(squared > 0, 4.0 * math.pi / jnp.where(squared > 0, squared, 1.0), 0.0)
    hart = mm3(rz, split(spectrum * (factor * weight)), mtm)
    slope = mm3(gz, both)
    full = cols + roll(hart, 40, 1) + roll(slope, 80, 1)
    group = jnp.where(lane % 40 < 36, lane % 40 // 12, 9)
    out = []
    for i in range(3):
        acc = jnp.zeros((64, 128), F32)
        for j in range(3):
            shift = (12 * (j - i)) % 128
            part = full[64 * j : 64 * j + 64]
            acc = jnp.where(group == j, roll(part, shift, 1) if shift else part, acc)
        out.append(acc)
    return out


def swap_minor(x):
    lane = lax.broadcasted_iota(jnp.int32, (16, 128), 1)
    moved = [x[u] if u == 0 else roll(x[u], u, 1) for u in range(12)]
    out = []
    for v in range(12):
        at = lane - v
        at = jnp.where((at >= 0) & (at < 120) & (at % 40 < 36), at % 40 % 12, 99)
        acc = jnp.zeros((16, 128), F32)
        for u in range(12):
            acc = jnp.where(at == u, moved[u], acc)
        out.append(acc if v == 0 else roll(acc, 128 - v, 1))
    return out


def stage_y(x, ryi):
    cols = split(jnp.concatenate(swap_minor(x), axis=0))
    along, slope = mm3((ryi[0][0], ryi[1][0]), cols), mm3((ryi[0][1], ryi[1][1]), cols)
    row = lax.broadcasted_iota(jnp.int32, (256, 128), 0) % 16
    lane = lax.broadcasted_iota(jnp.int32, (256, 128), 1)
    spare = roll(jnp.where(lane < 36, slope, 0.0), 12, 0)
    for h in (1, 2):
        moved = roll(roll(slope, 12 - 4 * h, 0), 40 * h, 1)
        spare = jnp.where((lane >= 40 * h) & (lane < 40 * h + 36), moved, spare)
    return jnp.where(row < 12, along, spare)


def stage_x(a, g, rxi):
    fill = jnp.zeros((64, 128), F32)
    f = jnp.concatenate(swap_minor(a) + [fill], axis=0).T[:, :N].astype(BF)
    s = jnp.concatenate(swap_minor(g) + [fill], axis=0).T[:, :N].astype(BF)
    both = mm(f, rxi[0]) + mm(f, rxi[1])
    gy = mm(s[0:64], rxi[0][:, :256]) + mm(s[0:64], rxi[1][:, :256])
    return both[0:40, :256], both[40:80, :256], both[0:40, 256:], gy[0:40], both[80:120, :256]


def stage_potential(rho, hart, gx, gy, gz):
    rho = jnp.where(rho > 0, rho, 1.0)
    cube_root = jnp.exp(jnp.log(rho) * (1.0 / 3.0))
    four = rho * cube_root
    reduced = (gx * gx + gy * gy + gz * gz) / (REDUCED * four * four)
    inverse = 1.0 / (1.0 + MU * reduced / KAPPA)
    enhance = 1.0 + KAPPA - KAPPA * inverse
    slope = MU * inverse * inverse
    return hart - SLATER * cube_root * ((4.0 / 3.0) * enhance - (8.0 / 3.0) * reduced * slope)


def stage_block(fields):
    lane = lax.broadcasted_iota(jnp.int32, (40, 128), 1)
    rows = [f[:, :128] for f in fields]
    for k in (0, 2):
        rows.append(jnp.where(lane < 64, fields[k][:, 128:], roll(fields[k + 1][:, 128:], 64, 1)))
    return jnp.concatenate(rows, axis=0).astype(BF)


def kernel(
    occ, *rest,
):
    far, rest = rest[:13], rest[13:]
    out, near, rest = rest[0], rest[1:14], rest[14:]
    orb, sticks, core, ta, tyc, ry, rx, rz, gz, ryi, rxi, qx, qy = near
    (
    ty, tx, s1, r1a, r1b, core_out, core_in, planes, part, r2a, sums, r2b, s3, r3a, r3b, s4, r4c,
    s5, r5b, wide, r6, send, recv, load, store,
    ) = rest
    band, px, py = lax.axis_index("band"), lax.axis_index("px"), lax.axis_index("py")
    cz, cc = band // 2, band % 2
    cx, lo = px % 8, px // 8
    cy = 2 * py + lo

    def at(z=None, c=None, x=None, y=None):
        z, c = cz if z is None else z, cc if c is None else c
        x, y = cx if x is None else x, cy if y is None else y
        return (z * 2 + c, (y % 2) * 8 + x, y // 2)

    open_scope = [None]

    def phase(name):
        if open_scope[0] is not None:
            open_scope[0].__exit__(None, None, None)
        open_scope[0] = jax.named_scope(name) if name else None
        if name:
            open_scope[0].__enter__()

    def ring(me, d, n):
        return lax.rem(me + d, n)

    bar = pltpu.get_barrier_semaphore()

    def hail(target):
        pl.semaphore_signal(bar, inc=1, device_id=target, device_id_type=MESH)

    swapped = (px, band, py)
    for d in range(1, 8):
        hail(at(x=ring(cx, d, 8)))
        hail(at(y=ring(cy, d, 8)))
        hail(at(z=ring(cz, d, 8)))
    hail(at(c=1 - cc))

    @pl.when(band != px)
    def _():
        hail(swapped)

    loads = {}
    for k in (0, 1, 3, 2, 4, 5, 6, 7, 8, 9, 10, 11, 12):
        loads[k] = pltpu.make_async_copy(far[k], near[k], load.at[k])
        loads[k].start()
    count = [0]

    def copy(src, dst, target, k=None):
        if k is None:
            k = count[0]
            count[0] += 1
        c = pltpu.make_async_remote_copy(
            src_ref=src, dst_ref=dst, send_sem=send.at[k], recv_sem=recv.at[k],
            device_id=target, device_id_type=MESH,
        )
        c.start()
        return c

    phase("columns")
    for k in (0, 1, 3):
        loads[k].wait()
    mine = pl.ds(pl.multiple_of(py * 128, 128), 128)
    s1[...] = stage_columns(orb[...], sticks[0:1, mine], sticks[1:2, mine], px, ta).reshape(8, 8, 8, 128)
    loads[2].wait()
    for j in range(3):
        core_out[j] = core[:, pl.ds(3 * band + j, 1)].reshape(12, N)
    phase("barrier")
    pl.semaphore_wait(bar, 22 + jnp.where(band != px, 1, 0))

    phase("e1_y")
    flights = [copy(s1.at[ring(cy, d, 8)], r1a.at[cy], at(y=ring(cy, d, 8))) for d in FAR_FIRST]
    core_copy = pltpu.make_async_remote_copy(
        src_ref=core_out, dst_ref=core_in, send_sem=send.at[179], recv_sem=recv.at[179],
        device_id=swapped, device_id_type=MESH,
    )

    @pl.when(band != px)
    def _():
        core_copy.start()

    @pl.when(band == px)
    def _():
        core_in[...] = core_out[...]

    r1a[cy] = s1[cy]
    for k in (4, 5, 6):
        loads[k].wait()
    stage_tables(tyc, ty, tx)
    for f in flights:
        f.wait()
    phase("e1_x_core")
    arrival = count[0] - 1
    flights = [
        copy(r1a.at[:, ring(cx, d, 8)], r1b.at[:, cx], at(x=ring(cx, d, 8)), arrival + d) for d in FAR_FIRST
    ]
    count[0] += 7
    for y in range(8):
        r1b[y, cx] = r1a[y, cx]

    @pl.when(band != px)
    def _():
        core_copy.wait()

    def core_step(j, carry):
        part[j] = stage_core(core_in[j], band, ry, rx)
        return carry

    lax.fori_loop(0, 3, core_step, 0)
    phase("scatter")
    def scatter_step(q, carry):
        odd = q % 2
        d = odd * ((q + 1) // 2) + (1 - odd) * (8 - q // 2)
        source = lax.rem(cx + 8 - d, 8)

        @pl.when(q > 0)
        def _():
            pltpu.make_async_remote_copy(
                src_ref=r1a.at[:, source], dst_ref=r1b.at[:, source],
                send_sem=send.at[arrival + d], recv_sem=recv.at[arrival + d],
                device_id=at(x=source), device_id_type=MESH,
            ).wait_recv()

        for l in range(2):
            block = stage_scatter([r1b[2 * q4 + l, source] for q4 in range(4)])
            row = pl.ds(pl.multiple_of(128 * l + source * 16, 16), 16)
            for r in range(6):
                planes[r, row, :] = block[16 * r : 16 * r + 16]
        return carry

    lax.fori_loop(0, 8, scatter_step, 0)
    for f in flights:
        f.wait_send()

    other = 1 - cc
    flights, pairs = [], []

    def spread(j):
        pairs[j].wait()
        total = part[j, pl.ds(pl.multiple_of(cc * 128, 128), 128)] + r2a[j]
        sums[j] = halves_for_wire(total).reshape(8, 16, 256)
        for d in FAR_FIRST:
            z = ring(cz, d, 8)
            flights.append(copy(sums.at[j, z], r2b.at[cz, j], at(z=z)))
        r2b[cz, j] = sums[j, cz]

    for j in range(3):
        phase(f"plane{j}")
        rho = stage_density(planes[j], planes[3 + j], occ[0], ty, tx)
        part[j] = part[j] + stage_plane(rho, ry, rx)
        pairs.append(copy(part.at[j, pl.ds(pl.multiple_of(other * 128, 128), 128)], r2a.at[j], at(c=other)))
        if j > 0:
            phase(f"spread{j}")
            spread(j - 1)
    phase("spread3")
    spread(2)
    phase("e2_z")
    for f in flights:
        f.wait()
    acc = r2b[0].astype(F32)
    for z in range(1, 8):
        acc = acc + r2b[z].astype(F32)

    phase("pack")
    s3[...] = stage_pack(acc).reshape(8, 8, 128)
    phase("e3_y")
    flights = [copy(s3.at[ring(cy, d, 8)], r3a.at[cy], at(y=ring(cy, d, 8))) for d in FAR_FIRST]
    r3a[cy] = s3[cy]
    for f in flights:
        f.wait()
    phase("e3_x")
    flights = [
        copy(r3a.at[:, pl.ds(ring(cx, d, 8), 1)], r3b.at[:, pl.ds(cx, 1)], at(x=ring(cx, d, 8))) for d in FAR_FIRST
    ]
    r3b[:, pl.ds(cx, 1)] = r3a[:, pl.ds(cx, 1)]
    for f in flights:
        f.wait()
    phase("z")
    for k in (7, 8, 9, 10, 11, 12):
        loads[k].wait()
    turned = stage_z(r3b[...].reshape(64, 128), qx[py * 16 + px], qy[band], rz, gz)

    phase("e4")
    for i in range(3):
        s4[:, i] = turned[i].reshape(4, 16, 128)
    flights = []
    for e in (2, 1, 3, 0):
        y = ring(py, e, 4)
        for d, flip in [(d, flip) for d in FAR_FIRST + (0,) for flip in (1, 0)]:
            if e or d or flip:
                z, c = ring(cz, d, 8), lax.rem(cc + flip, 2)
                rows = s4.at[y, :, pl.ds(c * 8 + z, 1)]
                flights.append(copy(rows, r4c.at[cc, py, :, pl.ds(cz, 1)], at(z=z, c=c, y=2 * y + lo)))
    r4c[cc, py, :, pl.ds(cz, 1)] = s4[py, :, pl.ds(cc * 8 + cz, 1)]
    for f in flights:
        f.wait()
    phase("y")
    x = [jnp.concatenate([r4c[0, q, i], r4c[1, q, i]], axis=0) for i in range(3) for q in range(4)]
    along = stage_y(x, ryi)

    s5[...] = along.astype(BF).reshape(2, 8, 16, 128)
    phase("e5")
    flights = []
    for d, flip in [(d, flip) for d in FAR_FIRST for flip in (1, 0)] + [(0, 1)]:
        to_x, to_lo = ring(cx, d, 8), lax.rem(lo + flip, 2)
        flights.append(copy(s5.at[to_lo, to_x], r5b.at[lo, cx], at(x=to_x, y=2 * py + to_lo)))
    r5b[lo, cx] = s5[lo, cx]
    for f in flights:
        f.wait()
    phase("x")
    wide[...] = r5b[...].astype(F32).reshape(256, 128)
    a = [wide[pl.ds(y, 16, stride=16), :] for y in range(16)]
    g = [a[12 + y % 4] if y < 4 else roll(a[12 + y % 4], 128 - 40 * (y // 4), 1) for y in range(12)]
    rho, hart, gx, gy, gzz = stage_x(a[:12], g, rxi)
    value = stage_potential(rho, hart, gx, gy, gzz)

    r6[cc, cz] = stage_block([value, gx, gy, gzz])
    phase("e6")
    chunks = (pl.ds(0, 128), pl.ds(128, 112))
    hops, relays, last, home = {}, {}, [], []

    def block(away):
        return r6.at[cc, ring(cz, away % 8, 8)]

    def go(ref, away):
        return copy(ref, ref, at(z=ring(cz, away % 8, 8)))

    def settle(away):
        last.append(copy(block(away), block(away), at(c=other)))
        for c in (cc, other):
            k = len(home)
            ref = (c, ring(cz, away % 8, 8))
            home.append(pltpu.make_async_copy(r6.at[ref], out.at[ref], store.at[k]))
        home[-2].start()

    for d in (2, -2):
        for h in (0, 1):
            hops[d, h] = go(block(0).at[chunks[h]], d)
    for d in (1, -1):
        hops[d, 0] = go(block(0), d)
    settle(0)
    for h in (0, 1):
        for way in (1, -1):
            hops[2 * way, h].wait_recv()
            got = block(-2 * way).at[chunks[h]]
            relays[3 * way, h] = go(got, way)
            if h == (1 - way) // 2:
                relays[4 * way, h] = go(got, 2 * way)
    settle(-2)
    settle(2)
    for way in (1, -1):
        hops[way, 0].wait_recv()
        settle(-way)
    for way in (1, -1):
        for h in (0, 1):
            relays[3 * way, h].wait_recv()
        settle(-3 * way)
    relays[4, 0].wait_recv()
    relays[-4, 1].wait_recv()
    settle(4)
    for k in range(8):
        last[k].wait()
        home[2 * k + 1].start()
    for f in list(hops.values()) + list(relays.values()):
        f.wait_send()
    for f in home:
        f.wait()
    phase(None)


def lay_kernel(r6, pot, grad, got, wide, woven, done, load, store):
    loads = [pltpu.make_async_copy(r6.at[c], got.at[c], load.at[c]) for c in range(2)]
    for c in loads:
        c.start()
    for c in range(2):
        loads[c].wait()
        wide[1920 * c : 1920 * c + 1920] = got[c].astype(F32).reshape(1920, 128)

    def step(y, carry):
        for k in range(4):
            for j in range(3):
                z = pl.ds(j, 16, stride=3)
                woven[k, 0, z] = wide[pl.ds(40 * k + 12 * j + y, 16, stride=240), :]
                tail = wide[pl.ds(160 + 40 * (k // 2) + 12 * j + y, 16, stride=240), :]
                woven[k, 1, z] = roll(tail, 64, 1) if k % 2 else tail
            done[k, y, :, 0:128] = woven[k, 0]
            done[k, y, :, 128:192] = woven[k, 1, :, 0:64]
        return carry

    stores = []
    for q in range(3):
        lax.fori_loop(4 * q, 4 * q + 4, step, 0)
        rows = pl.ds(4 * q, 4)
        for k in range(4):
            target = pot.at[rows] if k == 0 else grad.at[k - 1, rows]
            stores.append(pltpu.make_async_copy(done.at[k, rows], target, store.at[4 * q + k]))
            stores[-1].start()
    for c in stores:
        c.wait()


def body(orbitals, occupations, stick_map, core_density):
    tables = make_tables()
    far = pl.BlockSpec(memory_space=pltpu.HBM)
    operands = [orbitals[0], stick_map, core_density.transpose(1, 0, 2), *tables]
    scratch = [pltpu.VMEM(a.shape, a.dtype) for a in operands] + [
        pltpu.VMEM((1024, 512), BF),
        pltpu.VMEM((384, 1024), BF),
        pltpu.VMEM((8, 8, 8, 128), BF),
        pltpu.VMEM((8, 8, 8, 128), BF),
        pltpu.VMEM((8, 8, 8, 128), BF),
        pltpu.VMEM((3, 12, N), F32),
        pltpu.VMEM((3, 12, N), F32),
        pltpu.VMEM((6, 256, 256), BF),
        pltpu.VMEM((3, 256, 256), F32),
        pltpu.VMEM((3, 128, 256), F32),
        pltpu.VMEM((3, 8, 16, 256), BF),
        pltpu.VMEM((8, 3, 16, 256), BF),
        pltpu.VMEM((8, 8, 128), F32),
        pltpu.VMEM((8, 8, 128), F32),
        pltpu.VMEM((8, 8, 128), F32),
        pltpu.VMEM((4, 3, 16, 128), F32),
        pltpu.VMEM((2, 4, 3, 8, 128), F32),
        pltpu.VMEM((2, 8, 16, 128), BF),
        pltpu.VMEM((2, 8, 16, 128), BF),
        pltpu.VMEM((256, 128), F32),
        pltpu.VMEM((2, 8, 240, 128), BF),
        pltpu.SemaphoreType.DMA((180,)),
        pltpu.SemaphoreType.DMA((180,)),
        pltpu.SemaphoreType.DMA((13,)),
        pltpu.SemaphoreType.DMA((16,)),
    ]
    blocks = pl.pallas_call(
        kernel,
        out_shape=jax.ShapeDtypeStruct((2, 8, 240, 128), BF),
        in_specs=[pl.BlockSpec(memory_space=pltpu.SMEM)] + [far] * len(operands),
        out_specs=far,
        scratch_shapes=scratch,
        compiler_params=pltpu.CompilerParams(collective_id=0, has_side_effects=True, vmem_limit_bytes=67_043_328),
    )(occupations, *operands)
    pot, grad = pl.pallas_call(
        lay_kernel,
        out_shape=(
            jax.ShapeDtypeStruct((12, 48, N), F32),
            jax.ShapeDtypeStruct((3, 12, 48, N), F32),
        ),
        in_specs=[far],
        out_specs=(far, far),
        scratch_shapes=[
            pltpu.VMEM((2, 8, 240, 128), BF),
            pltpu.VMEM((3840, 128), F32),
            pltpu.VMEM((4, 2, 48, 128), F32),
            pltpu.VMEM((4, 12, 48, N), F32),
            pltpu.SemaphoreType.DMA((2,)),
            pltpu.SemaphoreType.DMA((12,)),
        ],
        compiler_params=pltpu.CompilerParams(vmem_limit_bytes=67_043_328),
    )(blocks)
    return pot.transpose(1, 0, 2), grad.transpose(0, 2, 1, 3)


def solution(mesh):
    return jax.shard_map(
        body,
        mesh=mesh,
        in_specs=(P("band", ("px", "py"), None), P("band"), P(None, "px"), P("py", "px", None)),
        out_specs=(P("py", "px", None), P(None, "py", "px", None)),
        check_vma=False,
    )
```

```python
import functools
import math

import jax
import jax.numpy as jnp
import numpy as np
from jax import lax
from jax.experimental import pallas as pl
from jax.experimental.pallas import tpu as pltpu
from jax.sharding import PartitionSpec as P

N = 192
SPACING = 0.25
KAPPA = 0.804
MU = 0.2195
SLATER = 0.75 * (3.0 / math.pi) ** (1.0 / 3.0)
REDUCED = 4.0 * (3.0 * math.pi**2) ** (2.0 / 3.0)
UNIT = 2.0 * math.pi / (N * SPACING)
F32 = jnp.float32
BF = jnp.bfloat16
MESH = pl.DeviceIdType.MESH
FAR_FIRST = (4, 3, 5, 2, 6, 1, 7)
roll = pltpu.roll


def hilo(a):
    a = np.asarray(a, np.float32)
    hi = a.astype(BF)
    lo = (a - hi.astype(np.float32)).astype(BF)
    return np.stack([hi, lo])


def real_basis():
    n = np.arange(N)
    k = np.where(n <= 96, n, n - 96)
    cosine = n <= 96
    x = np.arange(N)
    angle = 2 * np.pi * (k[:, None] * x[None, :] % N) / N
    forward = np.where(cosine[:, None], np.cos(angle), np.sin(angle))
    weight = np.where((k == 0) | (k == 96), 1.0, 2.0)
    weight = np.where(cosine, weight, 2.0) / N
    inverse = (forward * weight[:, None]).T
    g = np.where(k == 96, 0.0, k) * UNIT
    slope = np.where(cosine[:, None], -np.sin(angle), np.cos(angle)) * (g * weight)[:, None]
    return forward, inverse, slope.T, (UNIT * k) ** 2


def make_tables():
    fwd, inv, dif, q2 = real_basis()
    idx = np.arange(N)
    ang = 2 * np.pi * (idx[:, None] * idx[None, :] % N) / N
    c, s = np.cos(ang), np.sin(ang)
    ta = np.zeros((64, 8, 384))
    for j in range(3):
        z = 3 * np.arange(64) + j
        ta[:, j, :N], ta[:, j, N:] = c[z], -s[z]
        ta[:, 3 + j, :N], ta[:, 3 + j, N:] = s[z], c[z]
    xp = 16 * (idx // 12) + idx % 12
    tyc = np.zeros((256, 512))
    tyc[xp, :N], tyc[xp, 256 : 256 + N] = c, s
    band = idx // 12
    krow = 128 * (band % 2) + 16 * (band // 2) + idx % 12
    ry = np.zeros((256, 256))
    ry[krow, :N] = fwd
    px, py, i = idx // 12, (idx % 12) // 3, idx % 3
    rx = np.zeros((N, 256))
    rx[:, 64 * i + 16 * py + px] = fwd.T
    rx[:, 192] = fwd[0]
    zo = (3 * np.arange(64)[None, :] + np.arange(3)[:, None]).reshape(-1)
    rz = fwd[:, zo]
    gz = (dif @ fwd)[zo][:, zo]
    kcol = 16 * (idx % 12) + 8 * (band % 2) + band // 2
    ryi = np.zeros((2, 256, N))
    ryi[0][np.ix_(xp, kcol)] = inv
    ryi[1][np.ix_(xp, kcol)] = dif
    kx = 16 * (4 * i + py) + px
    rxi = np.zeros((N, 512))
    rxi[kx, :N] = inv.T
    rxi[kx, 256 : 256 + N] = dif.T
    qx = np.zeros((64, 1, 128), np.float32)
    qy = np.zeros((16, 1, 128), np.float32)
    for ii in range(3):
        for t in range(12):
            p = np.arange(64)
            qx[:, 0, 12 * ii + t] = q2[12 * (p % 16) + 3 * (p // 16) + ii]
            qy[:, 0, 12 * ii + t] = q2[12 * np.arange(16) + t]
    tabs = [hilo(a) for a in (ta.reshape(512, 384), tyc, ry, rx, rz, gz, ryi, rxi)]
    return tabs + [qx, qy]


def mm(a, b):
    return lax.dot_general(a, b, (((1,), (0,)), ((), ())), preferred_element_type=F32)


def mmt(a, b):
    return lax.dot_general(a, b, (((1,), (1,)), ((), ())), preferred_element_type=F32)


def split(x):
    hi = x.astype(BF)
    return hi, (x - hi.astype(F32)).astype(BF)


def mtm(a, b):
    return lax.dot_general(a, b, (((0,), (0,)), ((), ())), preferred_element_type=F32)


def mm3(a, b, dot=mm):
    return dot(a[0], b[0]) + dot(a[0], b[1]) + dot(a[1], b[0])


def stage_columns(orb, x_of, y_of, px, ta):
    out = mmt(ta[0], orb) + mmt(ta[1], orb)
    row = lax.broadcasted_iota(jnp.int32, (8, 128), 0)
    y_row = y_of + 4 * (y_of // 12)
    place = jnp.where(row == 6, (x_of - px * 12).astype(F32), jnp.where(row == 7, y_row.astype(F32), 0.0))
    return (out.reshape(64, 8, 128) + place[None]).astype(BF)


def stage_scatter(pieces):
    data = jnp.concatenate(pieces, axis=1).astype(F32)
    hot = (lax.broadcasted_iota(jnp.int32, (256, 512), 0).astype(F32) == data[7:8]).astype(F32).astype(BF)
    place = lax.broadcasted_iota(jnp.int32, (16, 512), 0).astype(F32) == data[6:7]
    rows = jnp.concatenate([jnp.where(place, data[r : r + 1], 0.0) for r in range(6)], axis=0)
    return mmt(rows.astype(BF), hot).astype(BF)


def stage_tables(tyc, ty, tx):
    for h in range(2):
        c, s = tyc[h, :, :256], tyc[h, :, 256:]
        ty[512 * h : 512 * h + 256, 0:256] = c
        ty[512 * h : 512 * h + 256, 256:512] = s
        ty[512 * h + 256 : 512 * h + 512, 0:256] = -s
        ty[512 * h + 256 : 512 * h + 512, 256:512] = c
        ct, st = (t.astype(F32).T[:N].astype(BF) for t in (c, s))
        tx[0:N, 512 * h : 512 * h + 256] = ct
        tx[0:N, 512 * h + 256 : 512 * h + 512] = -st
        tx[N : 2 * N, 512 * h : 512 * h + 256] = st
        tx[N : 2 * N, 512 * h + 256 : 512 * h + 512] = ct


def stage_density(p_re, p_im, weight, ty, tx):
    along = mm(jnp.concatenate([p_re, p_im, p_re, p_im], axis=1), ty[...]).astype(BF)
    rows = jnp.concatenate([along[:, :256], along[:, 256:]], axis=0)
    both = mm(tx[...], jnp.concatenate([rows, rows], axis=0))
    re, im = both[:N], both[N:]
    return weight * (re * re + im * im)


def stage_plane(rho, ry, rx):
    t = mm3(ry, split(rho), mmt)
    return mm3(split(t), rx)


def stage_core(core, band, ry, rx):
    core = jnp.concatenate([core, jnp.zeros((4, N), F32)], axis=0)
    part = split(mm3(split(core), rx))
    y = lax.broadcasted_iota(jnp.int32, (256, 16), 0)
    t = lax.broadcasted_iota(jnp.int32, (256, 16), 1)
    pick = jnp.where((y == 12 * band + t) & (t < 12), 1.0, 0.0).astype(BF)
    placed = [mm(pick, h).astype(BF) for h in part]
    return mm3(ry, placed)


def halves_for_wire(x):
    lane = lax.broadcasted_iota(jnp.int32, x.shape, x.ndim - 1)
    return jnp.where(lane == 192, x - x.astype(BF).astype(F32), x).astype(BF)


def stage_pack(s):
    gap = jnp.zeros((24, 256), F32)
    rows = jnp.concatenate([s[0], gap, s[1], gap, s[2], gap, gap[:8]], axis=0)
    t = rows.T
    return t[0:64] + t[192:256] + roll(t[64:128], 12, 1) + roll(t[128:192], 24, 1)


def stage_z(w, qx, qy, rz, gz):
    lane = lax.broadcasted_iota(jnp.int32, (64, 128), 1)
    inside = lane < 36
    cols = jnp.concatenate([jnp.where(inside, w if j == 0 else roll(w, 128 - 40 * j, 1), 0.0) for j in range(3)], axis=0)
    both = split(cols)
    spectrum = mm3(rz, both)
    n = lax.broadcasted_iota(jnp.int32, (N, 128), 0)
    k = jnp.where(n <= 96, n, n - 96)
    weight = jnp.where((n == 0) | (n == 96), 1.0 / N, 2.0 / N)
    squared = UNIT**2 * (k * k).astype(F32) + (qx + qy)
    factor = jnp.where(squared > 0, 4.0 * math.pi / jnp.where(squared > 0, squared, 1.0), 0.0)
    hart = mm3(rz, split(spectrum * (factor * weight)), mtm)
    slope = mm3(gz, both)
    full = cols + roll(hart, 40, 1) + roll(slope, 80, 1)
    group = jnp.where(lane % 40 < 36, lane % 40 // 12, 9)
    out = []
    for i in range(3):
        acc = jnp.zeros((64, 128), F32)
        for j in range(3):
            shift = (12 * (j - i)) % 128
            part = full[64 * j : 64 * j + 64]
            acc = jnp.where(group == j, roll(part, shift, 1) if shift else part, acc)
        out.append(acc)
    return out


def swap_minor(x):
    lane = lax.broadcasted_iota(jnp.int32, (16, 128), 1)
    moved = [x[u] if u == 0 else roll(x[u], u, 1) for u in range(12)]
    out = []
    for v in range(12):
        at = lane - v
        at = jnp.where((at >= 0) & (at < 120) & (at % 40 < 36), at % 40 % 12, 99)
        acc = jnp.zeros((16, 128), F32)
        for u in range(12):
            acc = jnp.where(at == u, moved[u], acc)
        out.append(acc if v == 0 else roll(acc, 128 - v, 1))
    return out


def stage_y(x, ryi):
    cols = split(jnp.concatenate(swap_minor(x), axis=0))
    along, slope = mm3((ryi[0][0], ryi[1][0]), cols), mm3((ryi[0][1], ryi[1][1]), cols)
    row = lax.broadcasted_iota(jnp.int32, (256, 128), 0) % 16
    lane = lax.broadcasted_iota(jnp.int32, (256, 128), 1)
    spare = roll(jnp.where(lane < 36, slope, 0.0), 12, 0)
    for h in (1, 2):
        moved = roll(roll(slope, 12 - 4 * h, 0), 40 * h, 1)
        spare = jnp.where((lane >= 40 * h) & (lane < 40 * h + 36), moved, spare)
    return jnp.where(row < 12, along, spare)


def stage_x(a, g, rxi):
    fill = jnp.zeros((64, 128), F32)
    f = jnp.concatenate(swap_minor(a) + [fill], axis=0).T[:, :N].astype(BF)
    s = jnp.concatenate(swap_minor(g) + [fill], axis=0).T[:, :N].astype(BF)
    both = mm(f, rxi[0]) + mm(f, rxi[1])
    gy = mm(s[0:64], rxi[0][:, :256]) + mm(s[0:64], rxi[1][:, :256])
    return both[0:40, :256], both[40:80, :256], both[0:40, 256:], gy[0:40], both[80:120, :256]


def stage_potential(rho, hart, gx, gy, gz):
    rho = jnp.where(rho > 0, rho, 1.0)
    cube_root = jnp.exp(jnp.log(rho) * (1.0 / 3.0))
    four = rho * cube_root
    reduced = (gx * gx + gy * gy + gz * gz) / (REDUCED * four * four)
    inverse = 1.0 / (1.0 + MU * reduced / KAPPA)
    enhance = 1.0 + KAPPA - KAPPA * inverse
    slope = MU * inverse * inverse
    return hart - SLATER * cube_root * ((4.0 / 3.0) * enhance - (8.0 / 3.0) * reduced * slope)


def stage_block(fields):
    lane = lax.broadcasted_iota(jnp.int32, (40, 128), 1)
    rows = [f[:, :128] for f in fields]
    for k in (0, 2):
        rows.append(jnp.where(lane < 64, fields[k][:, 128:], roll(fields[k + 1][:, 128:], 64, 1)))
    return jnp.concatenate(rows, axis=0).astype(BF)


def kernel(
    occ, *rest,
):
    far, rest = rest[:13], rest[13:]
    out, near, rest = rest[0], rest[1:14], rest[14:]
    orb, sticks, core, ta, tyc, ry, rx, rz, gz, ryi, rxi, qx, qy = near
    (
    ty, tx, s1, r1a, r1b, core_out, core_in, planes, part, r2a, sums, r2b, s3, r3b, s4, r4c,
    s5, r5b, wide, r6, send, recv, load, store,
    ) = rest
    band, px, py = lax.axis_index("band"), lax.axis_index("px"), lax.axis_index("py")
    cz, cc = band // 2, band % 2
    cx, lo = px % 8, px // 8
    cy = 2 * py + lo

    def at(z=None, c=None, x=None, y=None):
        z, c = cz if z is None else z, cc if c is None else c
        x, y = cx if x is None else x, cy if y is None else y
        return (z * 2 + c, (y % 2) * 8 + x, y // 2)

    open_scope = [None]

    def phase(name):
        if open_scope[0] is not None:
            open_scope[0].__exit__(None, None, None)
        open_scope[0] = jax.named_scope(name) if name else None
        if name:
            open_scope[0].__enter__()

    def ring(me, d, n):
        return lax.rem(me + d, n)

    bar = pltpu.get_barrier_semaphore()

    def hail(target):
        pl.semaphore_signal(bar, inc=1, device_id=target, device_id_type=MESH)

    swapped = (px, band, py)
    for d in range(1, 8):
        hail(at(x=ring(cx, d, 8)))
        hail(at(y=ring(cy, d, 8)))
        hail(at(z=ring(cz, d, 8)))
    hail(at(c=1 - cc))

    @pl.when(band != px)
    def _():
        hail(swapped)

    loads = {}
    for k in (0, 1, 3, 2, 4, 5, 6, 7, 8, 9, 10, 11, 12):
        loads[k] = pltpu.make_async_copy(far[k], near[k], load.at[k])
        loads[k].start()
    count = [0]

    def copy(src, dst, target, k=None):
        if k is None:
            k = count[0]
            count[0] += 1
        c = pltpu.make_async_remote_copy(
            src_ref=src, dst_ref=dst, send_sem=send.at[k], recv_sem=recv.at[k],
            device_id=target, device_id_type=MESH,
        )
        c.start()
        return c

    phase("columns")
    for k in (0, 1, 3):
        loads[k].wait()
    mine = pl.ds(pl.multiple_of(py * 128, 128), 128)
    s1[...] = stage_columns(orb[...], sticks[0:1, mine], sticks[1:2, mine], px, ta).reshape(8, 8, 8, 128)
    loads[2].wait()
    for j in range(3):
        core_out[j] = core[:, pl.ds(3 * band + j, 1)].reshape(12, N)
    phase("barrier")
    pl.semaphore_wait(bar, 22 + jnp.where(band != px, 1, 0))

    phase("e1_y")
    x_own = 4 * (cx // 4)
    x_far = 4 - x_own
    firsts = []
    for start in (x_far, x_own):
        cut = pl.ds(start, 4)
        firsts.append([copy(s1.at[ring(cy, d, 8), cut], r1a.at[cy, cut], at(y=ring(cy, d, 8))) for d in FAR_FIRST])
    core_copy = pltpu.make_async_remote_copy(
        src_ref=core_out, dst_ref=core_in, send_sem=send.at[239], recv_sem=recv.at[239],
        device_id=swapped, device_id_type=MESH,
    )

    @pl.when(band != px)
    def _():
        core_copy.start()

    @pl.when(band == px)
    def _():
        core_in[...] = core_out[...]

    r1a[cy] = s1[cy]
    for k in (4, 5, 6):
        loads[k].wait()
    stage_tables(tyc, ty, tx)
    arrival = count[0] - 1
    count[0] += 7
    flights = []
    for h, start in enumerate((x_far, x_own)):
        for f in firsts[h]:
            f.wait()
        phase("e1_x_core" if h else "e1_x_far")
        for m in (2, 1, 3, 0)[: 4 - h]:
            x = start + lax.rem(cx + m, 4)
            d = lax.rem(x + 8 - cx, 8)
            flights.append(copy(r1a.at[:, x], r1b.at[:, cx], at(x=x), arrival + d))
    for y in range(8):
        r1b[y, cx] = r1a[y, cx]

    @pl.when(band != px)
    def _():
        core_copy.wait()

    def core_step(j, carry):
        part[j] = stage_core(core_in[j], band, ry, rx)
        return carry

    lax.fori_loop(0, 3, core_step, 0)
    phase("scatter")
    def scatter_step(q, carry):
        odd = q % 2
        d = odd * ((q + 1) // 2) + (1 - odd) * (8 - q // 2)
        source = lax.rem(cx + 8 - d, 8)

        @pl.when(q > 0)
        def _():
            pltpu.make_async_remote_copy(
                src_ref=r1a.at[:, source], dst_ref=r1b.at[:, source],
                send_sem=send.at[arrival + d], recv_sem=recv.at[arrival + d],
                device_id=at(x=source), device_id_type=MESH,
            ).wait_recv()

        for l in range(2):
            block = stage_scatter([r1b[2 * q4 + l, source] for q4 in range(4)])
            row = pl.ds(pl.multiple_of(128 * l + source * 16, 16), 16)
            for r in range(6):
                planes[r, row, :] = block[16 * r : 16 * r + 16]
        return carry

    lax.fori_loop(0, 8, scatter_step, 0)
    for f in flights:
        f.wait_send()

    other = 1 - cc
    flights, pairs = [], []

    def spread(j):
        pairs[j].wait()
        total = part[j, pl.ds(pl.multiple_of(cc * 128, 128), 128)] + r2a[j]
        sums[j] = halves_for_wire(total).reshape(8, 16, 256)
        for d in FAR_FIRST:
            z = ring(cz, d, 8)
            flights.append(copy(sums.at[j, z], r2b.at[cz, j], at(z=z)))
        r2b[cz, j] = sums[j, cz]

    for j in range(3):
        phase(f"plane{j}")
        rho = stage_density(planes[j], planes[3 + j], occ[0], ty, tx)
        part[j] = part[j] + stage_plane(rho, ry, rx)
        pairs.append(copy(part.at[j, pl.ds(pl.multiple_of(other * 128, 128), 128)], r2a.at[j], at(c=other)))
        if j > 0:
            phase(f"spread{j}")
            spread(j - 1)
    phase("spread3")
    spread(2)
    phase("e2_z")
    for f in flights:
        f.wait()
    acc = r2b[0].astype(F32)
    for z in range(1, 8):
        acc = acc + r2b[z].astype(F32)

    phase("pack")
    s3[...] = stage_pack(acc).reshape(8, 8, 128)
    phase("e3")
    flights = []
    for e in FAR_FIRST + (0,):
        for d in FAR_FIRST + (0,):
            if e or d:
                y, x = ring(cy, e, 8), ring(cx, d, 8)
                flights.append(copy(s3.at[y, pl.ds(x, 1)], r3b.at[cy, pl.ds(cx, 1)], at(x=x, y=y)))
    r3b[cy, pl.ds(cx, 1)] = s3[cy, pl.ds(cx, 1)]
    for f in flights:
        f.wait()
    for k in (7, 8, 9, 10, 11, 12):
        loads[k].wait()
    turned = stage_z(r3b[...].reshape(64, 128), qx[py * 16 + px], qy[band], rz, gz)

    phase("e4")
    for i in range(3):
        s4[:, i] = turned[i].reshape(4, 16, 128)
    flights = []
    for e in (2, 1, 3, 0):
        y = ring(py, e, 4)
        for d, flip in [(d, flip) for d in FAR_FIRST + (0,) for flip in (1, 0)]:
            if e or d or flip:
                z, c = ring(cz, d, 8), lax.rem(cc + flip, 2)
                rows = s4.at[y, :, pl.ds(c * 8 + z, 1)]
                flights.append(copy(rows, r4c.at[cc, py, :, pl.ds(cz, 1)], at(z=z, c=c, y=2 * y + lo)))
    r4c[cc, py, :, pl.ds(cz, 1)] = s4[py, :, pl.ds(cc * 8 + cz, 1)]
    for f in flights:
        f.wait()
    phase("y")
    x = [jnp.concatenate([r4c[0, q, i], r4c[1, q, i]], axis=0) for i in range(3) for q in range(4)]
    along = stage_y(x, ryi)

    s5[...] = along.astype(BF).reshape(2, 8, 16, 128)
    phase("e5")
    flights = []
    for d, flip in [(d, flip) for d in FAR_FIRST for flip in (1, 0)] + [(0, 1)]:
        to_x, to_lo = ring(cx, d, 8), lax.rem(lo + flip, 2)
        flights.append(copy(s5.at[to_lo, to_x], r5b.at[lo, cx], at(x=to_x, y=2 * py + to_lo)))
    r5b[lo, cx] = s5[lo, cx]
    for f in flights:
        f.wait()
    phase("x")
    wide[...] = r5b[...].astype(F32).reshape(256, 128)
    a = [wide[pl.ds(y, 16, stride=16), :] for y in range(16)]
    g = [a[12 + y % 4] if y < 4 else roll(a[12 + y % 4], 128 - 40 * (y // 4), 1) for y in range(12)]
    rho, hart, gx, gy, gzz = stage_x(a[:12], g, rxi)
    value = stage_potential(rho, hart, gx, gy, gzz)

    r6[cc, cz] = stage_block([value, gx, gy, gzz])
    phase("e6")
    chunks = (pl.ds(0, 128), pl.ds(128, 112))
    hops, relays, last, home = {}, {}, [], []

    def block(away):
        return r6.at[cc, ring(cz, away % 8, 8)]

    def go(ref, away):
        return copy(ref, ref, at(z=ring(cz, away % 8, 8)))

    def settle(away):
        last.append(copy(block(away), block(away), at(c=other)))
        for c in (cc, other):
            k = len(home)
            ref = (c, ring(cz, away % 8, 8))
            home.append(pltpu.make_async_copy(r6.at[ref], out.at[ref], store.at[k]))
        home[-2].start()

    for d in (2, -2):
        for h in (0, 1):
            hops[d, h] = go(block(0).at[chunks[h]], d)
    for d in (1, -1):
        hops[d, 0] = go(block(0), d)
    settle(0)
    for h in (0, 1):
        for way in (1, -1):
            hops[2 * way, h].wait_recv()
            got = block(-2 * way).at[chunks[h]]
            relays[3 * way, h] = go(got, way)
            if h == (1 - way) // 2:
                relays[4 * way, h] = go(got, 2 * way)
    settle(-2)
    settle(2)
    for way in (1, -1):
        hops[way, 0].wait_recv()
        settle(-way)
    for way in (1, -1):
        for h in (0, 1):
            relays[3 * way, h].wait_recv()
        settle(-3 * way)
    relays[4, 0].wait_recv()
    relays[-4, 1].wait_recv()
    settle(4)
    for k in range(8):
        last[k].wait()
        home[2 * k + 1].start()
    for f in list(hops.values()) + list(relays.values()):
        f.wait_send()
    for f in home:
        f.wait()
    phase(None)


def lay_kernel(r6, pot, grad, got, wide, woven, done, load, store):
    loads = [pltpu.make_async_copy(r6.at[c], got.at[c], load.at[c]) for c in range(2)]
    for c in loads:
        c.start()
    for c in range(2):
        loads[c].wait()
        wide[1920 * c : 1920 * c + 1920] = got[c].astype(F32).reshape(1920, 128)

    def step(y, carry):
        for k in range(4):
            for j in range(3):
                z = pl.ds(j, 16, stride=3)
                woven[k, 0, z] = wide[pl.ds(40 * k + 12 * j + y, 16, stride=240), :]
                tail = wide[pl.ds(160 + 40 * (k // 2) + 12 * j + y, 16, stride=240), :]
                woven[k, 1, z] = roll(tail, 64, 1) if k % 2 else tail
            done[k, y, :, 0:128] = woven[k, 0]
            done[k, y, :, 128:192] = woven[k, 1, :, 0:64]
        return carry

    stores = []
    for q in range(3):
        lax.fori_loop(4 * q, 4 * q + 4, step, 0)
        rows = pl.ds(4 * q, 4)
        for k in range(4):
            target = pot.at[rows] if k == 0 else grad.at[k - 1, rows]
            stores.append(pltpu.make_async_copy(done.at[k, rows], target, store.at[4 * q + k]))
            stores[-1].start()
    for c in stores:
        c.wait()


def body(orbitals, occupations, stick_map, core_density):
    tables = make_tables()
    far = pl.BlockSpec(memory_space=pltpu.HBM)
    operands = [orbitals[0], stick_map, core_density.transpose(1, 0, 2), *tables]
    scratch = [pltpu.VMEM(a.shape, a.dtype) for a in operands] + [
        pltpu.VMEM((1024, 512), BF),
        pltpu.VMEM((384, 1024), BF),
        pltpu.VMEM((8, 8, 8, 128), BF),
        pltpu.VMEM((8, 8, 8, 128), BF),
        pltpu.VMEM((8, 8, 8, 128), BF),
        pltpu.VMEM((3, 12, N), F32),
        pltpu.VMEM((3, 12, N), F32),
        pltpu.VMEM((6, 256, 256), BF),
        pltpu.VMEM((3, 256, 256), F32),
        pltpu.VMEM((3, 128, 256), F32),
        pltpu.VMEM((3, 8, 16, 256), BF),
        pltpu.VMEM((8, 3, 16, 256), BF),
        pltpu.VMEM((8, 8, 128), F32),
        pltpu.VMEM((8, 8, 128), F32),
        pltpu.VMEM((4, 3, 16, 128), F32),
        pltpu.VMEM((2, 4, 3, 8, 128), F32),
        pltpu.VMEM((2, 8, 16, 128), BF),
        pltpu.VMEM((2, 8, 16, 128), BF),
        pltpu.VMEM((256, 128), F32),
        pltpu.VMEM((2, 8, 240, 128), BF),
        pltpu.SemaphoreType.DMA((240,)),
        pltpu.SemaphoreType.DMA((240,)),
        pltpu.SemaphoreType.DMA((13,)),
        pltpu.SemaphoreType.DMA((16,)),
    ]
    blocks = pl.pallas_call(
        kernel,
        out_shape=jax.ShapeDtypeStruct((2, 8, 240, 128), BF),
        in_specs=[pl.BlockSpec(memory_space=pltpu.SMEM)] + [far] * len(operands),
        out_specs=far,
        scratch_shapes=scratch,
        compiler_params=pltpu.CompilerParams(collective_id=0, has_side_effects=True, vmem_limit_bytes=67_043_328),
    )(occupations, *operands)
    pot, grad = pl.pallas_call(
        lay_kernel,
        out_shape=(
            jax.ShapeDtypeStruct((12, 48, N), F32),
            jax.ShapeDtypeStruct((3, 12, 48, N), F32),
        ),
        in_specs=[far],
        out_specs=(far, far),
        scratch_shapes=[
            pltpu.VMEM((2, 8, 240, 128), BF),
            pltpu.VMEM((3840, 128), F32),
            pltpu.VMEM((4, 2, 48, 128), F32),
            pltpu.VMEM((4, 12, 48, N), F32),
            pltpu.SemaphoreType.DMA((2,)),
            pltpu.SemaphoreType.DMA((12,)),
        ],
        compiler_params=pltpu.CompilerParams(vmem_limit_bytes=67_043_328),
    )(blocks)
    return pot.transpose(1, 0, 2), grad.transpose(0, 2, 1, 3)


def solution(mesh):
    return jax.shard_map(
        body,
        mesh=mesh,
        in_specs=(P("band", ("px", "py"), None), P("band"), P(None, "px"), P("py", "px", None)),
        out_specs=(P("py", "px", None), P(None, "py", "px", None)),
        check_vma=False,
    )
```

```python
import functools
import math

import jax
import jax.numpy as jnp
import numpy as np
from jax import lax
from jax.experimental import pallas as pl
from jax.experimental.pallas import tpu as pltpu
from jax.sharding import PartitionSpec as P

N = 192
SPACING = 0.25
KAPPA = 0.804
MU = 0.2195
SLATER = 0.75 * (3.0 / math.pi) ** (1.0 / 3.0)
REDUCED = 4.0 * (3.0 * math.pi**2) ** (2.0 / 3.0)
UNIT = 2.0 * math.pi / (N * SPACING)
F32 = jnp.float32
BF = jnp.bfloat16
MESH = pl.DeviceIdType.MESH
FAR_FIRST = (4, 3, 5, 2, 6, 1, 7)
roll = pltpu.roll


def hilo(a):
    a = np.asarray(a, np.float32)
    hi = a.astype(BF)
    lo = (a - hi.astype(np.float32)).astype(BF)
    return np.stack([hi, lo])


def real_basis():
    n = np.arange(N)
    k = np.where(n <= 96, n, n - 96)
    cosine = n <= 96
    x = np.arange(N)
    angle = 2 * np.pi * (k[:, None] * x[None, :] % N) / N
    forward = np.where(cosine[:, None], np.cos(angle), np.sin(angle))
    weight = np.where((k == 0) | (k == 96), 1.0, 2.0)
    weight = np.where(cosine, weight, 2.0) / N
    inverse = (forward * weight[:, None]).T
    g = np.where(k == 96, 0.0, k) * UNIT
    slope = np.where(cosine[:, None], -np.sin(angle), np.cos(angle)) * (g * weight)[:, None]
    return forward, inverse, slope.T, (UNIT * k) ** 2


def make_tables():
    fwd, inv, dif, q2 = real_basis()
    idx = np.arange(N)
    ang = 2 * np.pi * (idx[:, None] * idx[None, :] % N) / N
    c, s = np.cos(ang), np.sin(ang)
    ta = np.zeros((64, 8, 384))
    for j in range(3):
        z = 3 * np.arange(64) + j
        ta[:, j, :N], ta[:, j, N:] = c[z], -s[z]
        ta[:, 3 + j, :N], ta[:, 3 + j, N:] = s[z], c[z]
    xp = 16 * (idx // 12) + idx % 12
    tyc = np.zeros((256, 512))
    tyc[xp, :N], tyc[xp, 256 : 256 + N] = c, s
    band = idx // 12
    krow = 128 * (band % 2) + 16 * (band // 2) + idx % 12
    ry = np.zeros((256, 256))
    ry[krow, :N] = fwd
    px, py, i = idx // 12, (idx % 12) // 3, idx % 3
    rx = np.zeros((N, 256))
    rx[:, 64 * i + 16 * py + px] = fwd.T
    rx[:, 192] = fwd[0]
    zo = (3 * np.arange(64)[None, :] + np.arange(3)[:, None]).reshape(-1)
    rz = fwd[:, zo]
    gz = (dif @ fwd)[zo][:, zo]
    kcol = 16 * (idx % 12) + 8 * (band % 2) + band // 2
    ryi = np.zeros((2, 256, N))
    ryi[0][np.ix_(xp, kcol)] = inv
    ryi[1][np.ix_(xp, kcol)] = dif
    kx = 16 * (4 * i + py) + px
    rxi = np.zeros((N, 512))
    rxi[kx, :N] = inv.T
    rxi[kx, 256 : 256 + N] = dif.T
    qx = np.zeros((64, 1, 128), np.float32)
    qy = np.zeros((16, 1, 128), np.float32)
    for ii in range(3):
        for t in range(12):
            p = np.arange(64)
            qx[:, 0, 12 * ii + t] = q2[12 * (p % 16) + 3 * (p // 16) + ii]
            qy[:, 0, 12 * ii + t] = q2[12 * np.arange(16) + t]
    tabs = [hilo(a) for a in (ta.reshape(512, 384), tyc, ry, rx, rz, gz, ryi, rxi)]
    return tabs + [qx, qy]


def mm(a, b):
    return lax.dot_general(a, b, (((1,), (0,)), ((), ())), preferred_element_type=F32)


def mmt(a, b):
    return lax.dot_general(a, b, (((1,), (1,)), ((), ())), preferred_element_type=F32)


def split(x):
    hi = x.astype(BF)
    return hi, (x - hi.astype(F32)).astype(BF)


def mtm(a, b):
    return lax.dot_general(a, b, (((0,), (0,)), ((), ())), preferred_element_type=F32)


def mm3(a, b, dot=mm):
    return dot(a[0], b[0]) + dot(a[0], b[1]) + dot(a[1], b[0])


def stage_columns(orb, x_of, y_of, px, ta):
    out = mmt(ta[0], orb) + mmt(ta[1], orb)
    row = lax.broadcasted_iota(jnp.int32, (8, 128), 0)
    y_row = y_of + 4 * (y_of // 12)
    place = jnp.where(row == 6, (x_of - px * 12).astype(F32), jnp.where(row == 7, y_row.astype(F32), 0.0))
    return (out.reshape(64, 8, 128) + place[None]).astype(BF)


def stage_scatter(pieces):
    data = jnp.concatenate(pieces, axis=1).astype(F32)
    hot = (lax.broadcasted_iota(jnp.int32, (256, 512), 0).astype(F32) == data[7:8]).astype(F32).astype(BF)
    place = lax.broadcasted_iota(jnp.int32, (16, 512), 0).astype(F32) == data[6:7]
    rows = jnp.concatenate([jnp.where(place, data[r : r + 1], 0.0) for r in range(6)], axis=0)
    return mmt(rows.astype(BF), hot).astype(BF)


def stage_tables(tyc, ty, tx):
    for h in range(2):
        c, s = tyc[h, :, :256], tyc[h, :, 256:]
        ty[512 * h : 512 * h + 256, 0:256] = c
        ty[512 * h : 512 * h + 256, 256:512] = s
        ty[512 * h + 256 : 512 * h + 512, 0:256] = -s
        ty[512 * h + 256 : 512 * h + 512, 256:512] = c
        ct, st = (t.astype(F32).T[:N].astype(BF) for t in (c, s))
        tx[0:N, 512 * h : 512 * h + 256] = ct
        tx[0:N, 512 * h + 256 : 512 * h + 512] = -st
        tx[N : 2 * N, 512 * h : 512 * h + 256] = st
        tx[N : 2 * N, 512 * h + 256 : 512 * h + 512] = ct


def stage_density(p_re, p_im, weight, ty, tx):
    along = mm(jnp.concatenate([p_re, p_im, p_re, p_im], axis=1), ty[...]).astype(BF)
    rows = jnp.concatenate([along[:, :256], along[:, 256:]], axis=0)
    both = mm(tx[...], jnp.concatenate([rows, rows], axis=0))
    re, im = both[:N], both[N:]
    return weight * (re * re + im * im)


def stage_plane(rho, ry, rx):
    t = mm3(ry, split(rho), mmt)
    return mm3(split(t), rx)


def stage_core(core, band, ry, rx):
    core = jnp.concatenate([core, jnp.zeros((4, N), F32)], axis=0)
    part = split(mm3(split(core), rx))
    y = lax.broadcasted_iota(jnp.int32, (256, 16), 0)
    t = lax.broadcasted_iota(jnp.int32, (256, 16), 1)
    pick = jnp.where((y == 12 * band + t) & (t < 12), 1.0, 0.0).astype(BF)
    placed = [mm(pick, h).astype(BF) for h in part]
    return mm3(ry, placed)


def halves_for_wire(x):
    lane = lax.broadcasted_iota(jnp.int32, x.shape, x.ndim - 1)
    return jnp.where(lane == 192, x - x.astype(BF).astype(F32), x).astype(BF)


def stage_pack(s):
    gap = jnp.zeros((24, 256), F32)
    rows = jnp.concatenate([s[0], gap, s[1], gap, s[2], gap, gap[:8]], axis=0)
    t = rows.T
    return t[0:64] + t[192:256] + roll(t[64:128], 12, 1) + roll(t[128:192], 24, 1)


def stage_z(w, qx, qy, rz, gz):
    lane = lax.broadcasted_iota(jnp.int32, (64, 128), 1)
    inside = lane < 36
    cols = jnp.concatenate([jnp.where(inside, w if j == 0 else roll(w, 128 - 40 * j, 1), 0.0) for j in range(3)], axis=0)
    both = split(cols)
    spectrum = mm3(rz, both)
    n = lax.broadcasted_iota(jnp.int32, (N, 128), 0)
    k = jnp.where(n <= 96, n, n - 96)
    weight = jnp.where((n == 0) | (n == 96), 1.0 / N, 2.0 / N)
    squared = UNIT**2 * (k * k).astype(F32) + (qx + qy)
    factor = jnp.where(squared > 0, 4.0 * math.pi / jnp.where(squared > 0, squared, 1.0), 0.0)
    hart = mm3(rz, split(spectrum * (factor * weight)), mtm)
    slope = mm3(gz, both)
    full = cols + roll(hart, 40, 1) + roll(slope, 80, 1)
    group = jnp.where(lane % 40 < 36, lane % 40 // 12, 9)
    out = []
    for i in range(3):
        acc = jnp.zeros((64, 128), F32)
        for j in range(3):
            shift = (12 * (j - i)) % 128
            part = full[64 * j : 64 * j + 64]
            acc = jnp.where(group == j, roll(part, shift, 1) if shift else part, acc)
        out.append(acc)
    return out


def swap_minor(x):
    lane = lax.broadcasted_iota(jnp.int32, (16, 128), 1)
    moved = [x[u] if u == 0 else roll(x[u], u, 1) for u in range(12)]
    out = []
    for v in range(12):
        at = lane - v
        at = jnp.where((at >= 0) & (at < 120) & (at % 40 < 36), at % 40 % 12, 99)
        acc = jnp.zeros((16, 128), F32)
        for u in range(12):
            acc = jnp.where(at == u, moved[u], acc)
        out.append(acc if v == 0 else roll(acc, 128 - v, 1))
    return out


def stage_y(x, ryi):
    cols = split(jnp.concatenate(swap_minor(x), axis=0))
    along, slope = mm3((ryi[0][0], ryi[1][0]), cols), mm3((ryi[0][1], ryi[1][1]), cols)
    row = lax.broadcasted_iota(jnp.int32, (256, 128), 0) % 16
    lane = lax.broadcasted_iota(jnp.int32, (256, 128), 1)
    spare = roll(jnp.where(lane < 36, slope, 0.0), 12, 0)
    for h in (1, 2):
        moved = roll(roll(slope, 12 - 4 * h, 0), 40 * h, 1)
        spare = jnp.where((lane >= 40 * h) & (lane < 40 * h + 36), moved, spare)
    return jnp.where(row < 12, along, spare)


def stage_x(a, g, rxi):
    fill = jnp.zeros((64, 128), F32)
    f = jnp.concatenate(swap_minor(a) + [fill], axis=0).T[:, :N].astype(BF)
    s = jnp.concatenate(swap_minor(g) + [fill], axis=0).T[:, :N].astype(BF)
    both = mm(f, rxi[0]) + mm(f, rxi[1])
    gy = mm(s[0:64], rxi[0][:, :256]) + mm(s[0:64], rxi[1][:, :256])
    return both[0:40, :256], both[40:80, :256], both[0:40, 256:], gy[0:40], both[80:120, :256]


def stage_potential(rho, hart, gx, gy, gz):
    rho = jnp.where(rho > 0, rho, 1.0)
    cube_root = jnp.exp(jnp.log(rho) * (1.0 / 3.0))
    four = rho * cube_root
    reduced = (gx * gx + gy * gy + gz * gz) / (REDUCED * four * four)
    inverse = 1.0 / (1.0 + MU * reduced / KAPPA)
    enhance = 1.0 + KAPPA - KAPPA * inverse
    slope = MU * inverse * inverse
    return hart - SLATER * cube_root * ((4.0 / 3.0) * enhance - (8.0 / 3.0) * reduced * slope)


def stage_block(fields):
    lane = lax.broadcasted_iota(jnp.int32, (40, 128), 1)
    rows = [f[:, :128] for f in fields]
    for k in (0, 2):
        rows.append(jnp.where(lane < 64, fields[k][:, 128:], roll(fields[k + 1][:, 128:], 64, 1)))
    return jnp.concatenate(rows, axis=0).astype(BF)


def kernel(
    occ, *rest,
):
    far, rest = rest[:13], rest[13:]
    out, near, rest = rest[0], rest[1:14], rest[14:]
    orb, sticks, core, ta, tyc, ry, rx, rz, gz, ryi, rxi, qx, qy = near
    (
    ty, tx, s1, r1a, r1b, core_out, core_in, planes, part, r2a, sums, r2b, s3, r3a, r3b, s4, r4c,
    s5, r5b, wide, r6, send, recv, load, store,
    ) = rest
    band, px, py = lax.axis_index("band"), lax.axis_index("px"), lax.axis_index("py")
    cz, cc = band // 2, band % 2
    cx, lo = px % 8, px // 8
    cy = 2 * py + lo

    def at(z=None, c=None, x=None, y=None):
        z, c = cz if z is None else z, cc if c is None else c
        x, y = cx if x is None else x, cy if y is None else y
        return (z * 2 + c, (y % 2) * 8 + x, y // 2)

    open_scope = [None]

    def phase(name):
        if open_scope[0] is not None:
            open_scope[0].__exit__(None, None, None)
        open_scope[0] = jax.named_scope(name) if name else None
        if name:
            open_scope[0].__enter__()

    def ring(me, d, n):
        return lax.rem(me + d, n)

    bar = pltpu.get_barrier_semaphore()

    def hail(target):
        pl.semaphore_signal(bar, inc=1, device_id=target, device_id_type=MESH)

    swapped = (px, band, py)
    for d in range(1, 8):
        hail(at(x=ring(cx, d, 8)))
        hail(at(y=ring(cy, d, 8)))
        hail(at(z=ring(cz, d, 8)))
    hail(at(c=1 - cc))

    @pl.when(band != px)
    def _():
        hail(swapped)

    loads = {}
    for k in range(13):
        loads[k] = pltpu.make_async_copy(far[k], near[k], load.at[k])
    for k in (0, 3, 1, 2):
        loads[k].start()
    count = [0]

    def copy(src, dst, target, k=None):
        if k is None:
            k = count[0]
            count[0] += 1
        c = pltpu.make_async_remote_copy(
            src_ref=src, dst_ref=dst, send_sem=send.at[k], recv_sem=recv.at[k],
            device_id=target, device_id_type=MESH,
        )
        c.start()
        return c

    phase("columns")
    for k in (0, 1, 3):
        loads[k].wait()
    mine = pl.ds(pl.multiple_of(py * 128, 128), 128)
    s1[...] = stage_columns(orb[...], sticks[0:1, mine], sticks[1:2, mine], px, ta).reshape(8, 8, 8, 128)
    for k in range(4, 13):
        loads[k].start()
    loads[2].wait()
    for j in range(3):
        core_out[j] = core[:, pl.ds(3 * band + j, 1)].reshape(12, N)
    phase("barrier")
    pl.semaphore_wait(bar, 22 + jnp.where(band != px, 1, 0))

    phase("e1_y")
    x_own = 4 * (cx // 4)
    x_far = 4 - x_own
    firsts = []
    for start in (x_far, x_own):
        cut = pl.ds(start, 4)
        firsts.append([copy(s1.at[ring(cy, d, 8), cut], r1a.at[cy, cut], at(y=ring(cy, d, 8))) for d in FAR_FIRST])
    core_copy = pltpu.make_async_remote_copy(
        src_ref=core_out, dst_ref=core_in, send_sem=send.at[179], recv_sem=recv.at[179],
        device_id=swapped, device_id_type=MESH,
    )

    @pl.when(band != px)
    def _():
        core_copy.start()

    @pl.when(band == px)
    def _():
        core_in[...] = core_out[...]

    r1a[cy] = s1[cy]
    for k in (4, 5, 6):
        loads[k].wait()
    stage_tables(tyc, ty, tx)
    arrival = count[0] - 1
    count[0] += 7
    flights = []
    for h, start in enumerate((x_far, x_own)):
        for f in firsts[h]:
            f.wait()
        phase("e1_x_core" if h else "e1_x_far")
        for m in (2, 1, 3, 0)[: 4 - h]:
            x = start + lax.rem(cx + m, 4)
            d = lax.rem(x + 8 - cx, 8)
            flights.append(copy(r1a.at[:, x], r1b.at[:, cx], at(x=x), arrival + d))
    for y in range(8):
        r1b[y, cx] = r1a[y, cx]

    @pl.when(band != px)
    def _():
        core_copy.wait()

    def core_step(j, carry):
        part[j] = stage_core(core_in[j], band, ry, rx)
        return carry

    lax.fori_loop(0, 3, core_step, 0)
    phase("scatter")
    def scatter_step(q, carry):
        odd = q % 2
        d = odd * ((q + 1) // 2) + (1 - odd) * (8 - q // 2)
        source = lax.rem(cx + 8 - d, 8)

        @pl.when(q > 0)
        def _():
            pltpu.make_async_remote_copy(
                src_ref=r1a.at[:, source], dst_ref=r1b.at[:, source],
                send_sem=send.at[arrival + d], recv_sem=recv.at[arrival + d],
                device_id=at(x=source), device_id_type=MESH,
            ).wait_recv()

        for l in range(2):
            block = stage_scatter([r1b[2 * q4 + l, source] for q4 in range(4)])
            row = pl.ds(pl.multiple_of(128 * l + source * 16, 16), 16)
            for r in range(6):
                planes[r, row, :] = block[16 * r : 16 * r + 16]
        return carry

    lax.fori_loop(0, 8, scatter_step, 0)
    for f in flights:
        f.wait_send()

    other = 1 - cc
    flights, pairs = [], []

    def spread(j):
        pairs[j].wait()
        total = part[j, pl.ds(pl.multiple_of(cc * 128, 128), 128)] + r2a[j]
        sums[j] = halves_for_wire(total).reshape(8, 16, 256)
        for d in FAR_FIRST:
            z = ring(cz, d, 8)
            flights.append(copy(sums.at[j, z], r2b.at[cz, j], at(z=z)))
        r2b[cz, j] = sums[j, cz]

    for j in range(3):
        phase(f"plane{j}")
        rho = stage_density(planes[j], planes[3 + j], occ[0], ty, tx)
        part[j] = part[j] + stage_plane(rho, ry, rx)
        pairs.append(copy(part.at[j, pl.ds(pl.multiple_of(other * 128, 128), 128)], r2a.at[j], at(c=other)))
        if j > 0:
            phase(f"spread{j}")
            spread(j - 1)
    phase("spread3")
    spread(2)
    phase("e2_z")
    for f in flights:
        f.wait()
    acc = r2b[0].astype(F32)
    for z in range(1, 8):
        acc = acc + r2b[z].astype(F32)

    phase("pack")
    s3[...] = stage_pack(acc).reshape(8, 8, 128)
    phase("e3_y")
    flights = [copy(s3.at[ring(cy, d, 8)], r3a.at[cy], at(y=ring(cy, d, 8))) for d in FAR_FIRST]
    r3a[cy] = s3[cy]
    for f in flights:
        f.wait()
    phase("e3_x")
    flights = [
        copy(r3a.at[:, pl.ds(ring(cx, d, 8), 1)], r3b.at[:, pl.ds(cx, 1)], at(x=ring(cx, d, 8))) for d in FAR_FIRST
    ]
    r3b[:, pl.ds(cx, 1)] = r3a[:, pl.ds(cx, 1)]
    for f in flights:
        f.wait()
    phase("z")
    for k in (7, 8, 9, 10, 11, 12):
        loads[k].wait()
    turned = stage_z(r3b[...].reshape(64, 128), qx[py * 16 + px], qy[band], rz, gz)

    phase("e4")
    for i in range(3):
        s4[:, i] = turned[i].reshape(4, 16, 128)
    flights = []
    for e in (2, 1, 3, 0):
        y = ring(py, e, 4)
        for d, flip in [(d, flip) for d in FAR_FIRST + (0,) for flip in (1, 0)]:
            if e or d or flip:
                z, c = ring(cz, d, 8), lax.rem(cc + flip, 2)
                rows = s4.at[y, :, pl.ds(c * 8 + z, 1)]
                flights.append(copy(rows, r4c.at[cc, py, :, pl.ds(cz, 1)], at(z=z, c=c, y=2 * y + lo)))
    r4c[cc, py, :, pl.ds(cz, 1)] = s4[py, :, pl.ds(cc * 8 + cz, 1)]
    for f in flights:
        f.wait()
    phase("y")
    x = [jnp.concatenate([r4c[0, q, i], r4c[1, q, i]], axis=0) for i in range(3) for q in range(4)]
    along = stage_y(x, ryi)

    s5[...] = along.astype(BF).reshape(2, 8, 16, 128)
    phase("e5")
    flights = []
    for d, flip in [(d, flip) for d in FAR_FIRST for flip in (1, 0)] + [(0, 1)]:
        to_x, to_lo = ring(cx, d, 8), lax.rem(lo + flip, 2)
        flights.append(copy(s5.at[to_lo, to_x], r5b.at[lo, cx], at(x=to_x, y=2 * py + to_lo)))
    r5b[lo, cx] = s5[lo, cx]
    for f in flights:
        f.wait()
    phase("x")
    wide[...] = r5b[...].astype(F32).reshape(256, 128)
    a = [wide[pl.ds(y, 16, stride=16), :] for y in range(16)]
    g = [a[12 + y % 4] if y < 4 else roll(a[12 + y % 4], 128 - 40 * (y // 4), 1) for y in range(12)]
    rho, hart, gx, gy, gzz = stage_x(a[:12], g, rxi)
    value = stage_potential(rho, hart, gx, gy, gzz)

    r6[cz] = stage_block([value, gx, gy, gzz])
    phase("e6")
    chunks = (pl.ds(0, 128), pl.ds(128, 112))
    hops, relays, last, home = {}, {}, [], []

    def block(away):
        return r6.at[ring(cz, away % 8, 8)]

    def go(ref, away):
        return copy(ref, ref, at(z=ring(cz, away % 8, 8)))

    def settle(away):
        slot = out.at[cc, ring(cz, away % 8, 8)]
        last.append(copy(block(away), slot, at(c=other)))
        home.append(pltpu.make_async_copy(block(away), slot, store.at[len(home)]))
        home[-1].start()

    for d in (2, -2):
        for h in (0, 1):
            hops[d, h] = go(block(0).at[chunks[h]], d)
    for d in (1, -1):
        hops[d, 0] = go(block(0), d)
    settle(0)
    for h in (0, 1):
        for way in (1, -1):
            hops[2 * way, h].wait_recv()
            got = block(-2 * way).at[chunks[h]]
            relays[3 * way, h] = go(got, way)
            if h == (1 - way) // 2:
                relays[4 * way, h] = go(got, 2 * way)
    settle(-2)
    settle(2)
    for way in (1, -1):
        hops[way, 0].wait_recv()
        settle(-way)
    for way in (1, -1):
        for h in (0, 1):
            relays[3 * way, h].wait_recv()
        settle(-3 * way)
    relays[4, 0].wait_recv()
    relays[-4, 1].wait_recv()
    settle(4)
    for f in list(hops.values()) + list(relays.values()):
        f.wait_send()
    for f in last + home:
        f.wait()
    phase(None)


def lay_kernel(r6, pot, grad, got, wide, woven, done, load, store):
    loads = [pltpu.make_async_copy(r6.at[c], got.at[c], load.at[c]) for c in range(2)]
    for c in loads:
        c.start()
    for c in range(2):
        loads[c].wait()
        wide[1920 * c : 1920 * c + 1920] = got[c].astype(F32).reshape(1920, 128)

    def step(y, carry):
        for k in range(4):
            for j in range(3):
                z = pl.ds(j, 16, stride=3)
                woven[k, 0, z] = wide[pl.ds(40 * k + 12 * j + y, 16, stride=240), :]
                tail = wide[pl.ds(160 + 40 * (k // 2) + 12 * j + y, 16, stride=240), :]
                woven[k, 1, z] = roll(tail, 64, 1) if k % 2 else tail
            done[k, y, :, 0:128] = woven[k, 0]
            done[k, y, :, 128:192] = woven[k, 1, :, 0:64]
        return carry

    stores = []
    for q in range(3):
        lax.fori_loop(4 * q, 4 * q + 4, step, 0)
        rows = pl.ds(4 * q, 4)
        for k in range(4):
            target = pot.at[rows] if k == 0 else grad.at[k - 1, rows]
            stores.append(pltpu.make_async_copy(done.at[k, rows], target, store.at[4 * q + k]))
            stores[-1].start()
    for c in stores:
        c.wait()


def body(orbitals, occupations, stick_map, core_density):
    tables = make_tables()
    far = pl.BlockSpec(memory_space=pltpu.HBM)
    operands = [orbitals[0], stick_map, core_density.transpose(1, 0, 2), *tables]
    scratch = [pltpu.VMEM(a.shape, a.dtype) for a in operands] + [
        pltpu.VMEM((1024, 512), BF),
        pltpu.VMEM((384, 1024), BF),
        pltpu.VMEM((8, 8, 8, 128), BF),
        pltpu.VMEM((8, 8, 8, 128), BF),
        pltpu.VMEM((8, 8, 8, 128), BF),
        pltpu.VMEM((3, 12, N), F32),
        pltpu.VMEM((3, 12, N), F32),
        pltpu.VMEM((6, 256, 256), BF),
        pltpu.VMEM((3, 256, 256), F32),
        pltpu.VMEM((3, 128, 256), F32),
        pltpu.VMEM((3, 8, 16, 256), BF),
        pltpu.VMEM((8, 3, 16, 256), BF),
        pltpu.VMEM((8, 8, 128), F32),
        pltpu.VMEM((8, 8, 128), F32),
        pltpu.VMEM((8, 8, 128), F32),
        pltpu.VMEM((4, 3, 16, 128), F32),
        pltpu.VMEM((2, 4, 3, 8, 128), F32),
        pltpu.VMEM((2, 8, 16, 128), BF),
        pltpu.VMEM((2, 8, 16, 128), BF),
        pltpu.VMEM((256, 128), F32),
        pltpu.VMEM((8, 240, 128), BF),
        pltpu.SemaphoreType.DMA((180,)),
        pltpu.SemaphoreType.DMA((180,)),
        pltpu.SemaphoreType.DMA((13,)),
        pltpu.SemaphoreType.DMA((16,)),
    ]
    blocks = pl.pallas_call(
        kernel,
        out_shape=jax.ShapeDtypeStruct((2, 8, 240, 128), BF),
        in_specs=[pl.BlockSpec(memory_space=pltpu.SMEM)] + [far] * len(operands),
        out_specs=far,
        scratch_shapes=scratch,
        compiler_params=pltpu.CompilerParams(collective_id=0, has_side_effects=True, vmem_limit_bytes=67_043_328),
    )(occupations, *operands)
    pot, grad = pl.pallas_call(
        lay_kernel,
        out_shape=(
            jax.ShapeDtypeStruct((12, 48, N), F32),
            jax.ShapeDtypeStruct((3, 12, 48, N), F32),
        ),
        in_specs=[far],
        out_specs=(far, far),
        scratch_shapes=[
            pltpu.VMEM((2, 8, 240, 128), BF),
            pltpu.VMEM((3840, 128), F32),
            pltpu.VMEM((4, 2, 48, 128), F32),
            pltpu.VMEM((4, 12, 48, N), F32),
            pltpu.SemaphoreType.DMA((2,)),
            pltpu.SemaphoreType.DMA((12,)),
        ],
        compiler_params=pltpu.CompilerParams(vmem_limit_bytes=67_043_328),
    )(blocks)
    return pot.transpose(1, 0, 2), grad.transpose(0, 2, 1, 3)


def solution(mesh):
    return jax.shard_map(
        body,
        mesh=mesh,
        in_specs=(P("band", ("px", "py"), None), P("band"), P(None, "px"), P("py", "px", None)),
        out_specs=(P("py", "px", None), P(None, "py", "px", None)),
        check_vma=False,
    )
```
